128 devices in a mesh: fsdp: 16 (over z, y), model: 8 (over x, core).
Axes of the slice: x: 4, y: 4, z: 4, core: 2. Of those that a mesh axis runs over, the one named last changes fastest.
Arguments:
- x_in: bfloat16 [32, 512, 3072], P('fsdp', 'model')
- grad_out: bfloat16 [32, 512, 3072], P('fsdp', 'model')
- gain_attn: float32 [3072], replicated
- gain_mlp: float32 [3072], replicated
- w_qkv: bfloat16 [3072, 5120], P('fsdp', 'model')
- w_out: bfloat16 [3072, 3072], P('model', 'fsdp')
- w_gate: bfloat16 [3072, 8192], P('fsdp', 'model')
- w_up: bfloat16 [3072, 8192], P('fsdp', 'model')
- w_down: bfloat16 [8192, 3072], P('model', 'fsdp')
- rope_cos: float32 [512, 64], replicated
- rope_sin: float32 [512, 64], replicated
Outputs:
- output 1: bfloat16 [32, 512, 3072], P('fsdp', 'model')
- output 2: bfloat16 [32, 512, 3072], P('fsdp', 'model')
- output 3: float32 [3072], replicated
- output 4: float32 [3072], replicated
- output 5: float32 [3072, 5120], P('fsdp', 'model')
- output 6: float32 [3072, 3072], P('model', 'fsdp')
- output 7: float32 [3072, 8192], P('fsdp', 'model')
- output 8: float32 [3072, 8192], P('fsdp', 'model')
- output 9: float32 [8192, 3072], P('model', 'fsdp')
All inputs are finite; a program needn't handle non-finite values.
Results may differ from the reference program's by a relative error of at most 0.0161748.
Values are sent between devices in bfloat16 or wider.
A program may use at most 1 GiB of HBM per device.

```python
import jax
import jax.numpy as jnp
from jax import lax

BATCH = 32
SEQ_LEN = 512
D_MODEL = 3072
D_FF = 8192
HEADS = 24
KV_HEADS = 8
HEAD_DIM = 128
GROUP_SIZE = HEADS // KV_HEADS
QKV_COLS = KV_HEADS * (GROUP_SIZE + 2) * HEAD_DIM
NORM_EPS = 1e-5
ROPE_BASE = 500000.0


def rope_tables(key):
    step_key, offset_key = jax.random.split(key)
    steps = jax.random.randint(step_key, (SEQ_LEN,), 1, 4)
    offset = jax.random.randint(offset_key, (), 0, 1024)
    positions = (jnp.cumsum(steps) + offset).astype(jnp.float32)
    freqs = ROPE_BASE ** (-jnp.arange(0, HEAD_DIM, 2).astype(jnp.float32) / HEAD_DIM)
    angles = positions[:, None] * freqs[None, :]
    return jnp.cos(angles), jnp.sin(angles)


def normal_weight(key, rows, cols):
    return (jax.random.normal(key, (rows, cols), jnp.float32) * rows ** -0.5).astype(jnp.bfloat16)


def setup_inputs(seed: int = 0) -> dict:
    keys = jax.random.split(jax.random.key(seed), 10)
    act_shape = (BATCH, SEQ_LEN, D_MODEL)
    rope_cos, rope_sin = rope_tables(keys[9])
    return {
        'x_in': jax.random.normal(keys[0], act_shape, jnp.float32).astype(jnp.bfloat16),
        'grad_out': jax.random.normal(keys[1], act_shape, jnp.float32).astype(jnp.bfloat16),
        'gain_attn': 1.0 + 0.3 * jax.random.normal(keys[2], (D_MODEL,), jnp.float32),
        'gain_mlp': 1.0 + 0.3 * jax.random.normal(keys[3], (D_MODEL,), jnp.float32),
        'w_qkv': normal_weight(keys[4], D_MODEL, QKV_COLS),
        'w_out': normal_weight(keys[5], HEADS * HEAD_DIM, D_MODEL),
        'w_gate': normal_weight(keys[6], D_MODEL, D_FF),
        'w_up': normal_weight(keys[7], D_MODEL, D_FF),
        'w_down': normal_weight(keys[8], D_FF, D_MODEL),
        'rope_cos': rope_cos,
        'rope_sin': rope_sin,
    }


def rms_norm(x_f32, gain):
    inv_rms = lax.rsqrt(jnp.mean(x_f32 * x_f32, axis=-1, keepdims=True) + NORM_EPS)
    return (x_f32 * inv_rms * gain).astype(jnp.bfloat16)


def rotate(tensor, cos_t, sin_t):
    half = HEAD_DIM // 2
    first = tensor[..., :half]
    second = tensor[..., half:]
    return jnp.concatenate([first * cos_t - second * sin_t, second * cos_t + first * sin_t], axis=-1)


def matmul(left, right):
    return jnp.dot(left.astype(jnp.float32), right.astype(jnp.float32))


def layer_seq(x_seq, params, rope_cos, rope_sin):
    gain_attn, gain_mlp, w_qkv, w_out, w_gate, w_up, w_down = params
    x_f32 = x_seq.astype(jnp.float32)
    h_attn = rms_norm(x_f32, gain_attn)
    qkv = matmul(h_attn, w_qkv).reshape(SEQ_LEN, KV_HEADS, GROUP_SIZE + 2, HEAD_DIM)
    query = rotate(qkv[:, :, :GROUP_SIZE], rope_cos[:, None, None, :], rope_sin[:, None, None, :]).astype(jnp.bfloat16)
    key_rot = rotate(qkv[:, :, GROUP_SIZE], rope_cos[:, None, :], rope_sin[:, None, :]).astype(jnp.bfloat16)
    value = qkv[:, :, GROUP_SIZE + 1].astype(jnp.bfloat16)
    scores = jnp.einsum('qkgd,tkd->kgqt', query.astype(jnp.float32), key_rot.astype(jnp.float32)) * HEAD_DIM ** -0.5
    pos_ids = jnp.arange(SEQ_LEN)
    scores = jnp.where(pos_ids[:, None] >= pos_ids[None, :], scores, -1e30)
    attn_prob = jax.nn.softmax(scores, axis=-1).astype(jnp.bfloat16)
    attn = jnp.einsum('kgqt,tkd->qkgd', attn_prob.astype(jnp.float32), value.astype(jnp.float32)).astype(jnp.bfloat16)
    attn_proj = matmul(attn.reshape(SEQ_LEN, HEADS * HEAD_DIM), w_out).astype(jnp.bfloat16)
    mid_f32 = (x_f32 + attn_proj.astype(jnp.float32)).astype(jnp.bfloat16).astype(jnp.float32)
    h_mlp = rms_norm(mid_f32, gain_mlp)
    gate = matmul(h_mlp, w_gate)
    up_proj = matmul(h_mlp, w_up)
    gated_act = (jax.nn.silu(gate) * up_proj).astype(jnp.bfloat16)
    mlp_out = matmul(gated_act, w_down).astype(jnp.bfloat16)
    return (mid_f32 + mlp_out.astype(jnp.float32)).astype(jnp.bfloat16)


def reference(x_in, grad_out, gain_attn, gain_mlp, w_qkv, w_out, w_gate, w_up, w_down, rope_cos, rope_sin):
    params = tuple(weight.astype(jnp.float32) for weight in (gain_attn, gain_mlp, w_qkv, w_out, w_gate, w_up, w_down))

    def layer_fn(x_seq, param_set):
        return layer_seq(x_seq, param_set, rope_cos, rope_sin)

    def seq_step(accum, seq_pair):
        x_seq, dy_seq = seq_pair
        y_seq, vjp_fn = jax.vjp(layer_fn, x_seq, params)
        dx_seq, dparams = vjp_fn(dy_seq)
        return jax.tree.map(jnp.add, accum, dparams), (y_seq, dx_seq)

    zero_grads = jax.tree.map(jnp.zeros_like, params)
    grads, (y_out, dx_in) = lax.scan(seq_step, zero_grads, (x_in, grad_out))
    return (y_out, dx_in, grads[0], grads[1], grads[2], grads[3], grads[4], grads[5], grads[6])
```

```python
import functools

import jax
import jax.numpy as jnp
from jax import lax
from jax.experimental import pallas as pl
from jax.experimental.pallas import tpu as pltpu
from jax.sharding import PartitionSpec as P


NORM_EPS = 1e-5
F32 = jnp.float32
BF16 = jnp.bfloat16
MESH = pl.DeviceIdType.MESH
X_CHIPS = 4
ROWS = 16


def model_peers():
    m = lax.axis_index('model')
    x, c = m // 2, m % 2
    other = 2 * x + (1 - c)
    nxt = 2 * ((x + 1) % X_CHIPS) + c
    prv = 2 * ((x + 3) % X_CHIPS) + c
    return x, c, other, nxt, prv


def model_barrier(peers):
    sem = pltpu.get_barrier_semaphore()
    for peer in peers:
        pl.semaphore_signal(sem, inc=1, device_id={'model': peer}, device_id_type=MESH)
    pl.semaphore_wait(sem, len(peers))


def remote(src, dst, send_sem, recv_sem, peer):
    return pltpu.make_async_remote_copy(src_ref=src, dst_ref=dst, send_sem=send_sem, recv_sem=recv_sem,
                                        device_id={'model': peer}, device_id_type=MESH)


def row_loop(n_rows, fn):
    def step(i, carry):
        fn(pl.ds(pl.multiple_of(i * ROWS, ROWS), ROWS))
        return carry

    lax.fori_loop(0, n_rows // ROWS, step, 0)


class Gather:
    SEMS = 9

    def __init__(self, src, out, send, recv, local):
        self.src, self.out, self.send, self.recv, self.local = src, out, send, recv, local
        self.x, self.c, self.other, self.nxt, self.prv = model_peers()
        self.half = src.shape[0] // 2

    def slot(self, dx, core):
        return self.out.at[2 * ((self.x + dx) % X_CHIPS) + core]

    def part(self, dx, core, upper):
        return self.out.at[2 * ((self.x + dx) % X_CHIPS) + core, pl.ds(self.half * upper, self.half)]

    def copy(self, i, src, dst, peer):
        return remote(src, dst, self.send.at[i], self.recv.at[i], peer)

    def copies(self):
        c = self.c
        mine = self.slot(0, c)
        return [
            (self.src, mine, self.other), (self.src, mine, self.nxt), (self.src, mine, self.prv),
            (self.part(3, c, 0), self.part(3, c, 0), self.nxt), (self.part(1, c, 1), self.part(1, c, 1), self.prv),
            (self.slot(3, c), self.slot(3, c), self.other), (self.slot(1, c), self.slot(1, c), self.other),
            (self.part(2, c, 0), self.part(2, c, 0), self.other), (self.part(2, c, 1), self.part(2, c, 1), self.other),
        ]

    def landing(self):
        c, o = self.c, 1 - self.c
        return [self.slot(0, o), self.slot(3, c), self.slot(1, c), self.part(2, c, 0), self.part(2, c, 1),
                self.slot(3, o), self.slot(1, o), self.part(2, o, 0), self.part(2, o, 1)]

    def start(self, *which):
        table = self.copies()
        for i in which:
            self.copy(i, *table[i]).start()

    def wait_recv(self, *which):
        table = self.landing()
        for i in which:
            self.copy(i, table[i], table[i], self.other).wait_recv()

    def begin(self):
        pltpu.make_async_copy(self.src, self.slot(0, self.c), self.local).start()
        self.start(1, 2, 0)

    def forward_near(self):
        self.wait_recv(1)
        self.start(3, 5)
        self.wait_recv(2)
        self.start(4, 6)

    def forward_far(self):
        self.wait_recv(3)
        self.start(7)
        self.wait_recv(4)
        self.start(8)

    def finish(self):
        self.wait_recv(0, 5, 6, 7, 8)
        table = self.copies()
        for i in range(self.SEMS):
            self.copy(i, *table[i]).wait_send()
        pltpu.make_async_copy(self.src, self.slot(0, self.c), self.local).wait()


class RingGather:
    SEMS = 4

    def __init__(self, src, slot, nxt, prv, send, recv):
        self.src, self.slot, self.nxt, self.prv, self.send, self.recv = src, slot, nxt, prv, send, recv
        half = src.shape[0] // 2
        self.upper, self.lower = pl.ds(0, half), pl.ds(half, half)

    def copy(self, i, src, dst, peer):
        return pltpu.make_async_remote_copy(src_ref=src, dst_ref=dst, send_sem=self.send.at[i], recv_sem=self.recv.at[i],
                                            device_id={'fsdp': peer}, device_id_type=MESH)

    def copies(self):
        up, low = self.slot(3).at[self.upper], self.slot(1).at[self.lower]
        return [(self.src, self.slot(0), self.nxt), (self.src, self.slot(0), self.prv),
                (up, up, self.nxt), (low, low, self.prv)]

    def start(self, *which):
        table = self.copies()
        for i in which:
            self.copy(i, *table[i]).start()

    def wait_recv(self, *which):
        table = [self.slot(3), self.slot(1), self.slot(2).at[self.upper], self.slot(2).at[self.lower]]
        for i in which:
            self.copy(i, table[i], table[i], self.nxt).wait_recv()

    def near(self):
        self.wait_recv(0)
        self.start(2)
        self.wait_recv(1)
        self.start(3)

    def wait_send(self):
        table = self.copies()
        for i in range(self.SEMS):
            self.copy(i, *table[i]).wait_send()


class WeightGather:
    SEMS = 10

    def __init__(self, src, out, send, recv, local):
        self.src, self.out, self.local = src, out, local
        f = lax.axis_index('fsdp')
        z, y = f // 4, f % 4
        self.f = f
        rows = src.shape[0] // 2
        self.nxt = {'z': 4 * ((z + 1) % 4) + y, 'y': 4 * z + (y + 1) % 4}
        self.prv = {'z': 4 * ((z + 3) % 4) + y, 'y': 4 * z + (y + 3) % 4}
        self.first, self.second = [], []
        for color, (one, two) in enumerate((('y', 'z'), ('z', 'y'))):
            part = pl.ds(color * rows, rows)

            def at(d_one, d_two, one=one, part=part):
                dy, dz = (d_one, d_two) if one == 'y' else (d_two, d_one)
                return out.at[4 * ((z + dz) % 4) + (y + dy) % 4, part]

            base = 5 * color

            def ring(i, src_ref, slot, axis, base=base):
                return RingGather(src_ref, slot, self.nxt[axis], self.prv[axis], send.at[base + i], recv.at[base + i])

            self.first.append(ring(0, src.at[part], lambda d, at=at: at(d, 0), one))
            self.second.append([ring(1 + d, src.at[part] if d == 0 else at(d, 0),
                                     lambda e, d=d, at=at: at(d, e), two) for d in range(4)])

    def barrier_peers(self):
        return [self.nxt['z'], self.prv['z'], self.nxt['y'], self.prv['y']]

    def begin(self):
        pltpu.make_async_copy(self.src, self.out.at[self.f], self.local).start()
        for color in range(2):
            self.first[color].start(0, 1)
        for color in range(2):
            self.second[color][0].start(0, 1)

    def step_near(self):
        for color in range(2):
            one, two = self.first[color], self.second[color]
            one.wait_recv(0)
            one.start(2)
            two[3].start(0, 1)
        for color in range(2):
            one, two = self.first[color], self.second[color]
            one.wait_recv(1)
            one.start(3)
            two[1].start(0, 1)

    def step_own(self):
        for color in range(2):
            self.second[color][0].near()

    def step_far(self):
        for color in range(2):
            self.first[color].wait_recv(2, 3)
            self.second[color][2].start(0, 1)

    def step_second(self, d):
        for color in range(2):
            self.second[color][d].near()

    def finish(self):
        for color in range(2):
            for ring in self.second[color]:
                ring.wait_recv(2, 3)
            for ring in [self.first[color]] + self.second[color]:
                ring.wait_send()
        pltpu.make_async_copy(self.src, self.out.at[self.f], self.local).wait()


class Scatter:
    SEMS = 10
    DIST = (2, 1, 3, 0)
    CHUNKS = 4

    def __init__(self, rows_of, weight, box, pair, mine, far, near, send, recv):
        self.rows_of, self.weight, self.box = rows_of, weight, box
        self.pair, self.mine, self.far, self.near = pair, mine, far, near
        self.send, self.recv = send, recv
        self.x, self.c, self.other, self.nxt, self.prv = model_peers()
        self.rows, self.width = mine.shape[1], mine.shape[2]
        self.lo = pl.ds(0, self.width // 2)
        self.hi = pl.ds(self.width // 2, self.width // 2)

    def copies(self):
        rows = slice(None)
        m = self.mine
        return [(self.box.at[k], self.pair.at[k], self.other) for k in range(4)] + [
            (m.at[0, rows, self.lo], self.far.at[0], self.nxt), (m.at[0, rows, self.hi], self.far.at[1], self.prv),
            (m.at[1, rows, self.hi], self.near.at[0, rows, self.hi], self.nxt),
            (m.at[2, rows, self.lo], self.near.at[1, rows, self.lo], self.prv),
            (m.at[1, rows, self.lo], self.near.at[0, rows, self.lo], self.nxt),
            (m.at[2, rows, self.hi], self.near.at[1, rows, self.hi], self.prv),
        ]

    def copy(self, i):
        src, dst, peer = self.copies()[i]
        return remote(src, dst, self.send.at[i], self.recv.at[i], peer)

    def wait_recv(self, i):
        dst = self.copies()[i][1]
        remote(dst, dst, self.send.at[i], self.recv.at[i], self.other).wait_recv()

    def produce(self, k):
        place = 2 * ((self.x + self.DIST[k]) % X_CHIPS)
        left = jnp.concatenate([self.rows_of(place + self.c), self.rows_of(place + 1 - self.c)], axis=0)
        step = self.width // self.CHUNKS

        def chunk(i, carry):
            cols = pl.ds(pl.multiple_of(i * step, step), step)
            both = lax.dot_general(left, self.weight[cols, :], (((1,), (1,)), ((), ())), preferred_element_type=F32)
            self.box[k, :, cols] = both[self.rows:]
            self.mine[k, :, cols] = both[:self.rows]
            return carry

        lax.fori_loop(0, self.CHUNKS, chunk, 0)

    def pass_on(self, k):
        self.produce(k)
        self.copy(k).start()

    def pair_sum(self, k):
        self.wait_recv(k)

        def add(rows):
            self.mine[k, rows, :] = self.mine[k, rows, :] + self.pair[k, rows, :]

        row_loop(self.rows, add)

    def send_near(self):
        self.pass_on(0)
        self.pass_on(1)
        self.pair_sum(0)
        self.copy(4).start()
        self.copy(5).start()
        self.pass_on(2)
        self.pair_sum(1)
        self.copy(6).start()
        self.pass_on(3)
        self.pair_sum(2)
        self.copy(7).start()

    def send_far(self):
        self.wait_recv(4)

        def add_lo(rows):
            self.mine[1, rows, self.lo] = self.mine[1, rows, self.lo] + self.far[0, rows, :]

        row_loop(self.rows, add_lo)
        self.copy(8).start()
        self.wait_recv(5)

        def add_hi(rows):
            self.mine[2, rows, self.hi] = self.mine[2, rows, self.hi] + self.far[1, rows, :]

        row_loop(self.rows, add_hi)
        self.copy(9).start()

    def arrive(self):
        self.pair_sum(3)
        for i in (6, 8, 7, 9):
            self.wait_recv(i)

    def total(self, rows):
        return self.mine[3, rows, :] + self.near[0, rows, :] + self.near[1, rows, :]

    def finish(self):
        for i in range(self.SEMS):
            self.copy(i).wait_send()

    SCRATCH = 7

    @classmethod
    def scratch(cls, units, pos, width):
        return [pltpu.VMEM((units, 4, pos, width), F32), pltpu.VMEM((units, 4, pos, width), F32),
                pltpu.VMEM((units, 4, pos, width), F32),
                pltpu.VMEM((units, 2, pos, width // 2), F32), pltpu.VMEM((units, 2, pos, width), F32),
                pltpu.SemaphoreType.DMA((units, cls.SEMS)), pltpu.SemaphoreType.DMA((units, cls.SEMS))]

    @classmethod
    def of(cls, u, rows_of, weight, scratch):
        return cls(rows_of, weight, *(ref.at[u] for ref in scratch))


def gather_scratch(units):
    return [pltpu.SemaphoreType.DMA((units, Gather.SEMS)), pltpu.SemaphoreType.DMA((units, Gather.SEMS)),
            pltpu.SemaphoreType.DMA((units,))]


def gather_of(u, src, out, sems):
    send, recv, local = sems
    return Gather(src, out, send.at[u], recv.at[u], local.at[u])


def norm_rows(x_f32, gain):
    inv_rms = lax.rsqrt(jnp.mean(x_f32 * x_f32, axis=-1, keepdims=True) + NORM_EPS)
    return x_f32 * inv_rms * gain


def norm_rows_back(x_f32, gain, cotangent):
    inv_rms = lax.rsqrt(jnp.mean(x_f32 * x_f32, axis=-1, keepdims=True) + NORM_EPS)
    x_hat = x_f32 * inv_rms
    scaled = cotangent * gain
    inner = jnp.mean(scaled * x_hat, axis=-1, keepdims=True)
    return inv_rms * (scaled - x_hat * inner), cotangent * x_hat


def enter_kernel(x_ref, dy_ref, gain_ref, wqkv_ref, wout_ref, h_out, dy_out, w_out, h_src, w_src, *sems):
    n_seq, pos = x_ref.shape[:2]
    g_sems, w_sems = sems[:3], sems[3:]
    qkv_cols = wqkv_ref.shape[1]
    w_src[:, :qkv_cols] = wqkv_ref[...]
    w_src[:, qkv_cols:] = wout_ref[...]
    for s in range(n_seq):
        def norm(rows):
            h_src[s, rows, :] = norm_rows(x_ref[s, rows, :].astype(F32), gain_ref[...]).astype(BF16)

        row_loop(pos, norm)
    weights = WeightGather(w_src, w_out, *w_sems)
    _, _, other, nxt, prv = model_peers()
    sem = pltpu.get_barrier_semaphore()
    for peer in weights.barrier_peers():
        pl.semaphore_signal(sem, inc=1, device_id={'fsdp': peer}, device_id_type=MESH)
    for peer in (other, nxt, prv):
        pl.semaphore_signal(sem, inc=1, device_id={'model': peer}, device_id_type=MESH)
    pl.semaphore_wait(sem, 7)
    units = [gather_of(s, h_src.at[s], h_out.at[s], g_sems) for s in range(n_seq)]
    units += [gather_of(n_seq + s, dy_ref.at[s], dy_out.at[s], g_sems) for s in range(n_seq)]
    weights.begin()
    for unit in units:
        unit.begin()
    weights.step_near()
    units[0].forward_near()
    weights.step_own()
    weights.step_far()
    units[1].forward_near()
    weights.step_second(3)
    weights.step_second(1)
    units[2].forward_near()
    weights.step_second(2)
    units[3].forward_near()
    for unit in units:
        unit.forward_far()
    weights.finish()
    for unit in units:
        unit.finish()


def load_rows(refs, s, pos):
    def rows_of(place):
        rows = pl.ds(pl.multiple_of(place * pos, pos), pos)
        return jnp.concatenate([ref[s, rows, :] for ref in refs], axis=1)

    return rows_of


def fetch_weight(w_hbm, first_col, w_vmem, sem):
    return pltpu.make_async_copy(w_hbm.at[:, pl.ds(first_col, w_vmem.shape[1])], w_vmem, sem)


def middle_kernel(backward, first_col, n_left, *refs):
    left, refs = refs[:n_left], refs[n_left:]
    w_hbm, base_ref, mid_ref, gain_ref, res_ref, full_out, dgain_ref = refs[:7]
    scratch = refs[7:]
    n_seq, pos = base_ref.shape[:2]
    rs_scratch, scratch = scratch[:Scatter.SCRATCH], scratch[Scatter.SCRATCH:]
    w_vmem, w_sem, g_src, sums = scratch[:4]
    sems = scratch[4:]
    fetch_weight(w_hbm, first_col, w_vmem, w_sem).start()
    _, _, other, nxt, prv = model_peers()
    model_barrier((other, nxt, prv))
    units = [Scatter.of(s, load_rows(left, s, pos), w_vmem, rs_scratch) for s in range(n_seq)]
    sends = [gather_of(s, g_src.at[s], full_out.at[s], sems) for s in range(n_seq)]
    if backward:
        sums[...] = jnp.zeros_like(sums)

    def settle(s):
        units[s].arrive()

        def rows_fn(rows):
            red = units[s].total(rows).astype(BF16).astype(F32)
            if backward:
                d_norm, d_gain = norm_rows_back(mid_ref[s, rows, :].astype(F32), gain_ref[...], red)
                out = (base_ref[s, rows, :].astype(F32) + d_norm).astype(BF16)
                sums[...] += d_gain
                res_ref[s, rows, :] = out
                g_src[s, rows, :] = out
            else:
                mid = (base_ref[s, rows, :].astype(F32) + red).astype(BF16)
                res_ref[s, rows, :] = mid
                g_src[s, rows, :] = norm_rows(mid.astype(F32), gain_ref[...]).astype(BF16)

        row_loop(pos, rows_fn)

    fetch_weight(w_hbm, first_col, w_vmem, w_sem).wait()
    units[0].send_near()
    units[0].send_far()
    for s in range(n_seq):
        if s + 1 < n_seq:
            units[s + 1].send_near()
        settle(s)
        sends[s].begin()
        if s + 1 < n_seq:
            units[s + 1].send_far()
    for unit in sends:
        unit.forward_near()
    for unit in sends:
        unit.forward_far()
    if backward:
        dgain_ref[...] = jnp.sum(sums[...], axis=0, keepdims=True)
    else:
        dgain_ref[...] = jnp.zeros_like(dgain_ref)
    for unit in units:
        unit.finish()
    for unit in sends:
        unit.finish()


def leave_kernel(backward, first_col, left_ref, w_hbm, base_ref, x_ref, gain_ref, res_ref, dgain_ref, *scratch):
    n_seq, pos = base_ref.shape[:2]
    rs_scratch, (w_vmem, w_sem, sums) = scratch[:Scatter.SCRATCH], scratch[Scatter.SCRATCH:]
    fetch_weight(w_hbm, first_col, w_vmem, w_sem).start()
    _, _, other, nxt, prv = model_peers()
    model_barrier((other, nxt, prv))
    sums[...] = jnp.zeros_like(sums)
    units = [Scatter.of(s, load_rows([left_ref], s, pos), w_vmem, rs_scratch) for s in range(n_seq)]

    def settle(s):
        units[s].arrive()

        def rows_fn(rows):
            red = units[s].total(rows).astype(BF16).astype(F32)
            if backward:
                red, d_gain = norm_rows_back(x_ref[s, rows, :].astype(F32), gain_ref[...], red)
                sums[...] += d_gain
            res_ref[s, rows, :] = (base_ref[s, rows, :].astype(F32) + red).astype(BF16)

        row_loop(pos, rows_fn)

    fetch_weight(w_hbm, first_col, w_vmem, w_sem).wait()
    units[0].send_near()
    units[0].send_far()
    for s in range(n_seq):
        if s + 1 < n_seq:
            units[s + 1].send_near()
            units[s + 1].send_far()
        settle(s)
    dgain_ref[...] = jnp.sum(sums[...], axis=0, keepdims=True)
    for unit in units:
        unit.finish()


def spin(tensor, cos_t, sin_t):
    return tensor * cos_t + pltpu.roll(tensor, tensor.shape[1] // 2, 1) * sin_t


def probs(query, key, scale, first_row):
    scores = lax.dot_general(query, key, (((1,), (1,)), ((), ())), preferred_element_type=F32) * scale
    rows = first_row + lax.broadcasted_iota(jnp.int32, scores.shape, 0)
    cols = lax.broadcasted_iota(jnp.int32, scores.shape, 1)
    scores = jnp.where(rows >= cols, scores, -1e30)
    expd = jnp.exp(scores - jnp.max(scores, axis=-1, keepdims=True))
    return expd / jnp.sum(expd, axis=-1, keepdims=True)


def attn_kernel(heads, group, scale, h_ref, w_ref, cos_ref, sin_ref, qkv_ref, attn_ref):
    seq, head_dim = cos_ref.shape
    block = seq // 2
    n_groups = heads // group
    cols = qkv_ref.shape[2]

    def lanes(i):
        return slice(i * head_dim, (i + 1) * head_dim)

    def project(i, carry):
        rows = pl.ds(pl.multiple_of(i * block, block), block)
        qkv = jnp.dot(h_ref[0, rows, :], w_ref[:, :cols], preferred_element_type=F32)
        cos_t, sin_t = cos_ref[rows, :], sin_ref[rows, :]
        for j in range(cols // head_dim):
            one = qkv[:, lanes(j)]
            if j % (group + 2) <= group:
                one = spin(one, cos_t, sin_t)
            qkv_ref[0, rows, lanes(j)] = one.astype(BF16)
        return carry

    lax.fori_loop(0, seq // block, project, 0)
    for g in range(n_groups):
        first = g * (group + 2)
        for i in range(seq // block):
            rows, keys = slice(i * block, (i + 1) * block), slice(0, (i + 1) * block)
            key, value = qkv_ref[0, keys, lanes(first + group)], qkv_ref[0, keys, lanes(first + group + 1)]
            for j in range(group):
                prob = probs(qkv_ref[0, rows, lanes(first + j)], key, scale, i * block)
                attn_ref[0, rows, lanes(g * group + j)] = jnp.dot(
                    prob.astype(BF16), value, preferred_element_type=F32).astype(BF16)


def attn_back_kernel(heads, group, scale, dm_ref, w_ref, cos_ref, sin_ref, qkv_ref, dqkv_ref, do_ref, dk_ref, dv_ref):
    seq, head_dim = cos_ref.shape
    block = seq // 2
    n_groups = heads // group
    cols = qkv_ref.shape[2]

    def lanes(i):
        return slice(i * head_dim, (i + 1) * head_dim)

    def project(i, carry):
        rows = pl.ds(pl.multiple_of(i * block, block), block)
        do_ref[rows, :] = jnp.dot(dm_ref[0, rows, :], w_ref[:, cols:], preferred_element_type=F32).astype(BF16)
        return carry

    lax.fori_loop(0, seq // block, project, 0)
    over_rows = (((0,), (0,)), ((), ()))
    for g in range(n_groups):
        first = g * (group + 2)
        dk_ref[...] = jnp.zeros_like(dk_ref)
        dv_ref[...] = jnp.zeros_like(dv_ref)
        for i in range(seq // block):
            rows, keys = slice(i * block, (i + 1) * block), slice(0, (i + 1) * block)
            key, value = qkv_ref[0, keys, lanes(first + group)], qkv_ref[0, keys, lanes(first + group + 1)]
            for j in range(group):
                query = qkv_ref[0, rows, lanes(first + j)]
                d_out = do_ref[rows, lanes(g * group + j)]
                prob = probs(query, key, scale, i * block)
                d_prob = lax.dot_general(d_out, value, (((1,), (1,)), ((), ())), preferred_element_type=F32)
                row_dot = jnp.sum(d_prob * prob, axis=-1, keepdims=True)
                d_scores = (prob * (d_prob - row_dot) * scale).astype(BF16)
                d_query = jnp.dot(d_scores, key, preferred_element_type=F32)
                dqkv_ref[0, rows, lanes(first + j)] = spin(d_query, cos_ref[rows, :], -sin_ref[rows, :]).astype(BF16)
                dk_ref[keys, :] += lax.dot_general(d_scores, query, over_rows, preferred_element_type=F32)
                dv_ref[keys, :] += lax.dot_general(prob.astype(BF16), d_out, over_rows, preferred_element_type=F32)
        dqkv_ref[0, :, lanes(first + group)] = spin(dk_ref[...], cos_ref[...], -sin_ref[...]).astype(BF16)
        dqkv_ref[0, :, lanes(first + group + 1)] = dv_ref[...].astype(BF16)


def mlp_kernel(h_ref, dy_ref, wg_ref, wu_ref, wd_ref, act_ref, dgu_ref):
    tokens = h_ref.shape[0]
    block = tokens // 4

    def rows_fn(i, carry):
        rows = pl.ds(pl.multiple_of(i * block, block), block)
        gate = jnp.dot(h_ref[rows, :], wg_ref[...], preferred_element_type=F32)
        up_proj = jnp.dot(h_ref[rows, :], wu_ref[...], preferred_element_type=F32)
        d_act = jnp.dot(dy_ref[rows, :], wd_ref[...], preferred_element_type=F32).astype(BF16).astype(F32)
        sig_gate = jax.nn.sigmoid(gate)
        silu_gate = gate * sig_gate
        act_ref[rows, :] = (silu_gate * up_proj).astype(BF16)
        dgu_ref[0, rows, :] = (d_act * up_proj * sig_gate * (1.0 + gate * (1.0 - sig_gate))).astype(BF16)
        dgu_ref[1, rows, :] = (d_act * silu_gate).astype(BF16)
        return carry

    lax.fori_loop(0, tokens // block, rows_fn, 0)


def grad_kernel(n_first, *refs):
    one_ref, two_ref = refs[:2]
    first, second, out_ref = refs[2], refs[3], refs[4]
    over_rows = (((0,), (0,)), ((), ()))
    col = 0
    for i in range(n_first):
        right = first[i]
        out_ref[:, col:col + right.shape[1]] = lax.dot_general(one_ref[...], right, over_rows, preferred_element_type=F32)
        col += right.shape[1]
    out_ref[:, col:] = lax.dot_general(two_ref[...], second[...], over_rows, preferred_element_type=F32)


def gain_kernel(part_ref, out_ref, total, slots, send, recv):
    m = lax.axis_index('model')
    f = lax.axis_index('fsdp')
    x, c = m // 2, m % 2
    z, y = f // 4, f % 4
    stages = [[(f, 2 * x + (1 - c))],
              [(f, 2 * ((x + d) % 4) + c) for d in (1, 2, 3)],
              [(4 * z + (y + d) % 4, m) for d in (1, 2, 3)],
              [(4 * ((z + d) % 4) + y, m) for d in (1, 2, 3)]]
    places = [c, x, y, z]
    sem = pltpu.get_barrier_semaphore()
    n_peers = 0
    for peers in stages:
        for ff, mm in peers:
            pl.semaphore_signal(sem, inc=1, device_id={'fsdp': ff, 'model': mm}, device_id_type=MESH)
            n_peers += 1
    total[0] = part_ref[...]
    pl.semaphore_wait(sem, n_peers)
    for t, peers in enumerate(stages):
        n = len(peers) + 1
        place = places[t]
        copies = []
        for d, (ff, mm) in enumerate(peers):
            copies.append(pltpu.make_async_remote_copy(
                src_ref=total.at[t], dst_ref=slots.at[t, d], send_sem=send.at[t, d], recv_sem=recv.at[t, d],
                device_id={'fsdp': ff, 'model': mm}, device_id_type=MESH))
            copies[-1].start()
        for copy in copies:
            copy.wait_recv()
        terms = [total[t]] + [slots[t, d] for d in range(n - 1)]
        acc = None
        for place_i in range(n):
            term = terms[0]
            for d in range(n - 1):
                term = jnp.where((place + n - (d + 1)) % n == place_i, terms[d + 1], term)
            acc = term if acc is None else acc + term
        total[t + 1] = acc
        for copy in copies:
            copy.wait_send()
    out_ref[...] = total[len(stages)]


def solution(mesh):
    act_spec = P('fsdp', 'model', None)
    rows_spec = P('fsdp', 'model')
    cols_spec = P('model', 'fsdp')

    def device_fn(x_loc, dy_loc, gain_attn, gain_mlp, wqkv_sh, wout_sh, wgate_sh, wup_sh, wdown_sh, rope_cos, rope_sin):
        n_seq, pos, width = x_loc.shape
        seq = rope_cos.shape[0]
        tokens = n_seq * seq
        n_model = seq // pos
        head_dim = 2 * rope_cos.shape[1]
        heads = wout_sh.shape[0] // head_dim
        shard_rows, qkv_cols = wqkv_sh.shape
        out_rows, ff = wout_sh.shape[0], wgate_sh.shape[1]
        n_fsdp = width // shard_rows
        attn_cols = qkv_cols + out_rows
        kv = (qkv_cols // head_dim - heads) // 2
        group = heads // kv
        scale = head_dim ** -0.5
        gain_a, gain_m = gain_attn[None, :], gain_mlp[None, :]
        cos_t = jnp.concatenate([rope_cos, rope_cos], axis=1)
        sin_t = jnp.concatenate([-rope_sin, rope_sin], axis=1)

        vmem = pl.BlockSpec(memory_space=pltpu.VMEM)
        hbm = pl.BlockSpec(memory_space=pl.ANY)
        local_bf = jax.ShapeDtypeStruct((n_seq, pos, width), BF16)
        full_bf = jax.ShapeDtypeStruct((n_seq, n_model, pos, width), BF16)
        row_f32 = jax.ShapeDtypeStruct((1, width), F32)

        def params(cid):
            return pltpu.CompilerParams(collective_id=cid, has_side_effects=True, vmem_limit_bytes=60 * 2 ** 20)

        plain = pltpu.CompilerParams(vmem_limit_bytes=60 * 2 ** 20)

        def cost(flops, nbytes):
            return pl.CostEstimate(flops=int(flops), bytes_accessed=int(nbytes), transcendentals=0)

        def scatter_w(grad):
            return lax.psum_scatter(grad, 'fsdp', scatter_dimension=0, tiled=True)

        w_mlp = lax.all_gather(jnp.concatenate([wgate_sh, wup_sh, wdown_sh.T], axis=1), 'fsdp', axis=0, tiled=True)

        h_full, dy_full, w_attn = pl.pallas_call(
            enter_kernel,
            out_shape=(full_bf, full_bf, jax.ShapeDtypeStruct((n_fsdp, shard_rows, attn_cols), BF16)),
            in_specs=[vmem] * 5, out_specs=(hbm,) * 3,
            scratch_shapes=[pltpu.VMEM((n_seq, pos, width), BF16), pltpu.VMEM((shard_rows, attn_cols), BF16)]
            + gather_scratch(2 * n_seq)
            + [pltpu.SemaphoreType.DMA((WeightGather.SEMS, RingGather.SEMS)),
               pltpu.SemaphoreType.DMA((WeightGather.SEMS, RingGather.SEMS)), pltpu.SemaphoreType.DMA],
            compiler_params=params(0), name='enter', cost_estimate=cost(6e10, 2e7),
        )(x_loc, dy_loc, gain_a, wqkv_sh, wout_sh.T)
        h_attn = h_full.reshape(tokens, width)
        dy_full = dy_full.reshape(tokens, width)
        w_attn = w_attn.reshape(width, attn_cols)

        def per_seq(cols):
            return pl.BlockSpec((1, seq, cols), lambda s: (s, 0, 0))

        def whole(shape):
            return pl.BlockSpec(shape, lambda *_: (0,) * len(shape))

        qkv, attn = pl.pallas_call(
            functools.partial(attn_kernel, heads, group, scale), grid=(n_seq,),
            out_shape=(jax.ShapeDtypeStruct((n_seq, seq, qkv_cols), BF16),
                       jax.ShapeDtypeStruct((n_seq, seq, out_rows), BF16)),
            in_specs=[per_seq(width), whole((width, attn_cols)), whole((seq, head_dim)), whole((seq, head_dim))],
            out_specs=(per_seq(qkv_cols), per_seq(out_rows)), compiler_params=plain, name='attn',
            cost_estimate=cost(5e9, 2e7),
        )(h_attn.reshape(n_seq, seq, width), w_attn, cos_t, sin_t)

        def middle(backward, cid, left, w, first_col, base, mid):
            depth = sum(a.shape[-1] for a in left)
            scratch = (Scatter.scratch(n_seq, pos, width)
                       + [pltpu.VMEM((width, depth), BF16), pltpu.SemaphoreType.DMA,
                          pltpu.VMEM((n_seq, pos, width), BF16), pltpu.VMEM((ROWS, width), F32)]
                       + gather_scratch(n_seq))
            return pl.pallas_call(
                functools.partial(middle_kernel, backward, first_col, len(left)), out_shape=(local_bf, full_bf, row_f32),
                in_specs=[vmem] * len(left) + [hbm] + [vmem] * 3, out_specs=(vmem, hbm, vmem), scratch_shapes=scratch,
                compiler_params=params(cid), name='middle_bwd' if backward else 'middle_fwd',
                cost_estimate=cost(9e10, 2e7),
            )(*left, w, base, mid, gain_m)

        mid, h_mlp, _ = middle(False, 1, [attn], w_attn, qkv_cols, x_loc, x_loc)
        h_mlp = h_mlp.reshape(tokens, width)

        n_cols = 4
        ff_block = ff // n_cols

        def w_cols(part):
            return pl.BlockSpec((width, ff_block), lambda j: (0, part * n_cols + j))

        act, d_gu = pl.pallas_call(
            mlp_kernel, grid=(n_cols,),
            out_shape=(jax.ShapeDtypeStruct((tokens, ff), BF16), jax.ShapeDtypeStruct((2, tokens, ff), BF16)),
            in_specs=[whole((tokens, width)), whole((tokens, width)), w_cols(0), w_cols(1), w_cols(2)],
            out_specs=(pl.BlockSpec((tokens, ff_block), lambda j: (0, j)),
                       pl.BlockSpec((2, tokens, ff_block), lambda j: (0, 0, j))),
            compiler_params=plain, name='mlp', cost_estimate=cost(2e10, 4e7),
        )(h_mlp, dy_full, w_mlp, w_mlp, w_mlp)

        def weight_grads(one, two, first, second, block):
            n_first, _, cols = first.shape
            total = n_first * cols + second.shape[1]
            lhs = pl.BlockSpec((tokens, block), lambda i: (0, i))
            return pl.pallas_call(
                functools.partial(grad_kernel, n_first), grid=(width // block,),
                out_shape=jax.ShapeDtypeStruct((width, total), F32),
                in_specs=[lhs, lhs, whole(first.shape), whole(second.shape)],
                out_specs=pl.BlockSpec((block, total), lambda i: (i, 0)), compiler_params=plain,
                cost_estimate=cost(2 * tokens * width * total, 4 * width * total),
            )(one, two, first, second)

        dw_mlp = weight_grads(h_mlp, dy_full, d_gu, act, width // 12)
        rs_mlp = scatter_w(dw_mlp)
        d_gate, d_up, dw_mlp = lax.optimization_barrier((d_gu[0], d_gu[1], dw_mlp))

        def by_seq(arr):
            return arr.reshape(n_seq, seq, arr.shape[-1])

        d_mid, d_mid_full, dgain_mlp = middle(True, 2, [by_seq(d_gate), by_seq(d_up)], w_mlp, 0, dy_loc, mid)
        d_mid_full = d_mid_full.reshape(tokens, width)

        d_qkv = pl.pallas_call(
            functools.partial(attn_back_kernel, heads, group, scale), grid=(n_seq,),
            out_shape=jax.ShapeDtypeStruct((n_seq, seq, qkv_cols), BF16),
            in_specs=[per_seq(width), whole((width, attn_cols)), whole((seq, head_dim)), whole((seq, head_dim)),
                      per_seq(qkv_cols)],
            out_specs=per_seq(qkv_cols),
            scratch_shapes=[pltpu.VMEM((seq, out_rows), BF16), pltpu.VMEM((seq, head_dim), F32),
                            pltpu.VMEM((seq, head_dim), F32)],
            compiler_params=plain, name='attn_back', cost_estimate=cost(5e9, 2e7),
        )(d_mid_full.reshape(n_seq, seq, width), w_attn, cos_t, sin_t, qkv)

        dw_attn = weight_grads(h_attn, d_mid_full, d_qkv.reshape(1, tokens, qkv_cols), attn.reshape(tokens, out_rows),
                               width // 12)
        rs_attn = scatter_w(dw_attn)
        d_qkv, dw_attn = lax.optimization_barrier((d_qkv, dw_attn))

        def leave(backward, cid, left, w, first_col, base, x):
            return pl.pallas_call(
                functools.partial(leave_kernel, backward, first_col), out_shape=(local_bf, row_f32),
                in_specs=[vmem, hbm] + [vmem] * 3, out_specs=(vmem,) * 2,
                scratch_shapes=Scatter.scratch(n_seq, pos, width)
                + [pltpu.VMEM((width, left.shape[-1]), BF16), pltpu.SemaphoreType.DMA, pltpu.VMEM((ROWS, width), F32)],
                compiler_params=params(cid), name='leave_dx' if backward else 'leave_y', cost_estimate=cost(6e10, 2e7),
            )(left, w, base, x, gain_a)

        dx, dgain_attn = leave(True, 3, d_qkv, w_attn, 0, d_mid, x_loc)
        act, dgain_attn = lax.optimization_barrier((by_seq(act), dgain_attn))
        y, _ = leave(False, 5, act, w_mlp, 2 * ff, mid, x_loc)
        gain_part = jnp.concatenate([dgain_attn, dgain_mlp], axis=0).reshape(16, 2 * width // 16)
        gain_sum = pl.pallas_call(
            gain_kernel, out_shape=jax.ShapeDtypeStruct(gain_part.shape, F32), in_specs=[vmem], out_specs=vmem,
            scratch_shapes=[pltpu.VMEM((5,) + gain_part.shape, F32), pltpu.VMEM((4, 3) + gain_part.shape, F32),
                            pltpu.SemaphoreType.DMA((4, 3)), pltpu.SemaphoreType.DMA((4, 3))],
            compiler_params=params(4), name='gains', cost_estimate=cost(1e10, 1e5),
        )(gain_part).reshape(2, width)
        return (y, dx, gain_sum[0], gain_sum[1], rs_attn[:, :qkv_cols], rs_attn[:, qkv_cols:].T,
                rs_mlp[:, :ff], rs_mlp[:, ff:2 * ff], rs_mlp[:, 2 * ff:].T)

    in_specs = (act_spec, act_spec, P(), P(), rows_spec, cols_spec, rows_spec, rows_spec, cols_spec, P(), P())
    out_specs = (act_spec, act_spec, P(), P(), rows_spec, cols_spec, rows_spec, rows_spec, cols_spec)
    return jax.shard_map(device_fn, mesh=mesh, in_specs=in_specs, out_specs=out_specs, check_vma=False)
```

```python
import functools

import jax
import jax.numpy as jnp
from jax import lax
from jax.experimental import pallas as pl
from jax.experimental.pallas import tpu as pltpu
from jax.sharding import PartitionSpec as P

NORM_EPS = 1e-5
MASKED = -1e30
F32 = jnp.float32
BF16 = jnp.bfloat16
MESH = pl.DeviceIdType.MESH
DMA = pltpu.SemaphoreType.DMA
VMEM_LIMIT = 63 * 2 ** 20
RING = 4
ROWS = 16
PIECES = 4
HERE, NEXT, FAR, PREV = range(RING)
BY_RANK = (FAR, NEXT, PREV, HERE)
COLORS = range(2)
NT = (((1,), (1,)), ((), ()))
TN = (((0,), (0,)), ((), ()))


def go(place, distance):
    return (place + distance) % RING


def model_place():
    m = lax.axis_index('model')
    return m // 2, m % 2


def fsdp_place():
    f = lax.axis_index('fsdp')
    return f // RING, f % RING


def chip_targets():
    x, c = model_place()
    return [{'model': 2 * x + 1 - c}, {'model': 2 * go(x, NEXT) + c}, {'model': 2 * go(x, PREV) + c}]


def plane_targets():
    z, y = fsdp_place()
    return {'z': [{'fsdp': RING * go(z, d) + y} for d in (NEXT, PREV)],
            'y': [{'fsdp': RING * z + go(y, d)} for d in (NEXT, PREV)]}


def greet(targets):
    for target in targets:
        pl.semaphore_signal(pltpu.get_barrier_semaphore(), inc=1, device_id=target, device_id_type=MESH)


def met(targets):
    pl.semaphore_wait(pltpu.get_barrier_semaphore(), len(targets))


def chip_and_plane():
    plane = plane_targets()
    return chip_targets() + plane['z'] + plane['y']


def row_block(i, size, first=0):
    return pl.ds(pl.multiple_of(i * size + first, min(size, ROWS)), size)


def lane_block(i, size):
    return pl.ds(i * size if isinstance(i, int) else pl.multiple_of(i * size, size), size)


def row_loop(n_rows, fn, size=ROWS):
    def step(i, carry):
        fn(i)
        return carry
    lax.fori_loop(0, n_rows // size, step, None)


def row_sum(value):
    return jnp.sum(value, axis=-1, keepdims=True)


def row_mean(value):
    return jnp.mean(value, axis=-1, keepdims=True)


class Exchange:
    def __init__(self, send, recv):
        self.send, self.recv = send, recv

    def remote(self, i, src, dst, target):
        return pltpu.make_async_remote_copy(src_ref=src, dst_ref=dst, send_sem=self.send.at[i], recv_sem=self.recv.at[i],
                                            device_id=target, device_id_type=MESH)

    def landing(self):
        return [dst for _, dst, _ in self.copies()]

    def start(self, *which):
        table = self.copies()
        for i in which:
            self.remote(i, *table[i]).start()

    def arrived(self, *which):
        places, table = self.landing(), self.copies()
        for i in which:
            _, _, target = table[i]
            self.remote(i, places[i], places[i], target).wait_recv()

    def sent(self, *which):
        table = self.copies()
        for i in which or range(len(table)):
            self.remote(i, *table[i]).wait_send()


class Gather(Exchange):
    OTHER, UP, DOWN, PASS_UP, PASS_DOWN, PREV_OTHER, NEXT_OTHER, FAR_UP_OTHER, FAR_DOWN_OTHER = COPIES = range(9)

    def __init__(self, src, out, send, recv, local):
        super().__init__(send, recv)
        self.src, self.out, self.local = src, out, local
        self.x, self.c = model_place()
        self.pos, _ = src.shape
        self.half = self.pos // 2

    def block(self, distance, core):
        return self.out.at[row_block(2 * go(self.x, distance) + core, self.pos)]

    def part(self, distance, core, lower):
        place = 2 * go(self.x, distance) + core
        return self.out.at[row_block(2 * place + lower, self.half)]

    def copies(self):
        c = self.c
        other, nxt, prv = chip_targets()
        own = self.block(HERE, c)
        parts = [self.part(PREV, c, False), self.part(NEXT, c, True), self.block(PREV, c), self.block(NEXT, c),
                 self.part(FAR, c, False), self.part(FAR, c, True)]
        return [(self.src, own, other), (self.src, own, nxt), (self.src, own, prv)] + [
            (part, part, to) for part, to in zip(parts, (nxt, prv, other, other, other, other))]

    def landing(self):
        c, o = self.c, 1 - self.c
        return [self.block(HERE, o), self.block(PREV, c), self.block(NEXT, c), self.part(FAR, c, False),
                self.part(FAR, c, True), self.block(PREV, o), self.block(NEXT, o), self.part(FAR, o, False),
                self.part(FAR, o, True)]

    def own_copy(self):
        return pltpu.make_async_copy(self.src, self.block(HERE, self.c), self.local)

    def begin(self):
        if self.local is not None:
            self.own_copy().start()
        self.start(self.UP, self.DOWN, self.OTHER)

    def pass_near(self):
        self.arrived(self.UP)
        self.start(self.PASS_UP, self.PREV_OTHER)
        self.arrived(self.DOWN)
        self.start(self.PASS_DOWN, self.NEXT_OTHER)

    def pass_far(self):
        self.arrived(self.PASS_UP)
        self.start(self.FAR_UP_OTHER)
        self.arrived(self.PASS_DOWN)
        self.start(self.FAR_DOWN_OTHER)

    def complete(self):
        self.arrived(self.OTHER, self.PREV_OTHER, self.NEXT_OTHER, self.FAR_UP_OTHER, self.FAR_DOWN_OTHER)
        if self.local is not None:
            self.own_copy().wait()

    @classmethod
    def sems(cls, n):
        return [DMA((n, len(cls.COPIES))), DMA((n, len(cls.COPIES))), DMA((n,))]

    @classmethod
    def of(cls, i, src, out, sems, local=True):
        send, recv, local_sem = sems
        return cls(src, out, send.at[i], recv.at[i], local_sem.at[i] if local else None)


class RingGather(Exchange):
    UP, DOWN, PASS_UP, PASS_DOWN = COPIES = range(4)

    def __init__(self, src, at, targets, send, recv):
        super().__init__(send, recv)
        self.src, self.at, self.targets = src, at, targets
        rows, _ = src.shape
        self.upper, self.lower = row_block(0, rows // 2), row_block(1, rows // 2)

    def copies(self):
        nxt, prv = self.targets
        own, up, low = self.at(HERE), self.at(PREV).at[self.upper], self.at(NEXT).at[self.lower]
        return [(self.src, own, nxt), (self.src, own, prv), (up, up, nxt), (low, low, prv)]

    def landing(self):
        far = self.at(FAR)
        return [self.at(PREV), self.at(NEXT), far.at[self.upper], far.at[self.lower]]

    def begin(self):
        self.start(self.UP, self.DOWN)

    def pass_near(self):
        self.arrived(self.UP)
        self.start(self.PASS_UP)
        self.arrived(self.DOWN)
        self.start(self.PASS_DOWN)

    def far(self):
        self.arrived(self.PASS_UP, self.PASS_DOWN)


class WeightGather:
    def __init__(self, src, out, send, recv, local, first_row=0):
        self.src, self.out, self.local, self.first_row = src, out, local, first_row
        z, y = fsdp_place()
        self.place = RING * z + y
        self.rows, _ = src.shape
        half = self.rows // 2
        depth, _ = out.shape
        self.block = depth // RING ** 2
        targets = plane_targets()
        self.first, self.second = [], []
        for color, (one, two) in enumerate(('yz', 'zy')):
            part = src.at[row_block(color, half)]

            def at(d_one, d_two, one=one, color=color):
                dz, dy = (d_two, d_one) if one == 'y' else (d_one, d_two)
                first = (RING * go(z, dz) + go(y, dy)) * self.block + first_row + color * half
                return out.at[pl.ds(pl.multiple_of(first, ROWS), half)]
            self.first.append(RingGather(part, functools.partial(lambda at, d: at(d, HERE), at), targets[one],
                                         send.at[color, RING], recv.at[color, RING]))
            self.second.append([RingGather(at(d, HERE) if d else part, functools.partial(at, d), targets[two],
                                           send.at[color, d], recv.at[color, d]) for d in range(RING)])

    @staticmethod
    def sems(n):
        dims = (n, len(COLORS), RING + 1, len(RingGather.COPIES))
        return [DMA(dims), DMA(dims), DMA((n,))]

    @classmethod
    def of(cls, i, src, out, sems, local=True, first_row=0):
        send, recv, local_sem = sems
        return cls(src, out, send.at[i], recv.at[i], local_sem.at[i] if local else None, first_row)

    def own_rows(self):
        return pl.ds(pl.multiple_of(self.place * self.block + self.first_row, ROWS), self.rows)

    def own_copy(self):
        return pltpu.make_async_copy(self.src, self.out.at[self.own_rows()], self.local)

    def begin(self):
        if self.local is not None:
            self.own_copy().start()
        for ring in self.first:
            ring.begin()
        for rings in self.second:
            rings[HERE].begin()

    def pass_near(self):
        for one, two in zip(self.first, self.second):
            one.arrived(one.UP)
            one.start(one.PASS_UP)
            two[PREV].begin()
        for one, two in zip(self.first, self.second):
            one.arrived(one.DOWN)
            one.start(one.PASS_DOWN)
            two[NEXT].begin()
        self.pass_second(HERE)

    def pass_far(self):
        for one, two in zip(self.first, self.second):
            one.far()
            two[FAR].begin()

    def pass_second(self, d):
        for rings in self.second:
            rings[d].pass_near()

    def complete(self):
        for rings in self.second:
            for ring in rings:
                ring.far()
        if self.local is not None:
            self.own_copy().wait()

    def sent(self):
        for ring in self.first + sum(self.second, []):
            ring.sent()


class RingScatter(Exchange):
    FAR_UP, FAR_DOWN, UP_HI, DOWN_LO, UP_LO, DOWN_HI = COPIES = range(6)

    def __init__(self, mine, far, near, lo, hi, targets, send, recv):
        super().__init__(send, recv)
        self.mine, self.far, self.near, self.lo, self.hi, self.targets = mine, far, near, lo, hi, targets

    def copies(self):
        nxt, prv = self.targets
        far, up, down = (self.mine.at[BY_RANK.index(d)] for d in (FAR, NEXT, PREV))
        from_prv, from_nxt = self.near.at[0], self.near.at[1]
        lo, hi = self.lo, self.hi
        return [(far.at[lo], self.far.at[0], nxt), (far.at[hi], self.far.at[1], prv),
                (up.at[hi], from_prv.at[hi], nxt), (down.at[lo], from_nxt.at[lo], prv),
                (up.at[lo], from_prv.at[lo], nxt), (down.at[hi], from_nxt.at[hi], prv)]

    def begin(self):
        self.start(self.FAR_UP, self.FAR_DOWN, self.UP_HI, self.DOWN_LO)

    def add_far(self, add):
        up, down = (self.mine.at[BY_RANK.index(d)] for d in (NEXT, PREV))
        self.arrived(self.FAR_UP)
        add(up.at[self.lo], self.far.at[0])
        self.start(self.UP_LO)
        self.arrived(self.FAR_DOWN)
        add(down.at[self.hi], self.far.at[1])
        self.start(self.DOWN_HI)

    def arrive(self):
        self.arrived(self.UP_HI, self.DOWN_LO, self.UP_LO, self.DOWN_HI)

    def total(self, *at):
        return self.mine[(BY_RANK.index(HERE), *at)] + self.near[(0, *at)] + self.near[(1, *at)]


def add_rows(place, value):
    *outer, rows, _ = place.shape
    for at in [(i,) for i in range(*outer)] if outer else [()]:
        def add(i, at=at):
            place[(*at, row_block(i, ROWS))] += value[(*at, row_block(i, ROWS))]
        row_loop(rows, add)


class Scatter(Exchange):
    CHUNKS = 4

    def __init__(self, rows_of, weight, fetches, before, box, pair, mine, far, near, send, recv):
        super().__init__(send, recv)
        self.rows_of, self.weight, self.fetches, self.before = rows_of, weight, fetches, before
        self.box, self.pair, self.mine = box, pair, mine
        self.x, self.c = model_place()
        _, self.rows, self.width = mine.shape
        _, *ring_targets = chip_targets()
        half = self.width // 2
        rows = slice(None)
        ring_sems = (sem.at[pl.ds(RING, len(RingScatter.COPIES))] for sem in (send, recv))
        self.ring = RingScatter(mine, far, near, (rows, lane_block(0, half)), (rows, lane_block(1, half)), ring_targets,
                                *ring_sems)

    def copies(self):
        other, _, _ = chip_targets()
        return [(self.box.at[k], self.pair.at[k], other) for k in range(RING)]

    def pass_on(self, k):
        if self.before is not None:
            self.before.sent(k)
        chip = 2 * go(self.x, BY_RANK[k])
        left = jnp.concatenate([self.rows_of(chip + self.c), self.rows_of(chip + 1 - self.c)], axis=0)
        step = self.width // self.CHUNKS

        def chunk(i):
            if not k and self.fetches:
                for copy in self.fetches(i):
                    copy.wait()
            cols = lane_block(i, step)
            both = lax.dot_general(left, self.weight[cols, :], NT, preferred_element_type=F32)
            self.box[k, :, cols] = both[self.rows:]
            self.mine[k, :, cols] = both[:self.rows]
        row_loop(self.CHUNKS, chunk, 1)
        self.start(k)

    def pair_sum(self, k):
        self.arrived(k)
        add_rows(self.mine.at[k], self.pair.at[k])

    def send_near(self):
        far, up, down, here = range(RING)
        self.pass_on(far)
        self.pass_on(up)
        self.pair_sum(far)
        self.ring.start(RingScatter.FAR_UP, RingScatter.FAR_DOWN)
        self.pass_on(down)
        self.pair_sum(up)
        self.ring.start(RingScatter.UP_HI)
        self.pass_on(here)
        self.pair_sum(down)
        self.ring.start(RingScatter.DOWN_LO)

    def send_far(self):
        self.ring.add_far(add_rows)

    def arrive(self):
        self.pair_sum(BY_RANK.index(HERE))
        self.ring.arrive()

    def total(self, rows):
        return self.ring.total(rows)

    N_SCRATCH = 7

    @classmethod
    def scratch(cls, units, pos, width):
        sems = DMA((units, RING + len(RingScatter.COPIES)))
        return [pltpu.VMEM((RING, pos, width), F32), pltpu.VMEM((units, RING, pos, width), F32),
                pltpu.VMEM((units, RING, pos, width), F32), pltpu.VMEM((units, 2, pos, width // 2), F32),
                pltpu.VMEM((units, 2, pos, width), F32), sems, sems]

    @classmethod
    def all_of(cls, left, weight, fetches, scratch):
        box, *rest = scratch
        _, pos, _ = box.shape
        units, before = [], None
        n_seq, _, _ = left.shape
        for s in range(n_seq):
            def rows_of(place, s=s):
                return left[s, row_block(place, pos), :]
            before = cls(rows_of, weight, None if units else fetches, before, box, *(ref.at[s] for ref in rest))
            units.append(before)
        return units

    @staticmethod
    def all_sent(units):
        for unit in units:
            unit.ring.sent()
        unit.sent()


class GradScatter:
    N_SCRATCH = 9

    def __init__(self, part, out, mine1, far1, near1, mine2, far2, near2, send, recv, load):
        self.part, self.out, self.load, self.mine1, self.mine2 = part, out, load, mine1, mine2
        self.z, self.y = fsdp_place()
        rows, _ = out.shape
        self.half = rows // 2
        quarter = self.half // 2
        targets = plane_targets()
        self.one, self.two = [], []
        for color, (one, two) in enumerate(('yz', 'zy')):
            self.one.append(RingScatter(mine1.at[color], far1.at[color], near1.at[color], pl.ds(0, RING // 2),
                                        pl.ds(RING // 2, RING // 2), targets[one], send.at[color, 0], recv.at[color, 0]))
            self.two.append(RingScatter(mine2.at[color], far2.at[color], near2.at[color], row_block(0, quarter),
                                        row_block(1, quarter), targets[two], send.at[color, 1], recv.at[color, 1]))

    @staticmethod
    def scratch(rows, cols):
        half, n = rows // 2, len(COLORS)
        sems = DMA((n, 2, len(RingScatter.COPIES)))
        return [pltpu.VMEM((n, RING, RING, half, cols), F32), pltpu.VMEM((n, 2, RING // 2, half, cols), F32),
                pltpu.VMEM((n, 2, RING, half, cols), F32), pltpu.VMEM((n, RING, half, cols), F32),
                pltpu.VMEM((n, 2, half // 2, cols), F32), pltpu.VMEM((n, 2, half, cols), F32), sems, sems,
                DMA((n, RING, RING))]

    def loads(self):
        for color in COLORS:
            for k, d_one in enumerate(BY_RANK):
                for j, d_two in enumerate(BY_RANK):
                    dz, dy = (d_one, d_two) if color else (d_two, d_one)
                    place = RING * go(self.z, dz) + go(self.y, dy)
                    yield pltpu.make_async_copy(self.part.at[row_block(2 * place + color, self.half)],
                                                self.mine1.at[color, k, j], self.load.at[color, k, j])

    def fetch(self):
        for load in self.loads():
            load.start()

    def put(self, place, value):
        def rank(there, here):
            distance = (there + RING - here) % RING
            found = BY_RANK.index(HERE)
            for d in (NEXT, FAR, PREV):
                found = jnp.where(distance == d, BY_RANK.index(d), found)
            return found
        dz, dy = rank(place // RING, self.z), rank(place % RING, self.y)
        for color, at in enumerate(((dy, dz), (dz, dy))):
            self.mine1[(color, *at)] = value[color * self.half:(color + 1) * self.half]

    def begin(self):
        if self.part is not None:
            for load in self.loads():
                load.wait()
        for ring in self.one:
            ring.begin()

    def one_far(self):
        for ring in self.one:
            ring.add_far(add_rows)

    def one_done(self):
        for color, (one, two) in enumerate(zip(self.one, self.two)):
            one.arrive()
            for j in range(RING):
                def add(i, j=j):
                    rows = row_block(i, ROWS)
                    self.mine2[color, j, rows, :] = one.total(j, rows)
                row_loop(self.half, add)
            two.begin()

    def two_far(self):
        for ring in self.two:
            ring.add_far(add_rows)

    def two_done(self):
        for color, ring in enumerate(self.two):
            ring.arrive()

            def add(i):
                self.out[row_block(i, ROWS, color * self.half), :] = ring.total(row_block(i, ROWS))
            row_loop(self.half, add)

    def sent(self):
        for ring in self.one + self.two:
            ring.sent()


class GainSum:
    STAGES = 4

    def __init__(self, total, slots, send, recv):
        self.total, self.slots, self.send, self.recv = total, slots, send, recv
        (x, c), (z, y) = model_place(), fsdp_place()
        away = (NEXT, FAR, PREV)
        self.places = [c, x, y, z]
        self.targets = [[{'model': 2 * x + 1 - c}], [{'model': 2 * go(x, d) + c} for d in away],
                        [{'fsdp': RING * z + go(y, d)} for d in away], [{'fsdp': RING * go(z, d) + y} for d in away]]

    @classmethod
    def scratch(cls, *shape):
        dims = (cls.STAGES, RING - 1)
        return [pltpu.VMEM((cls.STAGES + 1, *shape), F32), pltpu.VMEM((*dims, *shape), F32), DMA(dims), DMA(dims)]

    def copies(self, t):
        return [pltpu.make_async_remote_copy(
            src_ref=self.total.at[t], dst_ref=self.slots.at[t, d], send_sem=self.send.at[t, d],
            recv_sem=self.recv.at[t, d], device_id=target, device_id_type=MESH)
            for d, target in enumerate(self.targets[t])]

    def start(self, t):
        for copy in self.copies(t):
            copy.start()

    def advance(self, t):
        others = len(self.targets[t])
        n = others + 1
        for copy in self.copies(t):
            copy.wait_recv()
        acc = None
        for i in range(n):
            term = self.total[t]
            for d in range(others):
                term = jnp.where((self.places[t] + others - d) % n == i, self.slots[t, d], term)
            acc = term if acc is None else acc + term
        self.total[t + 1] = acc
        if t + 1 < self.STAGES:
            self.start(t + 1)

    def sent(self):
        for t in range(self.STAGES):
            for copy in self.copies(t):
                copy.wait_send()


def norm_rows(x_f32, gain):
    return x_f32 * lax.rsqrt(row_mean(x_f32 * x_f32) + NORM_EPS) * gain


def norm_rows_back(x_f32, gain, cotangent):
    inv_rms = lax.rsqrt(row_mean(x_f32 * x_f32) + NORM_EPS)
    x_hat = x_f32 * inv_rms
    scaled = cotangent * gain
    return inv_rms * (scaled - x_hat * row_mean(scaled * x_hat)), cotangent * x_hat


def fold_row(row, out):
    rows, step = out.shape
    for i in range(rows):
        out[i:i + 1, :] = row[:, i * step:(i + 1) * step]


def unfold_row(rows_ref, out):
    rows, step = rows_ref.shape
    for i in range(rows):
        out[:, i * step:(i + 1) * step] = rows_ref[i:i + 1, :]


def rope_tables(cos_ref, sin_ref, cos_t, sin_t):
    cos, sin = cos_ref[...].T, sin_ref[...].T
    cos_t[...] = jnp.concatenate([cos, cos], axis=1)
    sin_t[...] = jnp.concatenate([-sin, sin], axis=1)


def spin(tensor, cos_t, sin_t):
    _, lanes = tensor.shape
    return tensor * cos_t + pltpu.roll(tensor, lanes // 2, 1) * sin_t


def probs(query, key, scale, first_row):
    scores = lax.dot_general(query, key, NT, preferred_element_type=F32) * scale
    rows, cols = (lax.broadcasted_iota(jnp.int32, scores.shape, dim) for dim in range(scores.ndim))
    scores = jnp.where(first_row + rows >= cols, scores, MASKED)
    expd = jnp.exp(scores - jnp.max(scores, axis=-1, keepdims=True))
    return expd / row_sum(expd)


def piece_of(refs, j, out):
    _, cols = out.shape
    step = cols // len(refs)
    for i, ref in enumerate(refs):
        out[:, lane_block(i, step)] = ref[:, lane_block(j, step)]


def fetch_weight(sources, w_vmem, sem):
    depth, _ = w_vmem.shape
    step = depth // Scatter.CHUNKS

    def chunk(i):
        rows, col, copies = row_block(i, step), 0, []
        for n, (ref, first, size) in enumerate(sources):
            copies.append(pltpu.make_async_copy(ref.at[rows, pl.ds(first, size)], w_vmem.at[rows, pl.ds(col, size)],
                                                sem.at[i, n]))
            col += size
        return copies
    for i in range(Scatter.CHUNKS):
        for copy in chunk(i):
            copy.start()
    return chunk


def piece_columns(pieces, first, size):
    return [(pieces.at[i], first, size) for i in range(PIECES)]


def early_rows(shard_rows):
    return 2 * shard_rows // 3


def first_kernel(heads, group, scale, x_ref, dy_ref, gain_ref, wqkv_src, wout_src, wg_ref, wu_ref, wd_ref, cos_ref, sin_ref,
                 h_out, dy_out, wqkv_out, wout_out, pieces_out, qkv_ref, attn_ref,
                 h_src, h_buf, w_buf, piece_src, cos_t, sin_t, flush, *sems):
    targets = chip_and_plane()
    greet(targets)
    n_seq, pos, _ = x_ref.shape
    seq, head_dim = cos_t.shape
    block = seq // 2
    _, cols = w_buf.shape
    x, c = model_place()
    mine = row_block(2 * x + c, pos)
    for s in range(n_seq):
        def norm(i, s=s):
            rows = row_block(i, ROWS)
            h_src[s, rows, :] = norm_rows(x_ref[s, rows, :].astype(F32), gain_ref[...]).astype(BF16)
        row_loop(pos, norm)
    g_sems, w_sems = sems[:3], sems[3:]
    w_qkv = WeightGather.of(0, wqkv_src, w_buf, w_sems[:3], local=False)
    w_out = WeightGather.of(0, wout_src, wout_out, w_sems[3:6])
    shard_rows, _ = wqkv_src.shape
    early = early_rows(shard_rows)
    piece = WeightGather.of(0, piece_src.at[pl.ds(0, early)], pieces_out.at[0], w_sems[6:])
    h0, h1 = (Gather.of(s, h_src.at[s], h_buf.at[s], g_sems, local=False) for s in range(n_seq))
    dy0, dy1 = (Gather.of(n_seq + s, dy_ref.at[s], dy_out.at[s], g_sems) for s in range(n_seq))
    met(targets)
    w_qkv.begin()
    h0.begin()
    h1.begin()
    piece_of((wg_ref, wu_ref, wd_ref), 0, piece_src)
    rope_tables(cos_ref, sin_ref, cos_t, sin_t)
    for s in range(n_seq):
        h_buf[s, mine, :] = h_src[s]
    w_buf[w_qkv.own_rows(), :] = wqkv_src[...]
    w_qkv.pass_near()
    h0.pass_near()
    w_qkv.pass_far()
    w_qkv.pass_second(PREV)
    w_qkv.pass_second(NEXT)
    w_out.begin()
    h1.pass_near()
    dy0.begin()
    w_qkv.pass_second(FAR)
    h0.pass_far()
    w_out.pass_near()
    w_qkv.complete()
    w_flush = pltpu.make_async_copy(w_buf, wqkv_out, flush.at[n_seq])
    w_flush.start()

    def lanes(i):
        return lane_block(i, head_dim)

    def project(s):
        def one_block(i):
            rows = row_block(i, block)
            qkv = jnp.dot(h_buf[s, rows, :], w_buf[...], preferred_element_type=F32)
            for j in range(cols // head_dim):
                one = qkv[:, j * head_dim:(j + 1) * head_dim]
                if j % (group + 2) <= group:
                    one = spin(one, cos_t[rows, :], sin_t[rows, :])
                qkv_ref[s, rows, lanes(j)] = one.astype(BF16)
        row_loop(seq, one_block, block)

    def attend(s):
        for g in range(heads // group):
            first = g * (group + 2)

            def head(j, first=first, g=g):
                for i in range(seq // block):
                    rows, keys = pl.ds(i * block, block), pl.ds(0, (i + 1) * block)
                    key, value = qkv_ref[s, keys, lanes(first + group)], qkv_ref[s, keys, lanes(first + group + 1)]
                    prob = probs(qkv_ref[s, rows, lanes(first + j)], key, scale, i * block)
                    attn_ref[s, rows, lanes(g * group + j)] = jnp.dot(
                        prob.astype(BF16), value, preferred_element_type=F32).astype(BF16)
            row_loop(group, head, 1)

    def h_flush(s):
        return pltpu.make_async_copy(h_buf.at[s], h_out.at[s], flush.at[s])

    h0.complete()
    h_flush(0).start()
    project(0)
    w_out.pass_far()
    h1.pass_far()
    dy1.begin()
    w_out.pass_second(PREV)
    w_out.pass_second(NEXT)
    piece.begin()
    attend(0)
    w_out.pass_second(FAR)
    dy0.pass_near()
    piece.pass_near()
    h1.complete()
    h_flush(1).start()
    project(1)
    piece.pass_far()
    piece.pass_second(PREV)
    dy0.pass_far()
    piece.pass_second(NEXT)
    dy1.pass_near()
    attend(1)
    piece.pass_second(FAR)
    dy1.pass_far()
    for each in (dy0, dy1, w_out, piece):
        each.complete()
    for each in (h0, h1, dy0, dy1, w_qkv, w_out, piece):
        each.sent()
    w_flush.wait()
    for s in range(n_seq):
        h_flush(s).wait()


def second_kernel(left, wout_hbm, base_ref, gain_ref, dy_hbm, wg_ref, wu_ref, wd_ref, pieces_in, mid_ref, h_out, act_ref,
                  dgu_ref, pieces_out, *scratch):
    targets = chip_and_plane()
    greet(targets)
    n_seq, pos, _ = base_ref.shape
    rs_scratch, scratch = scratch[:Scatter.N_SCRATCH], scratch[Scatter.N_SCRATCH:]
    wo_vmem, wo_sem, g_src, h_buf, dy_buf, dy_sem, w_bufs, w_sem, piece_src, flush, *scratch = scratch
    g_sems, p_sems = scratch[:3], scratch[3:]
    _, seq, _ = h_buf.shape
    block = seq // 2
    _, out_rows = wo_vmem.shape
    _, _, cols = w_bufs.shape
    step = cols // 3
    fetches = fetch_weight([(wout_hbm, 0, out_rows)], wo_vmem, wo_sem)
    shard_rows, _ = wg_ref.shape
    pieces = []
    for j in range(PIECES):
        piece_of((wg_ref, wu_ref, wd_ref), j, piece_src.at[j])
        early = 0 if j else early_rows(shard_rows)
        pieces.append(WeightGather.of(j, piece_src.at[j, pl.ds(early, shard_rows - early)], pieces_out.at[j], p_sems,
                                      first_row=early))
    p0, p1, p2, p3 = pieces
    x, c = model_place()
    mine = row_block(2 * x + c, pos)
    units = Scatter.all_of(left, wo_vmem, fetches, rs_scratch)
    u0, u1 = units
    h0, h1 = gathers = [Gather.of(s, g_src.at[s], h_buf.at[s], g_sems, local=False) for s in range(n_seq)]

    def settle(s, unit, gather):
        unit.arrive()

        def rows_fn(i):
            rows = row_block(i, ROWS)
            red = unit.total(rows).astype(BF16).astype(F32)
            mid = (base_ref[s, rows, :].astype(F32) + red).astype(BF16)
            mid_ref[s, rows, :] = mid
            g_src[s, rows, :] = norm_rows(mid.astype(F32), gain_ref[...]).astype(BF16)
        row_loop(pos, rows_fn)
        gather.begin()
        h_buf[s, mine, :] = g_src[s]

    def load_dy(s):
        return pltpu.make_async_copy(dy_hbm.at[s], dy_buf, dy_sem)

    def load_piece(t):
        return pltpu.make_async_copy(pieces_out.at[t % PIECES], w_bufs.at[t % 2], w_sem.at[t % 2])

    def h_flush(s):
        return pltpu.make_async_copy(h_buf.at[s], h_out.at[s], flush.at[s])

    def before_second():
        h1.pass_near()
        p3.pass_second(NEXT)
        p2.complete()

    def before_third():
        p3.pass_second(FAR)
        h1.pass_far()
        p3.complete()

    def before_next_sequence():
        load_dy(1).start()
        h1.complete()
        h_flush(1).start()
        load_dy(1).wait()

    def mlp(t):
        s, j, slot = t // PIECES, t % PIECES, t % 2
        for at, fn in {1: before_second, 2: before_third, PIECES: before_next_sequence}.items():
            pl.when(t == at)(fn)
        load_piece(t).wait()

        @pl.when(t + 1 < n_seq * PIECES)
        def _():
            load_piece(t + 1).start()

        def rows_fn(i):
            rows, there = row_block(i, block), row_block(i, block, s * seq)
            gate = jnp.dot(h_buf[s, rows, :], w_bufs[slot, :, :step], preferred_element_type=F32)
            up_proj = jnp.dot(h_buf[s, rows, :], w_bufs[slot, :, step:2 * step], preferred_element_type=F32)
            d_act = jnp.dot(dy_buf[rows, :], w_bufs[slot, :, 2 * step:],
                            preferred_element_type=F32).astype(BF16).astype(F32)
            sig_gate = jax.nn.sigmoid(gate)
            silu_gate = gate * sig_gate
            act_ref[there, lane_block(j, step)] = (silu_gate * up_proj).astype(BF16)
            dgu_ref[there, lane_block(2 * j, step)] = (
                d_act * up_proj * sig_gate * (1.0 + gate * (1.0 - sig_gate))).astype(BF16)
            dgu_ref[there, lane_block(2 * j + 1, step)] = (d_act * silu_gate).astype(BF16)
        row_loop(seq, rows_fn, block)

    load_dy(0).start()
    met(targets)
    p0.begin()
    p1.begin()
    u0.send_near()
    p0.pass_near()
    p1.pass_near()
    u0.send_far()
    p0.pass_far()
    p1.pass_far()
    p2.begin()
    p0.pass_second(PREV)
    p1.pass_second(PREV)
    u1.send_near()
    p0.pass_second(NEXT)
    p1.pass_second(NEXT)
    p0.pass_second(FAR)
    p2.pass_near()
    settle(0, u0, h0)
    u1.send_far()
    p1.pass_second(FAR)
    p2.pass_far()
    p3.begin()
    p2.pass_second(PREV)
    h0.pass_near()
    p2.pass_second(NEXT)
    p3.pass_near()
    p0.complete()
    load_piece(0).start()
    settle(1, u1, h1)
    h0.pass_far()
    p2.pass_second(FAR)
    p3.pass_far()
    p3.pass_second(PREV)
    p1.complete()
    h0.complete()
    h_flush(0).start()
    load_dy(0).wait()
    row_loop(n_seq * PIECES, mlp, 1)
    Scatter.all_sent(units)
    for each in gathers + pieces:
        each.sent()
    for s in range(n_seq):
        h_flush(s).wait()


def back_kernel(left, pieces, base_ref, mid_ref, gain_ref, res_ref, full_out, dgain_ref, *scratch):
    targets = chip_targets()
    greet(targets)
    n_seq, pos, _ = base_ref.shape
    rs_scratch, scratch = scratch[:Scatter.N_SCRATCH], scratch[Scatter.N_SCRATCH:]
    w_vmem, w_sem, g_src, sums, *sems = scratch
    _, depth = w_vmem.shape
    fetches = fetch_weight(piece_columns(pieces, 0, depth // PIECES), w_vmem, w_sem)
    units = Scatter.all_of(left, w_vmem, fetches, rs_scratch)
    u0, u1 = units
    g0, g1 = gathers = [Gather.of(s, g_src.at[s], full_out.at[s], sems) for s in range(n_seq)]
    sums[...] = jnp.zeros_like(sums)

    def settle(s, unit, gather):
        unit.arrive()

        def rows_fn(i):
            rows = row_block(i, ROWS)
            red = unit.total(rows).astype(BF16).astype(F32)
            d_norm, d_gain = norm_rows_back(mid_ref[s, rows, :].astype(F32), gain_ref[...], red)
            out = (base_ref[s, rows, :].astype(F32) + d_norm).astype(BF16)
            sums[...] += d_gain
            res_ref[s, rows, :] = out
            g_src[s, rows, :] = out
        row_loop(pos, rows_fn)
        gather.begin()

    met(targets)
    u0.send_near()
    u0.send_far()
    u1.send_near()
    settle(0, u0, g0)
    u1.send_far()
    g0.pass_near()
    settle(1, u1, g1)
    g0.pass_far()
    g1.pass_near()
    g1.pass_far()
    fold_row(jnp.sum(sums[...], axis=0, keepdims=True), dgain_ref)
    for gather in gathers:
        gather.complete()
    Scatter.all_sent(units)
    for gather in gathers:
        gather.sent()


def attn_back_kernel(heads, group, scale, dm_hbm, wo_hbm, h_hbm, left, pieces, rope_cos, rope_sin, qkv_ref, attn_ref, mid_ref,
                     dqkv_ref, dwqkv_out, y_ref, dwout_ref, *scratch):
    targets = chip_and_plane()
    greet(targets)
    _, pos, width = mid_ref.shape
    half_dim, seq = rope_cos.shape
    head_dim = 2 * half_dim
    block = seq // 2
    rs_scratch, scratch = scratch[:Scatter.N_SCRATCH], scratch[Scatter.N_SCRATCH:]
    grads = GradScatter(None, dwout_ref, *scratch[:GradScatter.N_SCRATCH])
    (wd_vmem, wd_sem, dm_ref, wo_ref, in_sem, h_buf, h_sem, dw_buf, dw_sem, do_ref, dk_ref, dv_ref, cos_ref,
     sin_ref) = scratch[GradScatter.N_SCRATCH:]
    _, ff = wd_vmem.shape
    piece_cols = ff // PIECES
    fetches = fetch_weight(piece_columns(pieces, 2 * piece_cols, piece_cols), wd_vmem, wd_sem)
    dm_copy = pltpu.make_async_copy(dm_hbm, dm_ref, in_sem.at[0])
    wo_copy = pltpu.make_async_copy(wo_hbm, wo_ref, in_sem.at[1])
    dm_copy.start()
    wo_copy.start()
    _, _, h_cols = h_buf.shape
    n_blocks = width // h_cols

    def h_copy(i):
        return pltpu.make_async_copy(h_hbm.at[:, lane_block(i, h_cols)], h_buf.at[i % 2], h_sem.at[i % 2])

    def dw_copy(i):
        return pltpu.make_async_copy(dw_buf.at[i % 2], dwqkv_out.at[row_block(i, h_cols)], dw_sem.at[i % 2])
    h_copy(0).start()
    rope_tables(rope_cos, rope_sin, cos_ref, sin_ref)
    units = Scatter.all_of(left, wd_vmem, fetches, rs_scratch)
    u0, u1 = units

    def settle(s, unit):
        unit.arrive()

        def rows_fn(i):
            rows = row_block(i, ROWS)
            red = unit.total(rows).astype(BF16).astype(F32)
            y_ref[s, rows, :] = (mid_ref[s, rows, :].astype(F32) + red).astype(BF16)
        row_loop(pos, rows_fn)

    def out_grads():
        shard, _ = dwout_ref.shape

        def two_places(i):
            both = lax.dot_general(dm_ref[:, lane_block(i, 2 * shard)], attn_ref[...], TN, preferred_element_type=F32)
            grads.put(2 * i, both[:shard])
            grads.put(2 * i + 1, both[shard:])
        row_loop(width, two_places, 2 * shard)

    def lanes(i):
        return lane_block(i, head_dim)

    def attention(s):
        base = s * seq

        def project(i):
            do_ref[row_block(i, block), :] = jnp.dot(dm_ref[row_block(i, block, base), :], wo_ref[...],
                                                     preferred_element_type=F32).astype(BF16)
        row_loop(seq, project, block)
        for g in range(heads // group):
            first = g * (group + 2)
            dk_ref[...] = jnp.zeros_like(dk_ref)
            dv_ref[...] = jnp.zeros_like(dv_ref)
            for i in range(seq // block):
                rows, keys = pl.ds(i * block, block), pl.ds(0, (i + 1) * block)
                g_rows, g_keys = pl.ds(base + i * block, block), pl.ds(base, (i + 1) * block)
                key, value = qkv_ref[g_keys, lanes(first + group)], qkv_ref[g_keys, lanes(first + group + 1)]

                def head(j, rows=rows, keys=keys, g_rows=g_rows, key=key, value=value, first=first, g=g, i=i):
                    query = qkv_ref[g_rows, lanes(first + j)]
                    d_out = do_ref[rows, lanes(g * group + j)]
                    prob = probs(query, key, scale, i * block)
                    d_prob = lax.dot_general(d_out, value, NT, preferred_element_type=F32)
                    d_scores = (prob * (d_prob - row_sum(d_prob * prob)) * scale).astype(BF16)
                    d_query = jnp.dot(d_scores, key, preferred_element_type=F32)
                    dqkv_ref[g_rows, lanes(first + j)] = spin(d_query, cos_ref[rows, :], -sin_ref[rows, :]).astype(BF16)
                    dk_ref[keys, :] += lax.dot_general(d_scores, query, TN, preferred_element_type=F32)
                    dv_ref[keys, :] += lax.dot_general(prob.astype(BF16), d_out, TN, preferred_element_type=F32)
                row_loop(group, head, 1)
            every = pl.ds(base, seq)
            dqkv_ref[every, lanes(first + group)] = spin(dk_ref[...], cos_ref[...], -sin_ref[...]).astype(BF16)
            dqkv_ref[every, lanes(first + group + 1)] = dv_ref[...].astype(BF16)

    def qkv_grads():
        def one_block(i):
            @pl.when(i + 1 < n_blocks)
            def _():
                h_copy(i + 1).start()
            h_copy(i).wait()

            @pl.when(i >= 2)
            def _():
                dw_copy(i - 2).wait()
            dw_buf[i % 2] = lax.dot_general(h_buf[i % 2], dqkv_ref[...], TN, preferred_element_type=F32)
            dw_copy(i).start()
        row_loop(n_blocks, one_block, 1)

    met(targets)
    u0.send_near()
    dm_copy.wait()
    out_grads()
    grads.begin()
    u0.send_far()
    u1.send_near()
    wo_copy.wait()
    attention(0)
    u1.send_far()
    grads.one_far()
    settle(0, u0)
    attention(1)
    grads.one_done()
    qkv_grads()
    settle(1, u1)
    grads.two_far()
    grads.two_done()
    for i in (n_blocks - 2, n_blocks - 1):
        dw_copy(i).wait()
    Scatter.all_sent(units)
    grads.sent()


def leave_kernel(left, w_hbm, base_ref, x_ref, gain_ref, grad_hbm, dgm_ref, res_ref, grad_ref, ga_ref, gm_ref, *scratch):
    _, pos, _ = base_ref.shape
    rs_scratch, scratch = scratch[:Scatter.N_SCRATCH], scratch[Scatter.N_SCRATCH:]
    grads = GradScatter(grad_hbm, grad_ref, *scratch[:GradScatter.N_SCRATCH])
    w_vmem, w_sem, sums, *gain_scratch = scratch[GradScatter.N_SCRATCH:]
    gains = GainSum(*gain_scratch)
    targets = sum(gains.targets, [])
    greet(targets)
    grads.fetch()
    _, depth = w_vmem.shape
    fetches = fetch_weight([(w_hbm, 0, depth)], w_vmem, w_sem)
    sums[...] = jnp.zeros_like(sums)
    units = Scatter.all_of(left, w_vmem, fetches, rs_scratch)
    u0, u1 = units

    def settle(s, unit):
        unit.arrive()

        def rows_fn(i):
            rows = row_block(i, ROWS)
            red = unit.total(rows).astype(BF16).astype(F32)
            red, d_gain = norm_rows_back(x_ref[s, rows, :].astype(F32), gain_ref[...], red)
            sums[...] += d_gain
            res_ref[s, rows, :] = (base_ref[s, rows, :].astype(F32) + red).astype(BF16)
        row_loop(pos, rows_fn)

    met(targets)
    grads.begin()
    u0.send_near()
    u0.send_far()
    grads.one_far()
    u1.send_near()
    u1.send_far()
    settle(0, u0)
    grads.one_done()
    settle(1, u1)
    rows, _ = dgm_ref.shape
    start, end = gains.total.at[0], gains.total.at[gains.STAGES]
    start[rows:, :] = dgm_ref[...]
    fold_row(jnp.sum(sums[...], axis=0, keepdims=True), start.at[pl.ds(0, rows)])
    gains.start(0)
    grads.two_far()
    for t in range(gains.STAGES):
        gains.advance(t)
    grads.two_done()
    unfold_row(end.at[pl.ds(0, rows)], ga_ref)
    unfold_row(end.at[pl.ds(rows, rows)], gm_ref)
    gains.sent()
    Scatter.all_sent(units)
    grads.sent()


def grad_kernel(h_ref, dy_ref, dgu_ref, act_ref, out_ref):
    _, cols = dgu_ref.shape
    out_ref[:, :cols] = lax.dot_general(h_ref[...], dgu_ref[...], TN, preferred_element_type=F32)
    out_ref[:, cols:] = lax.dot_general(dy_ref[...], act_ref[...], TN, preferred_element_type=F32)


def solution(mesh):
    act_spec = P('fsdp', 'model', None)
    rows_spec = P('fsdp', 'model')
    cols_spec = P('model', 'fsdp')

    def device_fn(x_loc, dy_loc, gain_attn, gain_mlp, wqkv_sh, wout_sh, wgate_sh, wup_sh, wdown_sh, rope_cos, rope_sin):
        n_seq, pos, width = x_loc.shape
        seq, half_dim = rope_cos.shape
        tokens = n_seq * seq
        head_dim = 2 * half_dim
        shard_rows, qkv_cols = wqkv_sh.shape
        out_rows, _ = wout_sh.shape
        ff, _ = wdown_sh.shape
        heads = out_rows // head_dim
        group = heads // ((qkv_cols - out_rows) // head_dim // 2)
        scale = head_dim ** -0.5
        gain_a, gain_m = gain_attn[None], gain_mlp[None]
        wout_t, wdown_t, cos_t, sin_t = wout_sh.T, wdown_sh.T, rope_cos.T, rope_sin.T
        piece_cols = 3 * ff // PIECES
        fold = 8

        vmem = pl.BlockSpec(memory_space=pltpu.VMEM)
        hbm = pl.BlockSpec(memory_space=pl.ANY)

        def shape(*dims, dtype=BF16):
            return jax.ShapeDtypeStruct(dims, dtype)

        def buf(*dims, dtype=BF16):
            return pltpu.VMEM(dims, dtype)

        def dma(*dims):
            return DMA(dims)

        def call(kernel, name, cid, us, ins, outs, scratch, args, aliases={}):
            spaces = {'V': vmem, 'H': hbm}
            shapes = tuple(out for _, out in outs)
            return pl.pallas_call(
                kernel, out_shape=shapes, in_specs=[spaces[i] for i in ins], out_specs=tuple(spaces[o] for o, _ in outs),
                scratch_shapes=scratch, name=name, input_output_aliases=aliases,
                cost_estimate=pl.CostEstimate(flops=us * 10 ** 9, bytes_accessed=10 ** 7, transcendentals=0),
                compiler_params=pltpu.CompilerParams(collective_id=cid, has_side_effects=True,
                                                     vmem_limit_bytes=VMEM_LIMIT))(*args)

        local, full = shape(n_seq, pos, width), shape(n_seq, seq, width)
        row_t, table = buf(ROWS, width, dtype=F32), buf(seq, head_dim, dtype=F32)
        shards = [wgate_sh, wup_sh, wdown_t]
        first, second, back, attn_back, leave = range(5)

        h_full, dy_full, w_qkv, w_out_t, pieces, qkv, attn = call(
            functools.partial(first_kernel, heads, group, scale), 'first', first, 50, 'V' * 10,
            [('H', full), ('H', full), ('H', shape(width, qkv_cols)), ('H', shape(width, out_rows)),
             ('H', shape(PIECES, width, piece_cols)), ('V', shape(n_seq, seq, qkv_cols)),
             ('V', shape(n_seq, seq, out_rows))],
            [buf(n_seq, pos, width), buf(n_seq, seq, width), buf(width, qkv_cols), buf(shard_rows, piece_cols), table,
             table, dma(n_seq + 1)] + Gather.sems(2 * n_seq) + 3 * WeightGather.sems(1),
            [x_loc, dy_loc, gain_a, wqkv_sh, wout_t] + shards + [cos_t, sin_t])

        mid, h_mlp, act, d_gu, pieces = call(
            second_kernel, 'second', second, 100, 'VHVVHVVVH',
            [('V', local), ('H', full), ('V', shape(tokens, ff)), ('V', shape(tokens, 2 * ff)),
             ('H', shape(PIECES, width, piece_cols))],
            Scatter.scratch(n_seq, pos, width)
            + [buf(width, out_rows), dma(Scatter.CHUNKS, 1), buf(n_seq, pos, width), buf(n_seq, seq, width),
               buf(seq, width), DMA, buf(2, width, piece_cols), dma(2), buf(PIECES, shard_rows, piece_cols), dma(n_seq)]
            + Gather.sems(n_seq) + WeightGather.sems(PIECES),
            [attn, w_out_t, x_loc, gain_m, dy_full] + shards + [pieces], aliases={8: 4})

        def whole(*dims):
            return pl.BlockSpec(dims, lambda i: (0,) * len(dims))

        block = width // 6

        def columns(rows):
            return pl.BlockSpec((rows, block), lambda i: (0, i))

        dw_mlp = pl.pallas_call(
            grad_kernel, grid=(width // block,), out_shape=shape(width, 3 * ff, dtype=F32),
            in_specs=[columns(tokens), columns(tokens), whole(tokens, 2 * ff), whole(tokens, ff)],
            out_specs=pl.BlockSpec((block, 3 * ff), lambda i: (i, 0)), name='grad_mlp',
            compiler_params=pltpu.CompilerParams(vmem_limit_bytes=VMEM_LIMIT),
        )(h_mlp.reshape(tokens, width), dy_full.reshape(tokens, width), d_gu, act)
        rs_mlp = lax.psum_scatter(dw_mlp, 'fsdp', scatter_dimension=0, tiled=True)
        d_gu, dw_mlp = lax.optimization_barrier((d_gu, dw_mlp))

        d_mid, d_mid_full, dgain_mlp = call(
            back_kernel, 'back', back, 90, 'VHVVV',
            [('V', local), ('H', full), ('V', shape(fold, width // fold, dtype=F32))],
            Scatter.scratch(n_seq, pos, width)
            + [buf(width, 2 * ff), dma(Scatter.CHUNKS, PIECES), buf(n_seq, pos, width), row_t] + Gather.sems(n_seq),
            [d_gu.reshape(n_seq, seq, 2 * ff), pieces, dy_loc, mid, gain_m])

        d_qkv, dw_qkv, y, rs_out_t = call(
            functools.partial(attn_back_kernel, heads, group, scale), 'attn_back', attn_back, 60, 'HHHVHVVVVV',
            [('V', shape(tokens, qkv_cols)), ('H', shape(width, qkv_cols, dtype=F32)), ('V', local),
             ('V', shape(shard_rows, out_rows, dtype=F32))],
            Scatter.scratch(n_seq, pos, width) + GradScatter.scratch(shard_rows, out_rows)
            + [buf(width, ff), dma(Scatter.CHUNKS, PIECES), buf(tokens, width), buf(width, out_rows), dma(2),
               buf(2, tokens, block), dma(2), buf(2, block, qkv_cols, dtype=F32), dma(2), buf(seq, out_rows)] + 4 * [table],
            [d_mid_full.reshape(tokens, width), w_out_t, h_full.reshape(tokens, width), act.reshape(n_seq, seq, ff), pieces,
             cos_t, sin_t, qkv.reshape(tokens, qkv_cols), attn.reshape(tokens, out_rows), mid])

        gain_out = shape(1, width, dtype=F32)
        dx, rs_qkv, gain_attn_sum, gain_mlp_sum = call(
            leave_kernel, 'leave', leave, 60, 'VHVVVHV',
            [('V', local), ('V', shape(shard_rows, qkv_cols, dtype=F32)), ('V', gain_out), ('V', gain_out)],
            Scatter.scratch(n_seq, pos, width) + GradScatter.scratch(shard_rows, qkv_cols)
            + [buf(width, qkv_cols), dma(Scatter.CHUNKS, 1), row_t] + GainSum.scratch(2 * fold, width // fold),
            [d_qkv.reshape(n_seq, seq, qkv_cols), w_qkv, d_mid, x_loc, gain_a, dw_qkv, dgain_mlp])

        def spread(i):
            step = ff // PIECES
            return jnp.concatenate([rs_mlp[:, (2 * j + i) * step:(2 * j + i + 1) * step] for j in range(PIECES)], axis=1)

        return (y, dx, gain_attn_sum[0], gain_mlp_sum[0], rs_qkv, rs_out_t.T, spread(0), spread(1), rs_mlp[:, 2 * ff:].T)

    in_specs = (act_spec, act_spec, P(), P(), rows_spec, cols_spec, rows_spec, rows_spec, cols_spec, P(), P())
    out_specs = (act_spec, act_spec, P(), P(), rows_spec, cols_spec, rows_spec, rows_spec, cols_spec)
    return jax.shard_map(device_fn, mesh=mesh, in_specs=in_specs, out_specs=out_specs, check_vma=False)
```

```python
import functools

import jax
import jax.numpy as jnp
from jax import lax
from jax.experimental import pallas as pl
from jax.experimental.pallas import tpu as pltpu
from jax.sharding import PartitionSpec as P

NORM_EPS = 1e-5
MASKED = -1e30
F32 = jnp.float32
BF16 = jnp.bfloat16
MESH = pl.DeviceIdType.MESH
DMA = pltpu.SemaphoreType.DMA
VMEM_LIMIT = 63 * 2 ** 20
RING = 4
ROWS = 16
PIECES = 4
HERE, NEXT, FAR, PREV = range(RING)
BY_RANK = (FAR, NEXT, PREV, HERE)
COLORS = range(2)
NT = (((1,), (1,)), ((), ()))
TN = (((0,), (0,)), ((), ()))


def go(place, distance):
    return (place + distance) % RING


def model_place():
    m = lax.axis_index('model')
    return m // 2, m % 2


def fsdp_place():
    f = lax.axis_index('fsdp')
    return f // RING, f % RING


def chip_targets():
    x, c = model_place()
    return [{'model': 2 * x + 1 - c}, {'model': 2 * go(x, NEXT) + c}, {'model': 2 * go(x, PREV) + c}]


def plane_targets():
    z, y = fsdp_place()
    return {'z': [{'fsdp': RING * go(z, d) + y} for d in (NEXT, PREV)],
            'y': [{'fsdp': RING * z + go(y, d)} for d in (NEXT, PREV)]}


def greet(targets):
    for target in targets:
        pl.semaphore_signal(pltpu.get_barrier_semaphore(), inc=1, device_id=target, device_id_type=MESH)


def met(targets):
    pl.semaphore_wait(pltpu.get_barrier_semaphore(), len(targets))


def chip_and_plane():
    plane = plane_targets()
    return chip_targets() + plane['z'] + plane['y']


def row_block(i, size, first=0):
    return pl.ds(pl.multiple_of(i * size + first, min(size, ROWS)), size)


def lane_block(i, size):
    return pl.ds(i * size if isinstance(i, int) else pl.multiple_of(i * size, size), size)


def row_loop(n_rows, fn, size=ROWS):
    def step(i, carry):
        fn(i)
        return carry
    lax.fori_loop(0, n_rows // size, step, None)


def row_sum(value):
    return jnp.sum(value, axis=-1, keepdims=True)


def row_mean(value):
    return jnp.mean(value, axis=-1, keepdims=True)


class Exchange:
    def __init__(self, send, recv):
        self.send, self.recv = send, recv

    def remote(self, i, src, dst, target):
        return pltpu.make_async_remote_copy(src_ref=src, dst_ref=dst, send_sem=self.send.at[i], recv_sem=self.recv.at[i],
                                            device_id=target, device_id_type=MESH)

    def landing(self):
        return [dst for _, dst, _ in self.copies()]

    def start(self, *which):
        table = self.copies()
        for i in which:
            self.remote(i, *table[i]).start()

    def arrived(self, *which):
        places, table = self.landing(), self.copies()
        for i in which:
            _, _, target = table[i]
            self.remote(i, places[i], places[i], target).wait_recv()

    def sent(self, *which):
        table = self.copies()
        for i in which or range(len(table)):
            self.remote(i, *table[i]).wait_send()


class Gather(Exchange):
    OTHER, UP, DOWN, PASS_UP, PASS_DOWN, PREV_OTHER, NEXT_OTHER, FAR_UP_OTHER, FAR_DOWN_OTHER = COPIES = range(9)

    def __init__(self, src, out, send, recv, local):
        super().__init__(send, recv)
        self.src, self.out, self.local = src, out, local
        self.x, self.c = model_place()
        self.pos, _ = src.shape
        self.half = self.pos // 2

    def block(self, distance, core):
        return self.out.at[row_block(2 * go(self.x, distance) + core, self.pos)]

    def part(self, distance, core, lower):
        place = 2 * go(self.x, distance) + core
        return self.out.at[row_block(2 * place + lower, self.half)]

    def copies(self):
        c = self.c
        other, nxt, prv = chip_targets()
        own = self.block(HERE, c)
        parts = [self.part(PREV, c, False), self.part(NEXT, c, True), self.block(PREV, c), self.block(NEXT, c),
                 self.part(FAR, c, False), self.part(FAR, c, True)]
        return [(self.src, own, other), (self.src, own, nxt), (self.src, own, prv)] + [
            (part, part, to) for part, to in zip(parts, (nxt, prv, other, other, other, other))]

    def landing(self):
        c, o = self.c, 1 - self.c
        return [self.block(HERE, o), self.block(PREV, c), self.block(NEXT, c), self.part(FAR, c, False),
                self.part(FAR, c, True), self.block(PREV, o), self.block(NEXT, o), self.part(FAR, o, False),
                self.part(FAR, o, True)]

    def own_copy(self):
        return pltpu.make_async_copy(self.src, self.block(HERE, self.c), self.local)

    def begin(self):
        if self.local is not None:
            self.own_copy().start()
        self.start(self.UP, self.DOWN, self.OTHER)

    def pass_near(self):
        self.arrived(self.UP)
        self.start(self.PASS_UP, self.PREV_OTHER)
        self.arrived(self.DOWN)
        self.start(self.PASS_DOWN, self.NEXT_OTHER)

    def pass_far(self):
        self.arrived(self.PASS_UP)
        self.start(self.FAR_UP_OTHER)
        self.arrived(self.PASS_DOWN)
        self.start(self.FAR_DOWN_OTHER)

    def complete(self):
        self.arrived(self.OTHER, self.PREV_OTHER, self.NEXT_OTHER, self.FAR_UP_OTHER, self.FAR_DOWN_OTHER)
        if self.local is not None:
            self.own_copy().wait()

    @classmethod
    def sems(cls, n):
        return [DMA((n, len(cls.COPIES))), DMA((n, len(cls.COPIES))), DMA((n,))]

    @classmethod
    def of(cls, i, src, out, sems, local=True):
        send, recv, local_sem = sems
        return cls(src, out, send.at[i], recv.at[i], local_sem.at[i] if local else None)


class RingGather(Exchange):
    UP, DOWN, PASS_UP, PASS_DOWN = COPIES = range(4)

    def __init__(self, src, at, targets, send, recv):
        super().__init__(send, recv)
        self.src, self.at, self.targets = src, at, targets
        rows, _ = src.shape
        self.upper, self.lower = row_block(0, rows // 2), row_block(1, rows // 2)

    def copies(self):
        nxt, prv = self.targets
        own, up, low = self.at(HERE), self.at(PREV).at[self.upper], self.at(NEXT).at[self.lower]
        return [(self.src, own, nxt), (self.src, own, prv), (up, up, nxt), (low, low, prv)]

    def landing(self):
        far = self.at(FAR)
        return [self.at(PREV), self.at(NEXT), far.at[self.upper], far.at[self.lower]]

    def begin(self):
        self.start(self.UP, self.DOWN)

    def pass_near(self):
        self.arrived(self.UP)
        self.start(self.PASS_UP)
        self.arrived(self.DOWN)
        self.start(self.PASS_DOWN)

    def far(self):
        self.arrived(self.PASS_UP, self.PASS_DOWN)


class WeightGather:
    def __init__(self, src, out, send, recv, local, first_row=0):
        self.src, self.out, self.local, self.first_row = src, out, local, first_row
        z, y = fsdp_place()
        self.place = RING * z + y
        self.rows, _ = src.shape
        half = self.rows // 2
        depth, _ = out.shape
        self.block = depth // RING ** 2
        targets = plane_targets()
        self.first, self.second = [], []
        for color, (one, two) in enumerate(('yz', 'zy')):
            part = src.at[row_block(color, half)]

            def at(d_one, d_two, one=one, color=color):
                dz, dy = (d_two, d_one) if one == 'y' else (d_one, d_two)
                first = (RING * go(z, dz) + go(y, dy)) * self.block + first_row + color * half
                return out.at[pl.ds(pl.multiple_of(first, ROWS), half)]
            self.first.append(RingGather(part, functools.partial(lambda at, d: at(d, HERE), at), targets[one],
                                         send.at[color, RING], recv.at[color, RING]))
            self.second.append([RingGather(at(d, HERE) if d else part, functools.partial(at, d), targets[two],
                                           send.at[color, d], recv.at[color, d]) for d in range(RING)])

    @staticmethod
    def sems(n):
        dims = (n, len(COLORS), RING + 1, len(RingGather.COPIES))
        return [DMA(dims), DMA(dims), DMA((n,))]

    @classmethod
    def of(cls, i, src, out, sems, local=True, first_row=0):
        send, recv, local_sem = sems
        return cls(src, out, send.at[i], recv.at[i], local_sem.at[i] if local else None, first_row)

    def own_rows(self):
        return pl.ds(pl.multiple_of(self.place * self.block + self.first_row, ROWS), self.rows)

    def own_copy(self):
        return pltpu.make_async_copy(self.src, self.out.at[self.own_rows()], self.local)

    def begin(self):
        if self.local is not None:
            self.own_copy().start()
        for ring in self.first:
            ring.begin()
        for rings in self.second:
            rings[HERE].begin()

    def pass_near(self):
        for one, two in zip(self.first, self.second):
            one.arrived(one.UP)
            one.start(one.PASS_UP)
            two[PREV].begin()
        for one, two in zip(self.first, self.second):
            one.arrived(one.DOWN)
            one.start(one.PASS_DOWN)
            two[NEXT].begin()
        self.pass_second(HERE)

    def pass_far(self):
        for one, two in zip(self.first, self.second):
            one.far()
            two[FAR].begin()

    def pass_second(self, d):
        for rings in self.second:
            rings[d].pass_near()

    def complete(self):
        for rings in self.second:
            for ring in rings:
                ring.far()
        if self.local is not None:
            self.own_copy().wait()

    def sent(self):
        for ring in self.first + sum(self.second, []):
            ring.sent()


class RingScatter(Exchange):
    FAR_UP, FAR_DOWN, UP_HI, DOWN_LO, UP_LO, DOWN_HI = COPIES = range(6)

    def __init__(self, mine, far, near, lo, hi, targets, send, recv):
        super().__init__(send, recv)
        self.mine, self.far, self.near, self.lo, self.hi, self.targets = mine, far, near, lo, hi, targets

    def copies(self):
        nxt, prv = self.targets
        far, up, down = (self.mine.at[BY_RANK.index(d)] for d in (FAR, NEXT, PREV))
        from_prv, from_nxt = self.near.at[0], self.near.at[1]
        lo, hi = self.lo, self.hi
        return [(far.at[lo], self.far.at[0], nxt), (far.at[hi], self.far.at[1], prv),
                (up.at[hi], from_prv.at[hi], nxt), (down.at[lo], from_nxt.at[lo], prv),
                (up.at[lo], from_prv.at[lo], nxt), (down.at[hi], from_nxt.at[hi], prv)]

    def begin(self):
        self.start(self.FAR_UP, self.FAR_DOWN, self.UP_HI, self.DOWN_LO)

    def add_far(self, add):
        up, down = (self.mine.at[BY_RANK.index(d)] for d in (NEXT, PREV))
        self.arrived(self.FAR_UP)
        add(up.at[self.lo], self.far.at[0])
        self.start(self.UP_LO)
        self.arrived(self.FAR_DOWN)
        add(down.at[self.hi], self.far.at[1])
        self.start(self.DOWN_HI)

    def arrive(self):
        self.arrived(self.UP_HI, self.DOWN_LO, self.UP_LO, self.DOWN_HI)

    def total(self, *at):
        return self.mine[(BY_RANK.index(HERE), *at)] + self.near[(0, *at)] + self.near[(1, *at)]


def add_rows(place, value):
    *outer, rows, _ = place.shape
    for at in [(i,) for i in range(*outer)] if outer else [()]:
        def add(i, at=at):
            place[(*at, row_block(i, ROWS))] += value[(*at, row_block(i, ROWS))]
        row_loop(rows, add)


class Scatter(Exchange):
    CHUNKS = 4

    def __init__(self, rows_of, weight, fetches, before, box, pair, mine, far, near, send, recv):
        super().__init__(send, recv)
        self.rows_of, self.weight, self.fetches, self.before = rows_of, weight, fetches, before
        self.box, self.pair, self.mine = box, pair, mine
        self.x, self.c = model_place()
        _, self.rows, self.width = mine.shape
        _, *ring_targets = chip_targets()
        half = self.width // 2
        rows = slice(None)
        ring_sems = (sem.at[pl.ds(RING, len(RingScatter.COPIES))] for sem in (send, recv))
        self.ring = RingScatter(mine, far, near, (rows, lane_block(0, half)), (rows, lane_block(1, half)), ring_targets,
                                *ring_sems)

    def copies(self):
        other, _, _ = chip_targets()
        return [(self.box.at[k], self.pair.at[k], other) for k in range(RING)]

    def pass_on(self, k):
        if self.before is not None:
            self.before.sent(k)
        chip = 2 * go(self.x, BY_RANK[k])
        left = jnp.concatenate([self.rows_of(chip + self.c), self.rows_of(chip + 1 - self.c)], axis=0)
        step = self.width // self.CHUNKS

        def chunk(i):
            if not k and self.fetches:
                for copy in self.fetches(i):
                    copy.wait()
            cols = lane_block(i, step)
            both = lax.dot_general(left, self.weight[cols, :], NT, preferred_element_type=F32)
            self.box[k, :, cols] = both[self.rows:]
            self.mine[k, :, cols] = both[:self.rows]
        row_loop(self.CHUNKS, chunk, 1)
        self.start(k)

    def pair_sum(self, k):
        self.arrived(k)
        add_rows(self.mine.at[k], self.pair.at[k])

    def send_near(self, meanwhile=None):
        far, up, down, here = range(RING)
        self.pass_on(far)
        if meanwhile is not None:
            meanwhile()
        self.pair_sum(far)
        self.ring.start(RingScatter.FAR_UP, RingScatter.FAR_DOWN)
        self.pass_on(up)
        self.pass_on(down)
        self.pair_sum(up)
        self.ring.start(RingScatter.UP_HI)
        self.pair_sum(down)
        self.ring.start(RingScatter.DOWN_LO)
        self.pass_on(here)

    def send_far(self):
        self.ring.add_far(add_rows)

    def arrive(self):
        self.pair_sum(BY_RANK.index(HERE))
        self.ring.arrive()

    def total(self, rows):
        return self.ring.total(rows)

    N_SCRATCH = 7

    @classmethod
    def scratch(cls, units, pos, width):
        sems = DMA((units, RING + len(RingScatter.COPIES)))
        return [pltpu.VMEM((RING, pos, width), F32), pltpu.VMEM((units, RING, pos, width), F32),
                pltpu.VMEM((units, RING, pos, width), F32), pltpu.VMEM((units, 2, pos, width // 2), F32),
                pltpu.VMEM((units, 2, pos, width), F32), sems, sems]

    @classmethod
    def all_of(cls, left, weight, fetches, scratch):
        box, *rest = scratch
        _, pos, _ = box.shape
        units, before = [], None
        n_seq, _, _ = left.shape
        for s in range(n_seq):
            def rows_of(place, s=s):
                return left[s, row_block(place, pos), :]
            before = cls(rows_of, weight, None if units else fetches, before, box, *(ref.at[s] for ref in rest))
            units.append(before)
        return units

    @staticmethod
    def all_sent(units):
        for unit in units:
            unit.ring.sent()
        unit.sent()


class GradScatter:
    N_SCRATCH = 9

    def __init__(self, part, out, mine1, far1, near1, mine2, far2, near2, send, recv, load):
        self.part, self.out, self.load, self.mine1, self.mine2 = part, out, load, mine1, mine2
        self.z, self.y = fsdp_place()
        rows, _ = out.shape
        self.half = rows // 2
        quarter = self.half // 2
        targets = plane_targets()
        self.one, self.two = [], []
        for color, (one, two) in enumerate(('yz', 'zy')):
            self.one.append(RingScatter(mine1.at[color], far1.at[color], near1.at[color], pl.ds(0, RING // 2),
                                        pl.ds(RING // 2, RING // 2), targets[one], send.at[color, 0], recv.at[color, 0]))
            self.two.append(RingScatter(mine2.at[color], far2.at[color], near2.at[color], row_block(0, quarter),
                                        row_block(1, quarter), targets[two], send.at[color, 1], recv.at[color, 1]))

    @staticmethod
    def scratch(rows, cols):
        half, n = rows // 2, len(COLORS)
        sems = DMA((n, 2, len(RingScatter.COPIES)))
        return [pltpu.VMEM((n, RING, RING, half, cols), F32), pltpu.VMEM((n, 2, RING // 2, half, cols), F32),
                pltpu.VMEM((n, 2, RING, half, cols), F32), pltpu.VMEM((n, RING, half, cols), F32),
                pltpu.VMEM((n, 2, half // 2, cols), F32), pltpu.VMEM((n, 2, half, cols), F32), sems, sems,
                DMA((n, RING, RING))]

    def loads(self):
        for color in COLORS:
            for k, d_one in enumerate(BY_RANK):
                for j, d_two in enumerate(BY_RANK):
                    dz, dy = (d_one, d_two) if color else (d_two, d_one)
                    place = RING * go(self.z, dz) + go(self.y, dy)
                    yield pltpu.make_async_copy(self.part.at[row_block(2 * place + color, self.half)],
                                                self.mine1.at[color, k, j], self.load.at[color, k, j])

    def fetch(self):
        for load in self.loads():
            load.start()

    def put(self, place, value):
        def rank(there, here):
            distance = (there + RING - here) % RING
            found = BY_RANK.index(HERE)
            for d in (NEXT, FAR, PREV):
                found = jnp.where(distance == d, BY_RANK.index(d), found)
            return found
        dz, dy = rank(place // RING, self.z), rank(place % RING, self.y)
        for color, at in enumerate(((dy, dz), (dz, dy))):
            self.mine1[(color, *at)] = value[color * self.half:(color + 1) * self.half]

    def begin(self):
        if self.part is not None:
            for load in self.loads():
                load.wait()
        for ring in self.one:
            ring.begin()

    def one_far(self):
        for ring in self.one:
            ring.add_far(add_rows)

    def one_done(self):
        for color, (one, two) in enumerate(zip(self.one, self.two)):
            one.arrive()
            for j in range(RING):
                def add(i, j=j):
                    rows = row_block(i, ROWS)
                    self.mine2[color, j, rows, :] = one.total(j, rows)
                row_loop(self.half, add)
            two.begin()

    def two_far(self):
        for ring in self.two:
            ring.add_far(add_rows)

    def two_done(self):
        for color, ring in enumerate(self.two):
            ring.arrive()

            def add(i):
                self.out[row_block(i, ROWS, color * self.half), :] = ring.total(row_block(i, ROWS))
            row_loop(self.half, add)

    def sent(self):
        for ring in self.one + self.two:
            ring.sent()


class GainSum:
    STAGES = 4

    def __init__(self, total, slots, send, recv):
        self.total, self.slots, self.send, self.recv = total, slots, send, recv
        (x, c), (z, y) = model_place(), fsdp_place()
        away = (NEXT, FAR, PREV)
        self.places = [c, x, y, z]
        self.targets = [[{'model': 2 * x + 1 - c}], [{'model': 2 * go(x, d) + c} for d in away],
                        [{'fsdp': RING * z + go(y, d)} for d in away], [{'fsdp': RING * go(z, d) + y} for d in away]]

    @classmethod
    def scratch(cls, *shape):
        dims = (cls.STAGES, RING - 1)
        return [pltpu.VMEM((cls.STAGES + 1, *shape), F32), pltpu.VMEM((*dims, *shape), F32), DMA(dims), DMA(dims)]

    def copies(self, t):
        return [pltpu.make_async_remote_copy(
            src_ref=self.total.at[t], dst_ref=self.slots.at[t, d], send_sem=self.send.at[t, d],
            recv_sem=self.recv.at[t, d], device_id=target, device_id_type=MESH)
            for d, target in enumerate(self.targets[t])]

    def start(self, t):
        for copy in self.copies(t):
            copy.start()

    def advance(self, t):
        others = len(self.targets[t])
        n = others + 1
        for copy in self.copies(t):
            copy.wait_recv()
        acc = None
        for i in range(n):
            term = self.total[t]
            for d in range(others):
                term = jnp.where((self.places[t] + others - d) % n == i, self.slots[t, d], term)
            acc = term if acc is None else acc + term
        self.total[t + 1] = acc
        if t + 1 < self.STAGES:
            self.start(t + 1)

    def sent(self):
        for t in range(self.STAGES):
            for copy in self.copies(t):
                copy.wait_send()


def norm_rows(x_f32, gain):
    return x_f32 * lax.rsqrt(row_mean(x_f32 * x_f32) + NORM_EPS) * gain


def norm_rows_back(x_f32, gain, cotangent):
    inv_rms = lax.rsqrt(row_mean(x_f32 * x_f32) + NORM_EPS)
    x_hat = x_f32 * inv_rms
    scaled = cotangent * gain
    return inv_rms * (scaled - x_hat * row_mean(scaled * x_hat)), cotangent * x_hat


def fold_row(row, out):
    rows, step = out.shape
    for i in range(rows):
        out[i:i + 1, :] = row[:, i * step:(i + 1) * step]


def unfold_row(rows_ref, out):
    rows, step = rows_ref.shape
    for i in range(rows):
        out[:, i * step:(i + 1) * step] = rows_ref[i:i + 1, :]


def rope_tables(cos_ref, sin_ref, cos_t, sin_t):
    cos, sin = cos_ref[...].T, sin_ref[...].T
    cos_t[...] = jnp.concatenate([cos, cos], axis=1)
    sin_t[...] = jnp.concatenate([-sin, sin], axis=1)


def spin(tensor, cos_t, sin_t):
    _, lanes = tensor.shape
    return tensor * cos_t + pltpu.roll(tensor, lanes // 2, 1) * sin_t


def probs(query, key, scale, first_row):
    scores = lax.dot_general(query, key, NT, preferred_element_type=F32) * scale
    rows, cols = (lax.broadcasted_iota(jnp.int32, scores.shape, dim) for dim in range(scores.ndim))
    scores = jnp.where(first_row + rows >= cols, scores, MASKED)
    expd = jnp.exp(scores - jnp.max(scores, axis=-1, keepdims=True))
    return expd / row_sum(expd)


def piece_of(refs, j, out):
    _, cols = out.shape
    step = cols // len(refs)
    for i, ref in enumerate(refs):
        out[:, lane_block(i, step)] = ref[:, lane_block(j, step)]


def fetch_weight(sources, w_vmem, sem):
    depth, _ = w_vmem.shape
    step = depth // Scatter.CHUNKS

    def chunk(i):
        rows, col, copies = row_block(i, step), 0, []
        for n, (ref, first, size) in enumerate(sources):
            copies.append(pltpu.make_async_copy(ref.at[rows, pl.ds(first, size)], w_vmem.at[rows, pl.ds(col, size)],
                                                sem.at[i, n]))
            col += size
        return copies
    for i in range(Scatter.CHUNKS):
        for copy in chunk(i):
            copy.start()
    return chunk


def early_rows(shard_rows):
    return shard_rows // 3


def first_kernel(heads, group, scale, x_ref, dy_ref, gain_ref, wqkv_src, wout_src, wd_src, cos_ref, sin_ref,
                 h_out, dy_out, wqkv_out, wout_out, wdown_out, qkv_ref, attn_ref,
                 h_src, h_buf, w_buf, cos_t, sin_t, flush, *sems):
    targets = chip_and_plane()
    greet(targets)
    n_seq, pos, _ = x_ref.shape
    seq, head_dim = cos_t.shape
    block = seq // 2
    _, cols = w_buf.shape
    x, c = model_place()
    mine = row_block(2 * x + c, pos)
    for s in range(n_seq):
        def norm(i, s=s):
            rows = row_block(i, ROWS)
            h_src[s, rows, :] = norm_rows(x_ref[s, rows, :].astype(F32), gain_ref[...]).astype(BF16)
        row_loop(pos, norm)
    g_sems, w_sems = sems[:3], sems[3:]
    w_qkv = WeightGather.of(0, wqkv_src, w_buf, w_sems[:3], local=False)
    w_out = WeightGather.of(0, wout_src, wout_out, w_sems[3:6])
    shard_rows, _ = wqkv_src.shape
    early = early_rows(shard_rows)
    w_down = WeightGather.of(0, wd_src.at[pl.ds(0, early)], wdown_out, w_sems[6:])
    h0, h1 = (Gather.of(s, h_src.at[s], h_buf.at[s], g_sems, local=False) for s in range(n_seq))
    dy0, dy1 = (Gather.of(n_seq + s, dy_ref.at[s], dy_out.at[s], g_sems) for s in range(n_seq))
    met(targets)
    w_qkv.begin()
    h0.begin()
    h1.begin()
    rope_tables(cos_ref, sin_ref, cos_t, sin_t)
    for s in range(n_seq):
        h_buf[s, mine, :] = h_src[s]
    w_buf[w_qkv.own_rows(), :] = wqkv_src[...]
    w_qkv.pass_near()
    w_out.begin()
    w_qkv.pass_far()
    h0.pass_near()
    w_qkv.pass_second(PREV)
    w_qkv.pass_second(NEXT)
    w_out.pass_near()
    w_down.begin()
    w_qkv.pass_second(FAR)
    h1.pass_near()
    dy0.begin()
    dy1.begin()
    w_out.pass_far()
    h0.pass_far()
    w_down.pass_near()
    w_out.pass_second(PREV)
    w_out.pass_second(NEXT)
    w_qkv.complete()
    w_flush = pltpu.make_async_copy(w_buf, wqkv_out, flush.at[n_seq])
    w_flush.start()

    def lanes(i):
        return lane_block(i, head_dim)

    def project(s):
        def one_block(i):
            rows = row_block(i, block)
            qkv = jnp.dot(h_buf[s, rows, :], w_buf[...], preferred_element_type=F32)
            for j in range(cols // head_dim):
                one = qkv[:, j * head_dim:(j + 1) * head_dim]
                if j % (group + 2) <= group:
                    one = spin(one, cos_t[rows, :], sin_t[rows, :])
                qkv_ref[s, rows, lanes(j)] = one.astype(BF16)
        row_loop(seq, one_block, block)

    def attend(s):
        for g in range(heads // group):
            first = g * (group + 2)

            def head(j, first=first, g=g):
                for i in range(seq // block):
                    rows, keys = pl.ds(i * block, block), pl.ds(0, (i + 1) * block)
                    key, value = qkv_ref[s, keys, lanes(first + group)], qkv_ref[s, keys, lanes(first + group + 1)]
                    prob = probs(qkv_ref[s, rows, lanes(first + j)], key, scale, i * block)
                    attn_ref[s, rows, lanes(g * group + j)] = jnp.dot(
                        prob.astype(BF16), value, preferred_element_type=F32).astype(BF16)
            row_loop(group, head, 1)

    def h_flush(s):
        return pltpu.make_async_copy(h_buf.at[s], h_out.at[s], flush.at[s])

    h0.complete()
    h_flush(0).start()
    project(0)
    w_down.pass_far()
    w_out.pass_second(FAR)
    h1.pass_far()
    attend(0)
    w_down.pass_second(PREV)
    w_down.pass_second(NEXT)
    h1.complete()
    h_flush(1).start()
    project(1)
    dy0.pass_near()
    w_down.pass_second(FAR)
    attend(1)
    dy0.pass_far()
    dy1.pass_near()
    dy1.pass_far()
    for each in (dy0, dy1, w_out, w_down):
        each.complete()
    for each in (h0, h1, dy0, dy1, w_qkv, w_out, w_down):
        each.sent()
    w_flush.wait()
    for s in range(n_seq):
        h_flush(s).wait()


def second_kernel(left, wout_hbm, base_ref, gain_ref, dy_hbm, wg_ref, wu_ref, wd_src, wdown_in, mid_ref, act_out, dgu_out,
                  dw_out, pieces_out, wdown_out, *scratch):
    targets = chip_and_plane()
    greet(targets)
    n_seq, pos, _ = base_ref.shape
    rs_scratch, scratch = scratch[:Scatter.N_SCRATCH], scratch[Scatter.N_SCRATCH:]
    (wo_vmem, wo_sem, g_src, h_buf, dy_buf, dy_sem, w_bufs, w_sem, piece_src, act_ref, dgu_ref, da_ref, dw_sem, flush,
     *scratch) = scratch
    _, _, stage, *_ = rs_scratch
    g_sems, p_sems = scratch[:3], scratch[3:]
    tokens, _ = dy_buf.shape
    seq = tokens // n_seq
    block = seq // 2
    _, out_rows = wo_vmem.shape
    _, _, cols = w_bufs.shape
    step = cols // 2
    fetches = fetch_weight([(wout_hbm, 0, out_rows)], wo_vmem, wo_sem)
    shard_rows, _ = wg_ref.shape
    early = early_rows(shard_rows)

    def fill(j):
        piece_of((wg_ref, wu_ref), j, piece_src.at[j])

    p0, p1, p2, p3 = pieces = [WeightGather.of(j, piece_src.at[j], pieces_out.at[j], p_sems) for j in range(PIECES)]
    w_down = WeightGather.of(PIECES, wd_src.at[pl.ds(early, shard_rows - early)], wdown_out, p_sems, first_row=early)
    x, c = model_place()
    units = Scatter.all_of(left, wo_vmem, fetches, rs_scratch)
    u0, u1 = units
    h0, h1 = gathers = [Gather.of(s, g_src.at[s], h_buf.at[pl.ds(s * seq, seq)], g_sems, local=False)
                        for s in range(n_seq)]

    def settle(s, unit, gather):
        unit.arrive()

        def rows_fn(i):
            rows = row_block(i, ROWS)
            red = unit.total(rows).astype(BF16).astype(F32)
            mid = (base_ref[s, rows, :].astype(F32) + red).astype(BF16)
            mid_ref[s, rows, :] = mid
            g_src[s, rows, :] = norm_rows(mid.astype(F32), gain_ref[...]).astype(BF16)
        row_loop(pos, rows_fn)
        gather.begin()
        h_buf[row_block(2 * x + c, pos, s * seq), :] = g_src[s]

    dy_load = pltpu.make_async_copy(dy_hbm, dy_buf, dy_sem)
    last = PIECES - 1

    def load_down(half):
        return pltpu.make_async_copy(wdown_out.at[:, lane_block(half, cols)], w_bufs.at[half], w_sem.at[half])

    def load_piece(load):
        piece = jnp.where(load == 2 * last, last, load % last)
        return pltpu.make_async_copy(pieces_out.at[piece], w_bufs.at[load % 2], w_sem.at[load % 2])

    def act_back(s, half):
        def rows_fn(i):
            there = row_block(i, block, s * seq)
            da_ref[there, lane_block(half, cols)] = jnp.dot(dy_buf[there, :], w_bufs[half],
                                                            preferred_element_type=F32).astype(BF16)
        row_loop(seq, rows_fn, block)

    def mlp(s, j, load):
        def rows_fn(i):
            there = row_block(i, block, s * seq)
            both = jnp.dot(h_buf[there, :], w_bufs[load % 2], preferred_element_type=F32)
            gate, up_proj = both[:, :step], both[:, step:]
            d_act = da_ref[there, lane_block(j, step)].astype(F32)
            sig_gate = jax.nn.sigmoid(gate)
            silu_gate = gate * sig_gate
            act_ref[there, lane_block(j, step)] = (silu_gate * up_proj).astype(BF16)
            dgu_ref[there, lane_block(2 * j, step)] = (
                d_act * up_proj * sig_gate * (1.0 + gate * (1.0 - sig_gate))).astype(BF16)
            dgu_ref[there, lane_block(2 * j + 1, step)] = (d_act * silu_gate).astype(BF16)
        row_loop(seq, rows_fn, block)

    def all_but_last(load):
        def ahead_of_second():
            h1.pass_near()
            p2.complete()
            p3.pass_far()

        def ahead_of_third():
            h1.pass_far()
            p3.pass_second(PREV)
            p3.pass_second(NEXT)

        def ahead_of_next_sequence():
            h1.complete()
            p3.pass_second(FAR)

        for at, fn in {1: ahead_of_second, 2: ahead_of_third, last: ahead_of_next_sequence, 2 * last - 1: p3.complete}.items():
            pl.when(load == at)(fn)
        load_piece(load).wait()
        load_piece(load + 1).start()
        mlp(load // last, load % last, load)

    _, kept_rows, _ = g_src.shape
    col_step = RING * kept_rows
    per_block = col_step // kept_rows
    width, _ = wo_vmem.shape
    _, cols_gu = dgu_ref.shape

    def dw_copies(i):
        return [pltpu.make_async_copy(stage.at[i % 2, k], dw_out.at[row_block(i * per_block + k, kept_rows)],
                                      dw_sem.at[i % 2, k]) for k in range(per_block)]

    def weight_grads(i):
        slot = i % 2

        @pl.when(i >= 2)
        def _():
            for copy in dw_copies(i - 2):
                copy.wait()
        half = cols_gu // 2
        h_t, dy_t = h_buf[:, lane_block(i, col_step)], dy_buf[:, lane_block(i, col_step)]
        for n, (left_cols, right) in enumerate(((h_t, dgu_ref[:, :half]), (h_t, dgu_ref[:, half:]), (dy_t, act_ref[...]))):
            block_of = lax.dot_general(left_cols, right, TN, preferred_element_type=F32)
            for k in range(per_block):
                stage[slot, k, :, lane_block(n, half)] = block_of[k * kept_rows:(k + 1) * kept_rows]
        for copy in dw_copies(i):
            copy.start()

    dy_load.start()

    def fill_first():
        for j in (0, 1):
            fill(j)
        w_down.begin()
        p0.begin()

    met(targets)
    u0.send_near(fill_first)
    for j in range(2, PIECES):
        fill(j)
    w_down.pass_near()
    u0.send_far()
    w_down.pass_far()
    p0.pass_near()
    w_down.pass_second(PREV)
    w_down.pass_second(NEXT)
    u1.send_near()
    p1.begin()
    w_down.pass_second(FAR)
    p0.pass_far()
    p0.pass_second(PREV)
    settle(0, u0, h0)
    p0.pass_second(NEXT)
    p1.pass_near()
    u1.send_far()
    w_down.complete()
    load_down(0).start()
    load_down(1).start()
    p0.pass_second(FAR)
    p1.pass_far()
    p2.begin()
    dy_load.wait()
    load_down(0).wait()
    act_back(0, 0)
    p1.pass_second(PREV)
    act_back(1, 0)
    p1.pass_second(NEXT)
    p2.pass_near()
    h0.pass_near()
    load_down(1).wait()
    act_back(0, 1)
    p1.pass_second(FAR)
    p2.pass_far()
    p3.begin()
    act_back(1, 1)
    p2.pass_second(PREV)
    p0.complete()
    load_piece(0).start()
    settle(1, u1, h1)
    h0.pass_far()
    p2.pass_second(NEXT)
    p2.pass_second(FAR)
    p3.pass_near()
    p1.complete()
    h0.complete()
    row_loop(2 * last, all_but_last, 1)
    load_piece(2 * last).wait()
    mlp(0, last, 2 * last)
    mlp(1, last, 2 * last)
    flushes = [pltpu.make_async_copy(act_ref, act_out, flush.at[0]), pltpu.make_async_copy(dgu_ref, dgu_out, flush.at[1])]
    for copy in flushes:
        copy.start()
    Scatter.all_sent(units)
    n_blocks = width // col_step
    row_loop(n_blocks, weight_grads, 1)
    for each in gathers + pieces + [w_down]:
        each.sent()
    for copy in flushes + dw_copies(n_blocks - 2) + dw_copies(n_blocks - 1):
        copy.wait()


def back_kernel(left, pieces, base_ref, mid_ref, gain_ref, res_ref, full_out, dgain_ref, *scratch):
    targets = chip_targets()
    greet(targets)
    n_seq, pos, _ = base_ref.shape
    rs_scratch, scratch = scratch[:Scatter.N_SCRATCH], scratch[Scatter.N_SCRATCH:]
    w_vmem, w_sem, g_src, sums, *sems = scratch
    _, depth = w_vmem.shape
    fetches = fetch_weight([(pieces.at[j], 0, depth // PIECES) for j in range(PIECES)], w_vmem, w_sem)
    units = Scatter.all_of(left, w_vmem, fetches, rs_scratch)
    u0, u1 = units
    g0, g1 = gathers = [Gather.of(s, g_src.at[s], full_out.at[s], sems) for s in range(n_seq)]
    sums[...] = jnp.zeros_like(sums)

    def settle(s, unit, gather):
        unit.arrive()

        def rows_fn(i):
            rows = row_block(i, ROWS)
            red = unit.total(rows).astype(BF16).astype(F32)
            d_norm, d_gain = norm_rows_back(mid_ref[s, rows, :].astype(F32), gain_ref[...], red)
            out = (base_ref[s, rows, :].astype(F32) + d_norm).astype(BF16)
            sums[...] += d_gain
            res_ref[s, rows, :] = out
            g_src[s, rows, :] = out
        row_loop(pos, rows_fn)
        gather.begin()

    met(targets)
    u0.send_near()
    u0.send_far()
    u1.send_near()
    settle(0, u0, g0)
    u1.send_far()
    g0.pass_near()
    settle(1, u1, g1)
    g0.pass_far()
    g1.pass_near()
    g1.pass_far()
    fold_row(jnp.sum(sums[...], axis=0, keepdims=True), dgain_ref)
    for gather in gathers:
        gather.complete()
    Scatter.all_sent(units)
    for gather in gathers:
        gather.sent()


def attn_back_kernel(heads, group, scale, dm_hbm, wo_hbm, h_hbm, left, wd_hbm, rope_cos, rope_sin, qkv_ref, attn_ref, mid_ref,
                     dqkv_ref, dwqkv_out, y_ref, dwout_ref, *scratch):
    targets = chip_and_plane()
    greet(targets)
    _, pos, width = mid_ref.shape
    half_dim, seq = rope_cos.shape
    head_dim = 2 * half_dim
    block = seq // 2
    rs_scratch, scratch = scratch[:Scatter.N_SCRATCH], scratch[Scatter.N_SCRATCH:]
    grads = GradScatter(None, dwout_ref, *scratch[:GradScatter.N_SCRATCH])
    (wd_vmem, wd_sem, dm_ref, wo_ref, in_sem, h_buf, h_sem, dw_buf, dw_sem, do_ref, dk_ref, dv_ref, cos_ref,
     sin_ref) = scratch[GradScatter.N_SCRATCH:]
    _, ff = wd_vmem.shape
    fetches = fetch_weight([(wd_hbm, 0, ff)], wd_vmem, wd_sem)
    dm_copy = pltpu.make_async_copy(dm_hbm, dm_ref, in_sem.at[0])
    wo_copy = pltpu.make_async_copy(wo_hbm, wo_ref, in_sem.at[1])
    dm_copy.start()
    wo_copy.start()
    _, _, h_cols = h_buf.shape
    n_blocks = width // h_cols

    def h_copy(i):
        return pltpu.make_async_copy(h_hbm.at[:, lane_block(i, h_cols)], h_buf.at[i % 2], h_sem.at[i % 2])

    def dw_copy(i):
        return pltpu.make_async_copy(dw_buf.at[i % 2], dwqkv_out.at[row_block(i, h_cols)], dw_sem.at[i % 2])
    h_copy(0).start()
    rope_tables(rope_cos, rope_sin, cos_ref, sin_ref)
    units = Scatter.all_of(left, wd_vmem, fetches, rs_scratch)
    u0, u1 = units

    def settle(s, unit):
        unit.arrive()

        def rows_fn(i):
            rows = row_block(i, ROWS)
            red = unit.total(rows).astype(BF16).astype(F32)
            y_ref[s, rows, :] = (mid_ref[s, rows, :].astype(F32) + red).astype(BF16)
        row_loop(pos, rows_fn)

    def out_grads():
        shard, _ = dwout_ref.shape

        def two_places(i):
            both = lax.dot_general(dm_ref[:, lane_block(i, 2 * shard)], attn_ref[...], TN, preferred_element_type=F32)
            grads.put(2 * i, both[:shard])
            grads.put(2 * i + 1, both[shard:])
        row_loop(width, two_places, 2 * shard)

    def lanes(i):
        return lane_block(i, head_dim)

    def attention(s):
        base = s * seq

        def project(i):
            do_ref[row_block(i, block), :] = jnp.dot(dm_ref[row_block(i, block, base), :], wo_ref[...],
                                                     preferred_element_type=F32).astype(BF16)
        row_loop(seq, project, block)
        for g in range(heads // group):
            first = g * (group + 2)
            dk_ref[...] = jnp.zeros_like(dk_ref)
            dv_ref[...] = jnp.zeros_like(dv_ref)
            for i in range(seq // block):
                rows, keys = pl.ds(i * block, block), pl.ds(0, (i + 1) * block)
                g_rows, g_keys = pl.ds(base + i * block, block), pl.ds(base, (i + 1) * block)
                key, value = qkv_ref[g_keys, lanes(first + group)], qkv_ref[g_keys, lanes(first + group + 1)]

                def head(j, rows=rows, keys=keys, g_rows=g_rows, key=key, value=value, first=first, g=g, i=i):
                    query = qkv_ref[g_rows, lanes(first + j)]
                    d_out = do_ref[rows, lanes(g * group + j)]
                    prob = probs(query, key, scale, i * block)
                    d_prob = lax.dot_general(d_out, value, NT, preferred_element_type=F32)
                    d_scores = (prob * (d_prob - row_sum(d_prob * prob)) * scale).astype(BF16)
                    d_query = jnp.dot(d_scores, key, preferred_element_type=F32)
                    dqkv_ref[g_rows, lanes(first + j)] = spin(d_query, cos_ref[rows, :], -sin_ref[rows, :]).astype(BF16)
                    dk_ref[keys, :] += lax.dot_general(d_scores, query, TN, preferred_element_type=F32)
                    dv_ref[keys, :] += lax.dot_general(prob.astype(BF16), d_out, TN, preferred_element_type=F32)
                row_loop(group, head, 1)
            every = pl.ds(base, seq)
            dqkv_ref[every, lanes(first + group)] = spin(dk_ref[...], cos_ref[...], -sin_ref[...]).astype(BF16)
            dqkv_ref[every, lanes(first + group + 1)] = dv_ref[...].astype(BF16)

    def qkv_grads():
        def one_block(i):
            @pl.when(i + 1 < n_blocks)
            def _():
                h_copy(i + 1).start()
            h_copy(i).wait()

            @pl.when(i >= 2)
            def _():
                dw_copy(i - 2).wait()
            dw_buf[i % 2] = lax.dot_general(h_buf[i % 2], dqkv_ref[...], TN, preferred_element_type=F32)
            dw_copy(i).start()
        row_loop(n_blocks, one_block, 1)

    met(targets)
    u0.send_near()
    dm_copy.wait()
    out_grads()
    grads.begin()
    u0.send_far()
    u1.send_near()
    wo_copy.wait()
    attention(0)
    u1.send_far()
    grads.one_far()
    settle(0, u0)
    attention(1)
    grads.one_done()
    qkv_grads()
    settle(1, u1)
    grads.two_far()
    grads.two_done()
    for i in (n_blocks - 2, n_blocks - 1):
        dw_copy(i).wait()
    Scatter.all_sent(units)
    grads.sent()


def leave_kernel(left, w_hbm, base_ref, x_ref, gain_ref, grad_hbm, dgm_ref, res_ref, grad_ref, ga_ref, gm_ref, *scratch):
    _, pos, _ = base_ref.shape
    rs_scratch, scratch = scratch[:Scatter.N_SCRATCH], scratch[Scatter.N_SCRATCH:]
    grads = GradScatter(grad_hbm, grad_ref, *scratch[:GradScatter.N_SCRATCH])
    w_vmem, w_sem, sums, *gain_scratch = scratch[GradScatter.N_SCRATCH:]
    gains = GainSum(*gain_scratch)
    targets = sum(gains.targets, [])
    greet(targets)
    grads.fetch()
    _, depth = w_vmem.shape
    fetches = fetch_weight([(w_hbm, 0, depth)], w_vmem, w_sem)
    sums[...] = jnp.zeros_like(sums)
    units = Scatter.all_of(left, w_vmem, fetches, rs_scratch)
    u0, u1 = units

    def settle(s, unit):
        unit.arrive()

        def rows_fn(i):
            rows = row_block(i, ROWS)
            red = unit.total(rows).astype(BF16).astype(F32)
            red, d_gain = norm_rows_back(x_ref[s, rows, :].astype(F32), gain_ref[...], red)
            sums[...] += d_gain
            res_ref[s, rows, :] = (base_ref[s, rows, :].astype(F32) + red).astype(BF16)
        row_loop(pos, rows_fn)

    met(targets)
    grads.begin()
    u0.send_near()
    u0.send_far()
    grads.one_far()
    u1.send_near()
    u1.send_far()
    settle(0, u0)
    grads.one_done()
    settle(1, u1)
    rows, _ = dgm_ref.shape
    start, end = gains.total.at[0], gains.total.at[gains.STAGES]
    start[rows:, :] = dgm_ref[...]
    fold_row(jnp.sum(sums[...], axis=0, keepdims=True), start.at[pl.ds(0, rows)])
    gains.start(0)
    grads.two_far()
    for t in range(gains.STAGES):
        gains.advance(t)
    grads.two_done()
    unfold_row(end.at[pl.ds(0, rows)], ga_ref)
    unfold_row(end.at[pl.ds(rows, rows)], gm_ref)
    gains.sent()
    Scatter.all_sent(units)
    grads.sent()


def outputs_kernel(grads_ref, *refs):
    *refs, gate_ref, up_ref, down_ref = refs
    n = len(refs) // 2
    for src, dst in zip(refs[:n], refs[n:]):
        dst[...] = src[...]
    _, ff = gate_ref.shape
    step = ff // PIECES
    for j in range(PIECES):
        gate_ref[:, lane_block(j, step)] = grads_ref[:, lane_block(2 * j, step)]
        up_ref[:, lane_block(j, step)] = grads_ref[:, lane_block(2 * j + 1, step)]
    down_ref[...] = grads_ref[:, lane_block(2, ff)]


def solution(mesh):
    act_spec = P('fsdp', 'model', None)
    rows_spec = P('fsdp', 'model')
    cols_spec = P('model', 'fsdp')

    def device_fn(x_loc, dy_loc, gain_attn, gain_mlp, wqkv_sh, wout_sh, wgate_sh, wup_sh, wdown_sh, rope_cos, rope_sin):
        n_seq, pos, width = x_loc.shape
        seq, half_dim = rope_cos.shape
        tokens = n_seq * seq
        head_dim = 2 * half_dim
        shard_rows, qkv_cols = wqkv_sh.shape
        out_rows, _ = wout_sh.shape
        ff, _ = wdown_sh.shape
        heads = out_rows // head_dim
        group = heads // ((qkv_cols - out_rows) // head_dim // 2)
        scale = head_dim ** -0.5
        gain_a, gain_m = gain_attn[None], gain_mlp[None]
        wout_t, wdown_t, cos_t, sin_t = wout_sh.T, wdown_sh.T, rope_cos.T, rope_sin.T
        piece_cols = 2 * ff // PIECES
        fold = 8

        vmem = pl.BlockSpec(memory_space=pltpu.VMEM)
        hbm = pl.BlockSpec(memory_space=pl.ANY)

        def shape(*dims, dtype=BF16):
            return jax.ShapeDtypeStruct(dims, dtype)

        def buf(*dims, dtype=BF16):
            return pltpu.VMEM(dims, dtype)

        def dma(*dims):
            return DMA(dims)

        def call(kernel, name, cid, us, ins, outs, scratch, args, aliases={}):
            spaces = {'V': vmem, 'H': hbm}
            shapes = tuple(out for _, out in outs)
            return pl.pallas_call(
                kernel, out_shape=shapes, in_specs=[spaces[i] for i in ins], out_specs=tuple(spaces[o] for o, _ in outs),
                scratch_shapes=scratch, name=name, input_output_aliases=aliases,
                cost_estimate=pl.CostEstimate(flops=us * 10 ** 9, bytes_accessed=10 ** 7, transcendentals=0),
                compiler_params=pltpu.CompilerParams(collective_id=cid, has_side_effects=True,
                                                     vmem_limit_bytes=VMEM_LIMIT))(*args)

        local, full = shape(n_seq, pos, width), shape(n_seq, seq, width)
        row_t, table = buf(ROWS, width, dtype=F32), buf(seq, head_dim, dtype=F32)
        first, second, back, attn_back, leave = range(5)

        h_full, dy_full, w_qkv, w_out_t, w_down_t, qkv, attn = call(
            functools.partial(first_kernel, heads, group, scale), 'first', first, 50, 'V' * 8,
            [('H', full), ('H', full), ('H', shape(width, qkv_cols)), ('H', shape(width, out_rows)),
             ('H', shape(width, ff)), ('V', shape(n_seq, seq, qkv_cols)),
             ('V', shape(n_seq, seq, out_rows))],
            [buf(n_seq, pos, width), buf(n_seq, seq, width), buf(width, qkv_cols), table,
             table, dma(n_seq + 1)] + Gather.sems(2 * n_seq) + 3 * WeightGather.sems(1),
            [x_loc, dy_loc, gain_a, wqkv_sh, wout_t, wdown_t, cos_t, sin_t])

        mid, act, d_gu, dw_mlp, pieces, w_down_t = call(
            second_kernel, 'second', second, 100, 'VHVVHVVVH',
            [('V', local), ('H', shape(tokens, ff)), ('H', shape(tokens, 2 * ff)), ('H', shape(width, 3 * ff, dtype=F32)),
             ('H', shape(PIECES, width, piece_cols)), ('H', shape(width, ff))],
            Scatter.scratch(n_seq, pos, width)
            + [buf(width, out_rows), dma(Scatter.CHUNKS, 1), buf(n_seq, pos, width), buf(tokens, width),
               buf(tokens, width), DMA, buf(2, width, piece_cols), dma(2), buf(PIECES, shard_rows, piece_cols),
               buf(tokens, ff), buf(tokens, 2 * ff), buf(tokens, ff), dma(2, RING), dma(2)]
            + Gather.sems(n_seq) + WeightGather.sems(PIECES + 1),
            [attn, w_out_t, x_loc, gain_m, dy_full.reshape(tokens, width), wgate_sh, wup_sh, wdown_t, w_down_t], aliases={8: 5})

        block = width // 6
        rs_mlp = lax.psum_scatter(dw_mlp, 'fsdp', scatter_dimension=0, tiled=True)
        d_gu, dw_mlp = lax.optimization_barrier((d_gu, dw_mlp))

        d_mid, d_mid_full, dgain_mlp = call(
            back_kernel, 'back', back, 90, 'VHVVV',
            [('V', local), ('H', full), ('V', shape(fold, width // fold, dtype=F32))],
            Scatter.scratch(n_seq, pos, width)
            + [buf(width, 2 * ff), dma(Scatter.CHUNKS, PIECES), buf(n_seq, pos, width), row_t] + Gather.sems(n_seq),
            [d_gu.reshape(n_seq, seq, 2 * ff), pieces, dy_loc, mid, gain_m])

        d_qkv, dw_qkv, y, rs_out_t = call(
            functools.partial(attn_back_kernel, heads, group, scale), 'attn_back', attn_back, 60, 'HHHVHVVVVV',
            [('V', shape(tokens, qkv_cols)), ('H', shape(width, qkv_cols, dtype=F32)), ('V', local),
             ('V', shape(shard_rows, out_rows, dtype=F32))],
            Scatter.scratch(n_seq, pos, width) + GradScatter.scratch(shard_rows, out_rows)
            + [buf(width, ff), dma(Scatter.CHUNKS, 1), buf(tokens, width), buf(width, out_rows), dma(2),
               buf(2, tokens, block), dma(2), buf(2, block, qkv_cols, dtype=F32), dma(2), buf(seq, out_rows)] + 4 * [table],
            [d_mid_full.reshape(tokens, width), w_out_t, h_full.reshape(tokens, width), act.reshape(n_seq, seq, ff), w_down_t,
             cos_t, sin_t, qkv.reshape(tokens, qkv_cols), attn.reshape(tokens, out_rows), mid])

        gain_out = shape(1, width, dtype=F32)
        dx, rs_qkv, gain_attn_sum, gain_mlp_sum = call(
            leave_kernel, 'leave', leave, 60, 'VHVVVHV',
            [('V', local), ('V', shape(shard_rows, qkv_cols, dtype=F32)), ('V', gain_out), ('V', gain_out)],
            Scatter.scratch(n_seq, pos, width) + GradScatter.scratch(shard_rows, qkv_cols)
            + [buf(width, qkv_cols), dma(Scatter.CHUNKS, 1), row_t] + GainSum.scratch(2 * fold, width // fold),
            [d_qkv.reshape(n_seq, seq, qkv_cols), w_qkv, d_mid, x_loc, gain_a, dw_qkv, dgain_mlp])

        parts = (y, dx, gain_attn_sum, gain_mlp_sum, rs_qkv, rs_out_t)
        outs = tuple(jax.ShapeDtypeStruct(part.shape, part.dtype) for part in parts) + (shape(shard_rows, ff, dtype=F32),) * 3
        y, dx, gain_attn_sum, gain_mlp_sum, rs_qkv, rs_out_t, d_gate_w, d_up_w, d_down_t = pl.pallas_call(
            outputs_kernel, out_shape=outs, in_specs=[vmem] * (len(parts) + 1), out_specs=(vmem,) * len(outs), name='outputs',
            compiler_params=pltpu.CompilerParams(vmem_limit_bytes=VMEM_LIMIT))(rs_mlp, *parts)
        return y, dx, gain_attn_sum[0], gain_mlp_sum[0], rs_qkv, rs_out_t.T, d_gate_w, d_up_w, d_down_t.T

    in_specs = (act_spec, act_spec, P(), P(), rows_spec, cols_spec, rows_spec, rows_spec, cols_spec, P(), P())
    out_specs = (act_spec, act_spec, P(), P(), rows_spec, cols_spec, rows_spec, rows_spec, cols_spec)
    return jax.shard_map(device_fn, mesh=mesh, in_specs=in_specs, out_specs=out_specs, check_vma=False)
```

```python
import functools

import jax
import jax.numpy as jnp
from jax import lax
from jax.experimental import pallas as pl
from jax.experimental.pallas import tpu as pltpu
from jax.sharding import PartitionSpec as P

NORM_EPS = 1e-5
MASKED = -1e30
F32 = jnp.float32
BF16 = jnp.bfloat16
MESH = pl.DeviceIdType.MESH
DMA = pltpu.SemaphoreType.DMA
VMEM_LIMIT = 63 * 2 ** 20
RING = 4
ROWS = 16
PIECES = 4
HERE, NEXT, FAR, PREV = range(RING)
BY_RANK = (FAR, NEXT, PREV, HERE)
COLORS = range(2)
NT = (((1,), (1,)), ((), ()))
TN = (((0,), (0,)), ((), ()))


def go(place, distance):
    return (place + distance) % RING


def model_place():
    m = lax.axis_index('model')
    return m // 2, m % 2


def fsdp_place():
    f = lax.axis_index('fsdp')
    return f // RING, f % RING


def chip_targets():
    x, c = model_place()
    return [{'model': 2 * x + 1 - c}, {'model': 2 * go(x, NEXT) + c}, {'model': 2 * go(x, PREV) + c}]


def plane_targets():
    z, y = fsdp_place()
    return {'z': [{'fsdp': RING * go(z, d) + y} for d in (NEXT, PREV)],
            'y': [{'fsdp': RING * z + go(y, d)} for d in (NEXT, PREV)]}


def greet(targets):
    for target in targets:
        pl.semaphore_signal(pltpu.get_barrier_semaphore(), inc=1, device_id=target, device_id_type=MESH)


def met(targets):
    pl.semaphore_wait(pltpu.get_barrier_semaphore(), len(targets))


def chip_and_plane():
    plane = plane_targets()
    return chip_targets() + plane['z'] + plane['y']


def row_block(i, size, first=0):
    return pl.ds(pl.multiple_of(i * size + first, min(size, ROWS)), size)


def lane_block(i, size):
    return pl.ds(i * size if isinstance(i, int) else pl.multiple_of(i * size, size), size)


def row_loop(n_rows, fn, size=ROWS):
    def step(i, carry):
        fn(i)
        return carry
    lax.fori_loop(0, n_rows // size, step, None)


def row_sum(value):
    return jnp.sum(value, axis=-1, keepdims=True)


def row_mean(value):
    return jnp.mean(value, axis=-1, keepdims=True)


class Exchange:
    def __init__(self, send, recv):
        self.send, self.recv = send, recv

    def remote(self, i, src, dst, target):
        return pltpu.make_async_remote_copy(src_ref=src, dst_ref=dst, send_sem=self.send.at[i], recv_sem=self.recv.at[i],
                                            device_id=target, device_id_type=MESH)

    def landing(self):
        return [dst for _, dst, _ in self.copies()]

    def start(self, *which):
        table = self.copies()
        for i in which:
            self.remote(i, *table[i]).start()

    def arrived(self, *which):
        places, table = self.landing(), self.copies()
        for i in which:
            _, _, target = table[i]
            self.remote(i, places[i], places[i], target).wait_recv()

    def sent(self, *which):
        table = self.copies()
        for i in which or range(len(table)):
            self.remote(i, *table[i]).wait_send()


class Gather(Exchange):
    OTHER, UP, DOWN, PASS_UP, PASS_DOWN, PREV_OTHER, NEXT_OTHER, FAR_UP_OTHER, FAR_DOWN_OTHER = COPIES = range(9)

    def __init__(self, src, out, send, recv, local):
        super().__init__(send, recv)
        self.src, self.out, self.local = src, out, local
        self.x, self.c = model_place()
        self.pos, _ = src.shape
        self.half = self.pos // 2

    def block(self, distance, core):
        return self.out.at[row_block(2 * go(self.x, distance) + core, self.pos)]

    def part(self, distance, core, lower):
        place = 2 * go(self.x, distance) + core
        return self.out.at[row_block(2 * place + lower, self.half)]

    def copies(self):
        c = self.c
        other, nxt, prv = chip_targets()
        own = self.block(HERE, c)
        parts = [self.part(PREV, c, False), self.part(NEXT, c, True), self.block(PREV, c), self.block(NEXT, c),
                 self.part(FAR, c, False), self.part(FAR, c, True)]
        return [(self.src, own, other), (self.src, own, nxt), (self.src, own, prv)] + [
            (part, part, to) for part, to in zip(parts, (nxt, prv, other, other, other, other))]

    def landing(self):
        c, o = self.c, 1 - self.c
        return [self.block(HERE, o), self.block(PREV, c), self.block(NEXT, c), self.part(FAR, c, False),
                self.part(FAR, c, True), self.block(PREV, o), self.block(NEXT, o), self.part(FAR, o, False),
                self.part(FAR, o, True)]

    def own_copy(self):
        return pltpu.make_async_copy(self.src, self.block(HERE, self.c), self.local)

    def begin(self):
        if self.local is not None:
            self.own_copy().start()
        self.start(self.UP, self.DOWN, self.OTHER)

    def pass_near(self):
        self.arrived(self.UP)
        self.start(self.PASS_UP, self.PREV_OTHER)
        self.arrived(self.DOWN)
        self.start(self.PASS_DOWN, self.NEXT_OTHER)

    def pass_far(self):
        self.arrived(self.PASS_UP)
        self.start(self.FAR_UP_OTHER)
        self.arrived(self.PASS_DOWN)
        self.start(self.FAR_DOWN_OTHER)

    def complete(self):
        self.arrived(self.OTHER, self.PREV_OTHER, self.NEXT_OTHER, self.FAR_UP_OTHER, self.FAR_DOWN_OTHER)
        if self.local is not None:
            self.own_copy().wait()

    @classmethod
    def sems(cls, n):
        return [DMA((n, len(cls.COPIES))), DMA((n, len(cls.COPIES))), DMA((n,))]

    @classmethod
    def of(cls, i, src, out, sems, local=True):
        send, recv, local_sem = sems
        return cls(src, out, send.at[i], recv.at[i], local_sem.at[i] if local else None)


class RingGather(Exchange):
    UP, DOWN, PASS_UP, PASS_DOWN = COPIES = range(4)

    def __init__(self, src, at, targets, send, recv):
        super().__init__(send, recv)
        self.src, self.at, self.targets = src, at, targets
        rows, _ = src.shape
        self.upper, self.lower = row_block(0, rows // 2), row_block(1, rows // 2)

    def copies(self):
        nxt, prv = self.targets
        own, up, low = self.at(HERE), self.at(PREV).at[self.upper], self.at(NEXT).at[self.lower]
        return [(self.src, own, nxt), (self.src, own, prv), (up, up, nxt), (low, low, prv)]

    def landing(self):
        far = self.at(FAR)
        return [self.at(PREV), self.at(NEXT), far.at[self.upper], far.at[self.lower]]

    def begin(self):
        self.start(self.UP, self.DOWN)

    def pass_near(self):
        self.arrived(self.UP)
        self.start(self.PASS_UP)
        self.arrived(self.DOWN)
        self.start(self.PASS_DOWN)

    def far(self):
        self.arrived(self.PASS_UP, self.PASS_DOWN)


class WeightGather:
    def __init__(self, src, out, send, recv, local, first_row=0):
        self.src, self.out, self.local, self.first_row = src, out, local, first_row
        z, y = fsdp_place()
        self.place = RING * z + y
        self.rows, _ = src.shape
        half = self.rows // 2
        depth, _ = out.shape
        self.block = depth // RING ** 2
        targets = plane_targets()
        self.first, self.second = [], []
        for color, (one, two) in enumerate(('yz', 'zy')):
            part = src.at[row_block(color, half)]

            def at(d_one, d_two, one=one, color=color):
                dz, dy = (d_two, d_one) if one == 'y' else (d_one, d_two)
                first = (RING * go(z, dz) + go(y, dy)) * self.block + first_row + color * half
                return out.at[pl.ds(pl.multiple_of(first, ROWS), half)]
            self.first.append(RingGather(part, functools.partial(lambda at, d: at(d, HERE), at), targets[one],
                                         send.at[color, RING], recv.at[color, RING]))
            self.second.append([RingGather(at(d, HERE) if d else part, functools.partial(at, d), targets[two],
                                           send.at[color, d], recv.at[color, d]) for d in range(RING)])

    @staticmethod
    def sems(n):
        dims = (n, len(COLORS), RING + 1, len(RingGather.COPIES))
        return [DMA(dims), DMA(dims), DMA((n,))]

    @classmethod
    def of(cls, i, src, out, sems, local=True, first_row=0):
        send, recv, local_sem = sems
        return cls(src, out, send.at[i], recv.at[i], local_sem.at[i] if local else None, first_row)

    def own_rows(self):
        return pl.ds(pl.multiple_of(self.place * self.block + self.first_row, ROWS), self.rows)

    def own_copy(self):
        return pltpu.make_async_copy(self.src, self.out.at[self.own_rows()], self.local)

    def begin(self):
        if self.local is not None:
            self.own_copy().start()
        for ring in self.first:
            ring.begin()
        for rings in self.second:
            rings[HERE].begin()

    def pass_near(self):
        for one, two in zip(self.first, self.second):
            one.arrived(one.UP)
            one.start(one.PASS_UP)
            two[PREV].begin()
        for one, two in zip(self.first, self.second):
            one.arrived(one.DOWN)
            one.start(one.PASS_DOWN)
            two[NEXT].begin()
        self.pass_second(HERE)

    def pass_far(self):
        for one, two in zip(self.first, self.second):
            one.far()
            two[FAR].begin()

    def pass_second(self, d):
        for rings in self.second:
            rings[d].pass_near()

    def complete(self):
        for rings in self.second:
            for ring in rings:
                ring.far()
        if self.local is not None:
            self.own_copy().wait()

    def sent(self):
        for ring in self.first + sum(self.second, []):
            ring.sent()


class RingScatter(Exchange):
    FAR_UP, FAR_DOWN, UP_HI, DOWN_LO, UP_LO, DOWN_HI = COPIES = range(6)

    def __init__(self, mine, far, near, lo, hi, targets, send, recv):
        super().__init__(send, recv)
        self.mine, self.far, self.near, self.lo, self.hi, self.targets = mine, far, near, lo, hi, targets

    def copies(self):
        nxt, prv = self.targets
        far, up, down = (self.mine.at[BY_RANK.index(d)] for d in (FAR, NEXT, PREV))
        from_prv, from_nxt = self.near.at[0], self.near.at[1]
        lo, hi = self.lo, self.hi
        return [(far.at[lo], self.far.at[0], nxt), (far.at[hi], self.far.at[1], prv),
                (up.at[hi], from_prv.at[hi], nxt), (down.at[lo], from_nxt.at[lo], prv),
                (up.at[lo], from_prv.at[lo], nxt), (down.at[hi], from_nxt.at[hi], prv)]

    def begin(self):
        self.start(self.FAR_UP, self.FAR_DOWN, self.UP_HI, self.DOWN_LO)

    def add_far(self, add):
        up, down = (self.mine.at[BY_RANK.index(d)] for d in (NEXT, PREV))
        self.arrived(self.FAR_UP)
        add(up.at[self.lo], self.far.at[0])
        self.start(self.UP_LO)
        self.arrived(self.FAR_DOWN)
        add(down.at[self.hi], self.far.at[1])
        self.start(self.DOWN_HI)

    def arrive(self):
        self.arrived(self.UP_HI, self.DOWN_LO, self.UP_LO, self.DOWN_HI)

    def total(self, *at):
        return self.mine[(BY_RANK.index(HERE), *at)] + self.near[(0, *at)] + self.near[(1, *at)]


def add_rows(place, value):
    *outer, rows, _ = place.shape
    for at in [(i,) for i in range(*outer)] if outer else [()]:
        def add(i, at=at):
            place[(*at, row_block(i, ROWS))] += value[(*at, row_block(i, ROWS))]
        row_loop(rows, add)


class Scatter(Exchange):
    CHUNKS = 4

    def __init__(self, rows_of, weight, fetches, before, box, pair, mine, far, near, send, recv):
        super().__init__(send, recv)
        self.rows_of, self.weight, self.fetches, self.before = rows_of, weight, fetches, before
        self.box, self.pair, self.mine = box, pair, mine
        self.x, self.c = model_place()
        _, self.rows, self.width = mine.shape
        _, *ring_targets = chip_targets()
        half = self.width // 2
        rows = slice(None)
        ring_sems = (sem.at[pl.ds(RING, len(RingScatter.COPIES))] for sem in (send, recv))
        self.ring = RingScatter(mine, far, near, (rows, lane_block(0, half)), (rows, lane_block(1, half)), ring_targets,
                                *ring_sems)

    def copies(self):
        other, _, _ = chip_targets()
        return [(self.box.at[k], self.pair.at[k], other) for k in range(RING)]

    def pass_on(self, k):
        if self.before is not None:
            self.before.sent(k)
        chip = 2 * go(self.x, BY_RANK[k])
        left = jnp.concatenate([self.rows_of(chip + self.c), self.rows_of(chip + 1 - self.c)], axis=0)
        step = self.width // self.CHUNKS

        def chunk(i):
            if not k and self.fetches:
                for copy in self.fetches(i):
                    copy.wait()
            cols = lane_block(i, step)
            both = lax.dot_general(left, self.weight[cols, :], NT, preferred_element_type=F32)
            self.box[k, :, cols] = both[self.rows:]
            self.mine[k, :, cols] = both[:self.rows]
        row_loop(self.CHUNKS, chunk, 1)
        self.start(k)

    def pair_sum(self, k):
        self.arrived(k)
        add_rows(self.mine.at[k], self.pair.at[k])

    def send_near(self, meanwhile=None):
        far, up, down, here = range(RING)
        self.pass_on(far)
        if meanwhile is not None:
            meanwhile()
        self.pair_sum(far)
        self.ring.start(RingScatter.FAR_UP, RingScatter.FAR_DOWN)
        self.pass_on(up)
        self.pass_on(down)
        self.pair_sum(up)
        self.ring.start(RingScatter.UP_HI)
        self.pair_sum(down)
        self.ring.start(RingScatter.DOWN_LO)
        self.pass_on(here)

    def send_far(self):
        self.ring.add_far(add_rows)

    def arrive(self):
        self.pair_sum(BY_RANK.index(HERE))
        self.ring.arrive()

    def total(self, rows):
        return self.ring.total(rows)

    N_SCRATCH = 7

    @classmethod
    def scratch(cls, units, pos, width):
        sems = DMA((units, RING + len(RingScatter.COPIES)))
        return [pltpu.VMEM((RING, pos, width), F32), pltpu.VMEM((units, RING, pos, width), F32),
                pltpu.VMEM((units, RING, pos, width), F32), pltpu.VMEM((units, 2, pos, width // 2), F32),
                pltpu.VMEM((units, 2, pos, width), F32), sems, sems]

    @classmethod
    def all_of(cls, left, weight, fetches, scratch):
        box, *rest = scratch
        _, pos, _ = box.shape
        units, before = [], None
        n_seq, _, _ = left.shape
        for s in range(n_seq):
            def rows_of(place, s=s):
                return left[s, row_block(place, pos), :]
            before = cls(rows_of, weight, None if units else fetches, before, box, *(ref.at[s] for ref in rest))
            units.append(before)
        return units

    @staticmethod
    def all_sent(units):
        for unit in units:
            unit.ring.sent()
        unit.sent()


class GradScatter:
    N_SCRATCH = 9

    def __init__(self, part, out, mine1, far1, near1, mine2, far2, near2, send, recv, load):
        self.part, self.out, self.load, self.mine1, self.mine2 = part, out, load, mine1, mine2
        self.z, self.y = fsdp_place()
        rows, _ = out.shape
        self.half = rows // 2
        quarter = self.half // 2
        targets = plane_targets()
        self.one, self.two = [], []
        for color, (one, two) in enumerate(('yz', 'zy')):
            self.one.append(RingScatter(mine1.at[color], far1.at[color], near1.at[color], pl.ds(0, RING // 2),
                                        pl.ds(RING // 2, RING // 2), targets[one], send.at[color, 0], recv.at[color, 0]))
            self.two.append(RingScatter(mine2.at[color], far2.at[color], near2.at[color], row_block(0, quarter),
                                        row_block(1, quarter), targets[two], send.at[color, 1], recv.at[color, 1]))

    @staticmethod
    def scratch(rows, cols):
        half, n = rows // 2, len(COLORS)
        sems = DMA((n, 2, len(RingScatter.COPIES)))
        return [pltpu.VMEM((n, RING, RING, half, cols), F32), pltpu.VMEM((n, 2, RING // 2, half, cols), F32),
                pltpu.VMEM((n, 2, RING, half, cols), F32), pltpu.VMEM((n, RING, half, cols), F32),
                pltpu.VMEM((n, 2, half // 2, cols), F32), pltpu.VMEM((n, 2, half, cols), F32), sems, sems,
                DMA((n, RING, RING))]

    def loads(self):
        for color in COLORS:
            for k, d_one in enumerate(BY_RANK):
                for j, d_two in enumerate(BY_RANK):
                    dz, dy = (d_one, d_two) if color else (d_two, d_one)
                    place = RING * go(self.z, dz) + go(self.y, dy)
                    yield pltpu.make_async_copy(self.part.at[row_block(2 * place + color, self.half)],
                                                self.mine1.at[color, k, j], self.load.at[color, k, j])

    def fetch(self):
        for load in self.loads():
            load.start()

    def put(self, place, value):
        def rank(there, here):
            distance = (there + RING - here) % RING
            found = BY_RANK.index(HERE)
            for d in (NEXT, FAR, PREV):
                found = jnp.where(distance == d, BY_RANK.index(d), found)
            return found
        dz, dy = rank(place // RING, self.z), rank(place % RING, self.y)
        for color, at in enumerate(((dy, dz), (dz, dy))):
            self.mine1[(color, *at)] = value[color * self.half:(color + 1) * self.half]

    def begin(self):
        if self.part is not None:
            for load in self.loads():
                load.wait()
        for ring in self.one:
            ring.begin()

    def one_far(self):
        for ring in self.one:
            ring.add_far(add_rows)

    def one_done(self):
        for color, (one, two) in enumerate(zip(self.one, self.two)):
            one.arrive()
            for j in range(RING):
                def add(i, j=j):
                    rows = row_block(i, ROWS)
                    self.mine2[color, j, rows, :] = one.total(j, rows)
                row_loop(self.half, add)
            two.begin()

    def two_far(self):
        for ring in self.two:
            ring.add_far(add_rows)

    def two_done(self):
        for color, ring in enumerate(self.two):
            ring.arrive()

            def add(i):
                self.out[row_block(i, ROWS, color * self.half), :] = ring.total(row_block(i, ROWS))
            row_loop(self.half, add)

    def sent(self):
        for ring in self.one + self.two:
            ring.sent()


class GainSum:
    STAGES = 4

    def __init__(self, total, slots, send, recv):
        self.total, self.slots, self.send, self.recv = total, slots, send, recv
        (x, c), (z, y) = model_place(), fsdp_place()
        away = (NEXT, FAR, PREV)
        self.places = [c, x, y, z]
        self.targets = [[{'model': 2 * x + 1 - c}], [{'model': 2 * go(x, d) + c} for d in away],
                        [{'fsdp': RING * z + go(y, d)} for d in away], [{'fsdp': RING * go(z, d) + y} for d in away]]

    @classmethod
    def scratch(cls, *shape):
        dims = (cls.STAGES, RING - 1)
        return [pltpu.VMEM((cls.STAGES + 1, *shape), F32), pltpu.VMEM((*dims, *shape), F32), DMA(dims), DMA(dims)]

    def copies(self, t):
        return [pltpu.make_async_remote_copy(
            src_ref=self.total.at[t], dst_ref=self.slots.at[t, d], send_sem=self.send.at[t, d],
            recv_sem=self.recv.at[t, d], device_id=target, device_id_type=MESH)
            for d, target in enumerate(self.targets[t])]

    def start(self, t):
        for copy in self.copies(t):
            copy.start()

    def advance(self, t):
        others = len(self.targets[t])
        n = others + 1
        for copy in self.copies(t):
            copy.wait_recv()
        acc = None
        for i in range(n):
            term = self.total[t]
            for d in range(others):
                term = jnp.where((self.places[t] + others - d) % n == i, self.slots[t, d], term)
            acc = term if acc is None else acc + term
        self.total[t + 1] = acc
        if t + 1 < self.STAGES:
            self.start(t + 1)

    def sent(self):
        for t in range(self.STAGES):
            for copy in self.copies(t):
                copy.wait_send()


def norm_rows(x_f32, gain):
    return x_f32 * lax.rsqrt(row_mean(x_f32 * x_f32) + NORM_EPS) * gain


def norm_rows_back(x_f32, gain, cotangent):
    inv_rms = lax.rsqrt(row_mean(x_f32 * x_f32) + NORM_EPS)
    x_hat = x_f32 * inv_rms
    scaled = cotangent * gain
    return inv_rms * (scaled - x_hat * row_mean(scaled * x_hat)), cotangent * x_hat


def fold_row(row, out):
    rows, step = out.shape
    for i in range(rows):
        out[i:i + 1, :] = row[:, i * step:(i + 1) * step]


def unfold_row(rows_ref, out):
    rows, step = rows_ref.shape
    for i in range(rows):
        out[:, i * step:(i + 1) * step] = rows_ref[i:i + 1, :]


def rope_tables(cos_ref, sin_ref, cos_t, sin_t):
    cos, sin = cos_ref[...].T, sin_ref[...].T
    cos_t[...] = jnp.concatenate([cos, cos], axis=1)
    sin_t[...] = jnp.concatenate([-sin, sin], axis=1)


def spin(tensor, cos_t, sin_t):
    _, lanes = tensor.shape
    return tensor * cos_t + pltpu.roll(tensor, lanes // 2, 1) * sin_t


def probs(query, key, scale, first_row):
    scores = lax.dot_general(query, key, NT, preferred_element_type=F32) * scale
    rows, cols = (lax.broadcasted_iota(jnp.int32, scores.shape, dim) for dim in range(scores.ndim))
    scores = jnp.where(first_row + rows >= cols, scores, MASKED)
    expd = jnp.exp(scores - jnp.max(scores, axis=-1, keepdims=True))
    return expd / row_sum(expd)


def piece_of(refs, j, out):
    _, cols = out.shape
    step = cols // len(refs)
    for i, ref in enumerate(refs):
        out[:, lane_block(i, step)] = ref[:, lane_block(j, step)]


def fetch_weight(sources, w_vmem, sem):
    depth, _ = w_vmem.shape
    step = depth // Scatter.CHUNKS

    def chunk(i):
        rows, col, copies = row_block(i, step), 0, []
        for n, (ref, first, size) in enumerate(sources):
            copies.append(pltpu.make_async_copy(ref.at[rows, pl.ds(first, size)], w_vmem.at[rows, pl.ds(col, size)],
                                                sem.at[i, n]))
            col += size
        return copies
    for i in range(Scatter.CHUNKS):
        for copy in chunk(i):
            copy.start()
    return chunk


def early_rows(shard_rows):
    return shard_rows // 3


def first_kernel(heads, group, scale, x_ref, dy_ref, gain_ref, wqkv_src, wout_src, wd_src, cos_ref, sin_ref,
                 h_out, dy_out, wqkv_out, wout_out, wdown_out, qkv_ref, attn_ref,
                 h_src, h_buf, w_buf, cos_t, sin_t, flush, *sems):
    targets = chip_and_plane()
    greet(targets)
    n_seq, pos, _ = x_ref.shape
    seq, head_dim = cos_t.shape
    block = seq // 2
    _, cols = w_buf.shape
    x, c = model_place()
    mine = row_block(2 * x + c, pos)
    for s in range(n_seq):
        def norm(i, s=s):
            rows = row_block(i, ROWS)
            h_src[s, rows, :] = norm_rows(x_ref[s, rows, :].astype(F32), gain_ref[...]).astype(BF16)
        row_loop(pos, norm)
    g_sems, w_sems = sems[:3], sems[3:]
    w_qkv = WeightGather.of(0, wqkv_src, w_buf, w_sems[:3], local=False)
    w_out = WeightGather.of(0, wout_src, wout_out, w_sems[3:6])
    shard_rows, _ = wqkv_src.shape
    early = early_rows(shard_rows)
    w_down = WeightGather.of(0, wd_src.at[pl.ds(0, early)], wdown_out, w_sems[6:])
    h0, h1 = (Gather.of(s, h_src.at[s], h_buf.at[s], g_sems, local=False) for s in range(n_seq))
    dy0, dy1 = (Gather.of(n_seq + s, dy_ref.at[s], dy_out.at[s], g_sems) for s in range(n_seq))
    met(targets)
    w_qkv.begin()
    h0.begin()
    h1.begin()
    rope_tables(cos_ref, sin_ref, cos_t, sin_t)
    for s in range(n_seq):
        h_buf[s, mine, :] = h_src[s]
    w_buf[w_qkv.own_rows(), :] = wqkv_src[...]
    w_qkv.pass_near()
    w_out.begin()
    w_qkv.pass_far()
    h0.pass_near()
    w_qkv.pass_second(PREV)
    w_qkv.pass_second(NEXT)
    w_out.pass_near()
    w_down.begin()
    w_qkv.pass_second(FAR)
    h1.pass_near()
    dy0.begin()
    dy1.begin()
    w_out.pass_far()
    h0.pass_far()
    w_down.pass_near()
    w_out.pass_second(PREV)
    w_out.pass_second(NEXT)
    w_qkv.complete()
    w_flush = pltpu.make_async_copy(w_buf, wqkv_out, flush.at[n_seq])
    w_flush.start()

    def lanes(i):
        return lane_block(i, head_dim)

    def project(s):
        def one_block(i):
            rows = row_block(i, block)
            qkv = jnp.dot(h_buf[s, rows, :], w_buf[...], preferred_element_type=F32)
            for j in range(cols // head_dim):
                one = qkv[:, j * head_dim:(j + 1) * head_dim]
                if j % (group + 2) <= group:
                    one = spin(one, cos_t[rows, :], sin_t[rows, :])
                qkv_ref[s, rows, lanes(j)] = one.astype(BF16)
        row_loop(seq, one_block, block)

    def attend(s):
        for g in range(heads // group):
            first = g * (group + 2)

            def head(j, first=first, g=g):
                for i in range(seq // block):
                    rows, keys = pl.ds(i * block, block), pl.ds(0, (i + 1) * block)
                    key, value = qkv_ref[s, keys, lanes(first + group)], qkv_ref[s, keys, lanes(first + group + 1)]
                    prob = probs(qkv_ref[s, rows, lanes(first + j)], key, scale, i * block)
                    attn_ref[s, rows, lanes(g * group + j)] = jnp.dot(
                        prob.astype(BF16), value, preferred_element_type=F32).astype(BF16)
            row_loop(group, head, 1)

    def h_flush(s):
        return pltpu.make_async_copy(h_buf.at[s], h_out.at[s], flush.at[s])

    h0.complete()
    h_flush(0).start()
    project(0)
    w_down.pass_far()
    w_out.pass_second(FAR)
    h1.pass_far()
    attend(0)
    w_down.pass_second(PREV)
    w_down.pass_second(NEXT)
    h1.complete()
    h_flush(1).start()
    project(1)
    dy0.pass_near()
    w_down.pass_second(FAR)
    attend(1)
    dy0.pass_far()
    dy1.pass_near()
    dy1.pass_far()
    for each in (dy0, dy1, w_out, w_down):
        each.complete()
    for each in (h0, h1, dy0, dy1, w_qkv, w_out, w_down):
        each.sent()
    w_flush.wait()
    for s in range(n_seq):
        h_flush(s).wait()


def second_kernel(left, wout_hbm, base_ref, gain_ref, dy_hbm, wg_ref, wu_ref, wd_src, wdown_in, mid_ref, act_out, dgu_out,
                  dw_out, pieces_out, wdown_out, *scratch):
    targets = chip_and_plane()
    greet(targets)
    n_seq, pos, _ = base_ref.shape
    rs_scratch, scratch = scratch[:Scatter.N_SCRATCH], scratch[Scatter.N_SCRATCH:]
    (wo_vmem, wo_sem, g_src, h_buf, dy_buf, dy_sem, w_bufs, w_sem, piece_src, act_ref, dgu_ref, da_ref, dw_sem, flush,
     *scratch) = scratch
    _, _, stage, *_ = rs_scratch
    g_sems, p_sems = scratch[:3], scratch[3:]
    tokens, _ = dy_buf.shape
    seq = tokens // n_seq
    block = seq // 2
    _, out_rows = wo_vmem.shape
    _, _, cols = w_bufs.shape
    step = cols // 2
    fetches = fetch_weight([(wout_hbm, 0, out_rows)], wo_vmem, wo_sem)
    shard_rows, _ = wg_ref.shape
    early = early_rows(shard_rows)

    def fill(j):
        piece_of((wg_ref, wu_ref), j, piece_src.at[j])

    p0, p1, p2, p3 = pieces = [WeightGather.of(j, piece_src.at[j], pieces_out.at[j], p_sems) for j in range(PIECES)]
    w_down = WeightGather.of(PIECES, wd_src.at[pl.ds(early, shard_rows - early)], wdown_out, p_sems, first_row=early)
    x, c = model_place()
    units = Scatter.all_of(left, wo_vmem, fetches, rs_scratch)
    u0, u1 = units
    h0, h1 = gathers = [Gather.of(s, g_src.at[s], h_buf.at[pl.ds(s * seq, seq)], g_sems, local=False)
                        for s in range(n_seq)]

    def settle(s, unit, gather):
        unit.arrive()

        def rows_fn(i):
            rows = row_block(i, ROWS)
            red = unit.total(rows).astype(BF16).astype(F32)
            mid = (base_ref[s, rows, :].astype(F32) + red).astype(BF16)
            mid_ref[s, rows, :] = mid
            g_src[s, rows, :] = norm_rows(mid.astype(F32), gain_ref[...]).astype(BF16)
        row_loop(pos, rows_fn)
        gather.begin()
        h_buf[row_block(2 * x + c, pos, s * seq), :] = g_src[s]

    dy_load = pltpu.make_async_copy(dy_hbm, dy_buf, dy_sem)
    last = PIECES - 1

    def load_down(half):
        return pltpu.make_async_copy(wdown_out.at[:, lane_block(half, cols)], w_bufs.at[half], w_sem.at[half])

    def load_piece(load):
        piece = jnp.where(load == 2 * last, last, load % last)
        return pltpu.make_async_copy(pieces_out.at[piece], w_bufs.at[load % 2], w_sem.at[load % 2])

    def act_back(s, half):
        def rows_fn(i):
            there = row_block(i, block, s * seq)
            da_ref[there, lane_block(half, cols)] = jnp.dot(dy_buf[there, :], w_bufs[half],
                                                            preferred_element_type=F32).astype(BF16)
        row_loop(seq, rows_fn, block)

    def mlp(s, j, load):
        def rows_fn(i):
            there = row_block(i, block, s * seq)
            both = jnp.dot(h_buf[there, :], w_bufs[load % 2], preferred_element_type=F32)
            gate, up_proj = both[:, :step], both[:, step:]
            d_act = da_ref[there, lane_block(j, step)].astype(F32)
            sig_gate = jax.nn.sigmoid(gate)
            silu_gate = gate * sig_gate
            act_ref[there, lane_block(j, step)] = (silu_gate * up_proj).astype(BF16)
            dgu_ref[there, lane_block(2 * j, step)] = (
                d_act * up_proj * sig_gate * (1.0 + gate * (1.0 - sig_gate))).astype(BF16)
            dgu_ref[there, lane_block(2 * j + 1, step)] = (d_act * silu_gate).astype(BF16)
        row_loop(seq, rows_fn, block)

    def all_but_last(load):
        def ahead_of_second():
            h1.pass_near()
            p2.complete()
            p3.pass_far()

        def ahead_of_third():
            h1.pass_far()
            p3.pass_second(PREV)
            p3.pass_second(NEXT)

        def ahead_of_next_sequence():
            h1.complete()
            p3.pass_second(FAR)

        for at, fn in {1: ahead_of_second, 2: ahead_of_third, last: ahead_of_next_sequence, 2 * last - 1: p3.complete}.items():
            pl.when(load == at)(fn)
        load_piece(load).wait()
        load_piece(load + 1).start()
        mlp(load // last, load % last, load)

    _, kept_rows, _ = g_src.shape
    col_step = RING * kept_rows
    per_block = col_step // kept_rows
    width, _ = wo_vmem.shape
    _, cols_gu = dgu_ref.shape

    def dw_copies(i):
        return [pltpu.make_async_copy(stage.at[i % 2, k], dw_out.at[row_block(i * per_block + k, kept_rows)],
                                      dw_sem.at[i % 2, k]) for k in range(per_block)]

    def weight_grads(i):
        slot = i % 2

        @pl.when(i >= 2)
        def _():
            for copy in dw_copies(i - 2):
                copy.wait()
        half = cols_gu // 2
        h_t, dy_t = h_buf[:, lane_block(i, col_step)], dy_buf[:, lane_block(i, col_step)]
        for n, (left_cols, right) in enumerate(((h_t, dgu_ref[:, :half]), (h_t, dgu_ref[:, half:]), (dy_t, act_ref[...]))):
            block_of = lax.dot_general(left_cols, right, TN, preferred_element_type=F32)
            for k in range(per_block):
                stage[slot, k, :, lane_block(n, half)] = block_of[k * kept_rows:(k + 1) * kept_rows]
        for copy in dw_copies(i):
            copy.start()

    dy_load.start()

    def fill_first():
        for j in (0, 1):
            fill(j)
        w_down.begin()
        p0.begin()

    met(targets)
    u0.send_near(fill_first)
    for j in range(2, PIECES):
        fill(j)
    w_down.pass_near()
    u0.send_far()
    w_down.pass_far()
    w_down.pass_second(PREV)
    w_down.pass_second(NEXT)
    u1.send_near()
    p0.pass_near()
    p1.begin()
    w_down.pass_second(FAR)
    p0.pass_far()
    p0.pass_second(PREV)
    settle(0, u0, h0)
    p0.pass_second(NEXT)
    p1.pass_near()
    u1.send_far()
    w_down.complete()
    load_down(0).start()
    load_down(1).start()
    p0.pass_second(FAR)
    p1.pass_far()
    p2.begin()
    dy_load.wait()
    load_down(0).wait()
    act_back(0, 0)
    p1.pass_second(PREV)
    act_back(1, 0)
    p1.pass_second(NEXT)
    p2.pass_near()
    h0.pass_near()
    load_down(1).wait()
    act_back(0, 1)
    p1.pass_second(FAR)
    p2.pass_far()
    p3.begin()
    act_back(1, 1)
    p2.pass_second(PREV)
    p0.complete()
    load_piece(0).start()
    settle(1, u1, h1)
    h0.pass_far()
    p2.pass_second(NEXT)
    p2.pass_second(FAR)
    p3.pass_near()
    p1.complete()
    h0.complete()
    row_loop(2 * last, all_but_last, 1)
    load_piece(2 * last).wait()
    mlp(0, last, 2 * last)
    mlp(1, last, 2 * last)
    flushes = [pltpu.make_async_copy(act_ref, act_out, flush.at[0]), pltpu.make_async_copy(dgu_ref, dgu_out, flush.at[1])]
    for copy in flushes:
        copy.start()
    Scatter.all_sent(units)
    n_blocks = width // col_step
    row_loop(n_blocks, weight_grads, 1)
    for each in gathers + pieces + [w_down]:
        each.sent()
    for copy in flushes + dw_copies(n_blocks - 2) + dw_copies(n_blocks - 1):
        copy.wait()


def back_kernel(left, pieces, base_ref, mid_ref, gain_ref, res_ref, full_out, dgain_ref, *scratch):
    targets = chip_targets()
    greet(targets)
    n_seq, pos, _ = base_ref.shape
    rs_scratch, scratch = scratch[:Scatter.N_SCRATCH], scratch[Scatter.N_SCRATCH:]
    w_vmem, w_sem, g_src, sums, *sems = scratch
    _, depth = w_vmem.shape
    fetches = fetch_weight([(pieces.at[j], 0, depth // PIECES) for j in range(PIECES)], w_vmem, w_sem)
    units = Scatter.all_of(left, w_vmem, fetches, rs_scratch)
    u0, u1 = units
    g0, g1 = gathers = [Gather.of(s, g_src.at[s], full_out.at[s], sems) for s in range(n_seq)]
    sums[...] = jnp.zeros_like(sums)

    def settle(s, unit, gather):
        unit.arrive()

        def rows_fn(i):
            rows = row_block(i, ROWS)
            red = unit.total(rows).astype(BF16).astype(F32)
            d_norm, d_gain = norm_rows_back(mid_ref[s, rows, :].astype(F32), gain_ref[...], red)
            out = (base_ref[s, rows, :].astype(F32) + d_norm).astype(BF16)
            sums[...] += d_gain
            res_ref[s, rows, :] = out
            g_src[s, rows, :] = out
        row_loop(pos, rows_fn)
        gather.begin()

    met(targets)
    u0.send_near()
    u0.send_far()
    u1.send_near()
    settle(0, u0, g0)
    u1.send_far()
    g0.pass_near()
    settle(1, u1, g1)
    g0.pass_far()
    g1.pass_near()
    g1.pass_far()
    fold_row(jnp.sum(sums[...], axis=0, keepdims=True), dgain_ref)
    for gather in gathers:
        gather.complete()
    Scatter.all_sent(units)
    for gather in gathers:
        gather.sent()


def attn_back_kernel(heads, group, scale, dm_hbm, wo_hbm, h_hbm, left, wd_hbm, rope_cos, rope_sin, qkv_ref, attn_ref, mid_ref,
                     dqkv_ref, dwqkv_out, y_ref, dwout_ref, *scratch):
    targets = chip_and_plane()
    greet(targets)
    _, pos, width = mid_ref.shape
    half_dim, seq = rope_cos.shape
    head_dim = 2 * half_dim
    block = seq // 2
    rs_scratch, scratch = scratch[:Scatter.N_SCRATCH], scratch[Scatter.N_SCRATCH:]
    grads = GradScatter(None, dwout_ref, *scratch[:GradScatter.N_SCRATCH])
    (wd_vmem, wd_sem, dm_ref, wo_ref, in_sem, h_buf, h_sem, dw_buf, dw_sem, do_ref, dk_ref, dv_ref, cos_ref,
     sin_ref) = scratch[GradScatter.N_SCRATCH:]
    _, ff = wd_vmem.shape
    fetches = fetch_weight([(wd_hbm, 0, ff)], wd_vmem, wd_sem)
    dm_copy = pltpu.make_async_copy(dm_hbm, dm_ref, in_sem.at[0])
    wo_copy = pltpu.make_async_copy(wo_hbm, wo_ref, in_sem.at[1])
    dm_copy.start()
    wo_copy.start()
    _, _, h_cols = h_buf.shape
    n_blocks = width // h_cols

    def h_copy(i):
        return pltpu.make_async_copy(h_hbm.at[:, lane_block(i, h_cols)], h_buf.at[i % 2], h_sem.at[i % 2])

    def dw_copy(i):
        return pltpu.make_async_copy(dw_buf.at[i % 2], dwqkv_out.at[row_block(i, h_cols)], dw_sem.at[i % 2])
    h_copy(0).start()
    rope_tables(rope_cos, rope_sin, cos_ref, sin_ref)
    units = Scatter.all_of(left, wd_vmem, fetches, rs_scratch)
    u0, u1 = units

    def settle(s, unit):
        unit.arrive()

        def rows_fn(i):
            rows = row_block(i, ROWS)
            red = unit.total(rows).astype(BF16).astype(F32)
            y_ref[s, rows, :] = (mid_ref[s, rows, :].astype(F32) + red).astype(BF16)
        row_loop(pos, rows_fn)

    def out_grads():
        shard, _ = dwout_ref.shape

        def two_places(i):
            both = lax.dot_general(dm_ref[:, lane_block(i, 2 * shard)], attn_ref[...], TN, preferred_element_type=F32)
            grads.put(2 * i, both[:shard])
            grads.put(2 * i + 1, both[shard:])
        row_loop(width, two_places, 2 * shard)

    def lanes(i):
        return lane_block(i, head_dim)

    def attention(s):
        base = s * seq

        def project(i):
            do_ref[row_block(i, block), :] = jnp.dot(dm_ref[row_block(i, block, base), :], wo_ref[...],
                                                     preferred_element_type=F32).astype(BF16)
        row_loop(seq, project, block)
        for g in range(heads // group):
            first = g * (group + 2)
            dk_ref[...] = jnp.zeros_like(dk_ref)
            dv_ref[...] = jnp.zeros_like(dv_ref)
            for i in range(seq // block):
                rows, keys = pl.ds(i * block, block), pl.ds(0, (i + 1) * block)
                g_rows, g_keys = pl.ds(base + i * block, block), pl.ds(base, (i + 1) * block)
                key, value = qkv_ref[g_keys, lanes(first + group)], qkv_ref[g_keys, lanes(first + group + 1)]

                def head(j, rows=rows, keys=keys, g_rows=g_rows, key=key, value=value, first=first, g=g, i=i):
                    query = qkv_ref[g_rows, lanes(first + j)]
                    d_out = do_ref[rows, lanes(g * group + j)]
                    prob = probs(query, key, scale, i * block)
                    d_prob = lax.dot_general(d_out, value, NT, preferred_element_type=F32)
                    d_scores = (prob * (d_prob - row_sum(d_prob * prob)) * scale).astype(BF16)
                    d_query = jnp.dot(d_scores, key, preferred_element_type=F32)
                    dqkv_ref[g_rows, lanes(first + j)] = spin(d_query, cos_ref[rows, :], -sin_ref[rows, :]).astype(BF16)
                    dk_ref[keys, :] += lax.dot_general(d_scores, query, TN, preferred_element_type=F32)
                    dv_ref[keys, :] += lax.dot_general(prob.astype(BF16), d_out, TN, preferred_element_type=F32)
                row_loop(group, head, 1)
            every = pl.ds(base, seq)
            dqkv_ref[every, lanes(first + group)] = spin(dk_ref[...], cos_ref[...], -sin_ref[...]).astype(BF16)
            dqkv_ref[every, lanes(first + group + 1)] = dv_ref[...].astype(BF16)

    def qkv_grads():
        def one_block(i):
            @pl.when(i + 1 < n_blocks)
            def _():
                h_copy(i + 1).start()
            h_copy(i).wait()

            @pl.when(i >= 2)
            def _():
                dw_copy(i - 2).wait()
            dw_buf[i % 2] = lax.dot_general(h_buf[i % 2], dqkv_ref[...], TN, preferred_element_type=F32)
            dw_copy(i).start()
        row_loop(n_blocks, one_block, 1)

    met(targets)
    u0.send_near()
    dm_copy.wait()
    out_grads()
    grads.begin()
    u0.send_far()
    u1.send_near()
    wo_copy.wait()
    attention(0)
    u1.send_far()
    grads.one_far()
    settle(0, u0)
    attention(1)
    grads.one_done()
    qkv_grads()
    settle(1, u1)
    grads.two_far()
    grads.two_done()
    for i in (n_blocks - 2, n_blocks - 1):
        dw_copy(i).wait()
    Scatter.all_sent(units)
    grads.sent()


def leave_kernel(left, w_hbm, base_ref, x_ref, gain_ref, grad_hbm, dgm_ref, res_ref, grad_ref, ga_ref, gm_ref, *scratch):
    _, pos, _ = base_ref.shape
    rs_scratch, scratch = scratch[:Scatter.N_SCRATCH], scratch[Scatter.N_SCRATCH:]
    grads = GradScatter(grad_hbm, grad_ref, *scratch[:GradScatter.N_SCRATCH])
    w_vmem, w_sem, sums, *gain_scratch = scratch[GradScatter.N_SCRATCH:]
    gains = GainSum(*gain_scratch)
    targets = sum(gains.targets, [])
    greet(targets)
    grads.fetch()
    _, depth = w_vmem.shape
    fetches = fetch_weight([(w_hbm, 0, depth)], w_vmem, w_sem)
    sums[...] = jnp.zeros_like(sums)
    units = Scatter.all_of(left, w_vmem, fetches, rs_scratch)
    u0, u1 = units

    def settle(s, unit):
        unit.arrive()

        def rows_fn(i):
            rows = row_block(i, ROWS)
            red = unit.total(rows).astype(BF16).astype(F32)
            red, d_gain = norm_rows_back(x_ref[s, rows, :].astype(F32), gain_ref[...], red)
            sums[...] += d_gain
            res_ref[s, rows, :] = (base_ref[s, rows, :].astype(F32) + red).astype(BF16)
        row_loop(pos, rows_fn)

    met(targets)
    grads.begin()
    u0.send_near()
    u0.send_far()
    grads.one_far()
    u1.send_near()
    u1.send_far()
    settle(0, u0)
    grads.one_done()
    settle(1, u1)
    rows, _ = dgm_ref.shape
    start, end = gains.total.at[0], gains.total.at[gains.STAGES]
    start[rows:, :] = dgm_ref[...]
    fold_row(jnp.sum(sums[...], axis=0, keepdims=True), start.at[pl.ds(0, rows)])
    gains.start(0)
    grads.two_far()
    for t in range(gains.STAGES):
        gains.advance(t)
    grads.two_done()
    unfold_row(end.at[pl.ds(0, rows)], ga_ref)
    unfold_row(end.at[pl.ds(rows, rows)], gm_ref)
    gains.sent()
    Scatter.all_sent(units)
    grads.sent()


def outputs_kernel(grads_ref, *refs):
    *refs, gate_ref, up_ref, down_ref = refs
    n = len(refs) // 2
    for src, dst in zip(refs[:n], refs[n:]):
        dst[...] = src[...]
    _, ff = gate_ref.shape
    step = ff // PIECES
    for j in range(PIECES):
        gate_ref[:, lane_block(j, step)] = grads_ref[:, lane_block(2 * j, step)]
        up_ref[:, lane_block(j, step)] = grads_ref[:, lane_block(2 * j + 1, step)]
    down_ref[...] = grads_ref[:, lane_block(2, ff)]


def solution(mesh):
    act_spec = P('fsdp', 'model', None)
    rows_spec = P('fsdp', 'model')
    cols_spec = P('model', 'fsdp')

    def device_fn(x_loc, dy_loc, gain_attn, gain_mlp, wqkv_sh, wout_sh, wgate_sh, wup_sh, wdown_sh, rope_cos, rope_sin):
        n_seq, pos, width = x_loc.shape
        seq, half_dim = rope_cos.shape
        tokens = n_seq * seq
        head_dim = 2 * half_dim
        shard_rows, qkv_cols = wqkv_sh.shape
        out_rows, _ = wout_sh.shape
        ff, _ = wdown_sh.shape
        heads = out_rows // head_dim
        group = heads // ((qkv_cols - out_rows) // head_dim // 2)
        scale = head_dim ** -0.5
        gain_a, gain_m = gain_attn[None], gain_mlp[None]
        wout_t, wdown_t, cos_t, sin_t = wout_sh.T, wdown_sh.T, rope_cos.T, rope_sin.T
        piece_cols = 2 * ff // PIECES
        fold = 8

        vmem = pl.BlockSpec(memory_space=pltpu.VMEM)
        hbm = pl.BlockSpec(memory_space=pl.ANY)

        def shape(*dims, dtype=BF16):
            return jax.ShapeDtypeStruct(dims, dtype)

        def buf(*dims, dtype=BF16):
            return pltpu.VMEM(dims, dtype)

        def dma(*dims):
            return DMA(dims)

        def call(kernel, name, cid, us, ins, outs, scratch, args, aliases={}):
            spaces = {'V': vmem, 'H': hbm}
            shapes = tuple(out for _, out in outs)
            return pl.pallas_call(
                kernel, out_shape=shapes, in_specs=[spaces[i] for i in ins], out_specs=tuple(spaces[o] for o, _ in outs),
                scratch_shapes=scratch, name=name, input_output_aliases=aliases,
                cost_estimate=pl.CostEstimate(flops=us * 10 ** 9, bytes_accessed=10 ** 7, transcendentals=0),
                compiler_params=pltpu.CompilerParams(collective_id=cid, has_side_effects=True,
                                                     vmem_limit_bytes=VMEM_LIMIT))(*args)

        local, full = shape(n_seq, pos, width), shape(n_seq, seq, width)
        row_t, table = buf(ROWS, width, dtype=F32), buf(seq, head_dim, dtype=F32)
        first, second, back, attn_back, leave = range(5)

        h_full, dy_full, w_qkv, w_out_t, w_down_t, qkv, attn = call(
            functools.partial(first_kernel, heads, group, scale), 'first', first, 50, 'V' * 8,
            [('H', full), ('H', full), ('H', shape(width, qkv_cols)), ('H', shape(width, out_rows)),
             ('H', shape(width, ff)), ('V', shape(n_seq, seq, qkv_cols)),
             ('V', shape(n_seq, seq, out_rows))],
            [buf(n_seq, pos, width), buf(n_seq, seq, width), buf(width, qkv_cols), table,
             table, dma(n_seq + 1)] + Gather.sems(2 * n_seq) + 3 * WeightGather.sems(1),
            [x_loc, dy_loc, gain_a, wqkv_sh, wout_t, wdown_t, cos_t, sin_t])

        mid, act, d_gu, dw_mlp, pieces, w_down_t = call(
            second_kernel, 'second', second, 100, 'VHVVHVVVH',
            [('V', local), ('H', shape(tokens, ff)), ('H', shape(tokens, 2 * ff)), ('H', shape(width, 3 * ff, dtype=F32)),
             ('H', shape(PIECES, width, piece_cols)), ('H', shape(width, ff))],
            Scatter.scratch(n_seq, pos, width)
            + [buf(width, out_rows), dma(Scatter.CHUNKS, 1), buf(n_seq, pos, width), buf(tokens, width),
               buf(tokens, width), DMA, buf(2, width, piece_cols), dma(2), buf(PIECES, shard_rows, piece_cols),
               buf(tokens, ff), buf(tokens, 2 * ff), buf(tokens, ff), dma(2, RING), dma(2)]
            + Gather.sems(n_seq) + WeightGather.sems(PIECES + 1),
            [attn, w_out_t, x_loc, gain_m, dy_full.reshape(tokens, width), wgate_sh, wup_sh, wdown_t, w_down_t], aliases={8: 5})

        block = width // 6
        rs_mlp = lax.psum_scatter(dw_mlp, 'fsdp', scatter_dimension=0, tiled=True)
        d_gu, dw_mlp = lax.optimization_barrier((d_gu, dw_mlp))

        d_mid, d_mid_full, dgain_mlp = call(
            back_kernel, 'back', back, 90, 'VHVVV',
            [('V', local), ('H', full), ('V', shape(fold, width // fold, dtype=F32))],
            Scatter.scratch(n_seq, pos, width)
            + [buf(width, 2 * ff), dma(Scatter.CHUNKS, PIECES), buf(n_seq, pos, width), row_t] + Gather.sems(n_seq),
            [d_gu.reshape(n_seq, seq, 2 * ff), pieces, dy_loc, mid, gain_m])

        d_qkv, dw_qkv, y, rs_out_t = call(
            functools.partial(attn_back_kernel, heads, group, scale), 'attn_back', attn_back, 60, 'HHHVHVVVVV',
            [('V', shape(tokens, qkv_cols)), ('H', shape(width, qkv_cols, dtype=F32)), ('V', local),
             ('V', shape(shard_rows, out_rows, dtype=F32))],
            Scatter.scratch(n_seq, pos, width) + GradScatter.scratch(shard_rows, out_rows)
            + [buf(width, ff), dma(Scatter.CHUNKS, 1), buf(tokens, width), buf(width, out_rows), dma(2),
               buf(2, tokens, block), dma(2), buf(2, block, qkv_cols, dtype=F32), dma(2), buf(seq, out_rows)] + 4 * [table],
            [d_mid_full.reshape(tokens, width), w_out_t, h_full.reshape(tokens, width), act.reshape(n_seq, seq, ff), w_down_t,
             cos_t, sin_t, qkv.reshape(tokens, qkv_cols), attn.reshape(tokens, out_rows), mid])

        gain_out = shape(1, width, dtype=F32)
        dx, rs_qkv, gain_attn_sum, gain_mlp_sum = call(
            leave_kernel, 'leave', leave, 60, 'VHVVVHV',
            [('V', local), ('V', shape(shard_rows, qkv_cols, dtype=F32)), ('V', gain_out), ('V', gain_out)],
            Scatter.scratch(n_seq, pos, width) + GradScatter.scratch(shard_rows, qkv_cols)
            + [buf(width, qkv_cols), dma(Scatter.CHUNKS, 1), row_t] + GainSum.scratch(2 * fold, width // fold),
            [d_qkv.reshape(n_seq, seq, qkv_cols), w_qkv, d_mid, x_loc, gain_a, dw_qkv, dgain_mlp])

        parts = (y, dx, gain_attn_sum, gain_mlp_sum, rs_qkv, rs_out_t)
        outs = tuple(jax.ShapeDtypeStruct(part.shape, part.dtype) for part in parts) + (shape(shard_rows, ff, dtype=F32),) * 3
        y, dx, gain_attn_sum, gain_mlp_sum, rs_qkv, rs_out_t, d_gate_w, d_up_w, d_down_t = pl.pallas_call(
            outputs_kernel, out_shape=outs, in_specs=[vmem] * (len(parts) + 1), out_specs=(vmem,) * len(outs), name='outputs',
            compiler_params=pltpu.CompilerParams(vmem_limit_bytes=VMEM_LIMIT))(rs_mlp, *parts)
        return y, dx, gain_attn_sum[0], gain_mlp_sum[0], rs_qkv, rs_out_t.T, d_gate_w, d_up_w, d_down_t.T

    in_specs = (act_spec, act_spec, P(), P(), rows_spec, cols_spec, rows_spec, rows_spec, cols_spec, P(), P())
    out_specs = (act_spec, act_spec, P(), P(), rows_spec, cols_spec, rows_spec, rows_spec, cols_spec)
    return jax.shard_map(device_fn, mesh=mesh, in_specs=in_specs, out_specs=out_specs, check_vma=False)
```
